32 devices in a mesh: fsdp: 4 (over z), ep: 8 (over y, x, core).
Axes of the slice: x: 2, y: 2, z: 4, core: 2. Of those that a mesh axis runs over, the one named last changes fastest.
Arguments:
- x_tok: bfloat16 [8192, 512], P(('fsdp', 'ep'))
- dy_tok: bfloat16 [8192, 512], P(('fsdp', 'ep'))
- expert_ids: int32 [8192, 2], P(('fsdp', 'ep'))
- route_w: float32 [8192, 2], P(('fsdp', 'ep'))
- w_gate: bfloat16 [8, 512, 1792], P('ep', 'fsdp')
- w_up: bfloat16 [8, 512, 1792], P('ep', 'fsdp')
- w_down: bfloat16 [8, 1792, 512], P('ep', None, 'fsdp')
Outputs:
- output 1: bfloat16 [8192, 512], P(('fsdp', 'ep'))
- output 2: float32 [8192, 2], P(('fsdp', 'ep'))
- output 3: float32 [8, 512, 1792], P('ep', 'fsdp')
- output 4: float32 [8, 512, 1792], P('ep', 'fsdp')
- output 5: float32 [8, 1792, 512], P('ep', None, 'fsdp')
All inputs are finite; a program needn't handle non-finite values.
Results may differ from the reference program's by a relative error of at most 0.00103.
Values are sent between devices in bfloat16 or wider.
A program may use at most 1 GiB of HBM per device.

```python
import jax
import jax.numpy as jnp
from jax import lax

D_MODEL = 512
D_FF = 1792
EXPERTS = 8
TOP_K = 2
TOK_DEV = 256
DEVICES = 32
CAPACITY = 192

TOKENS = DEVICES * TOK_DEV
SLOTS = EXPERTS * CAPACITY
HOT_COUNT = max(1, TOP_K // 2)


def draw_routing(root_key):
    key_hot, key_score = jax.random.split(root_key)
    hot_rank = jax.random.permutation(key_hot, EXPERTS)
    bias = jnp.where(hot_rank < HOT_COUNT, 768, 0).astype(jnp.int32)
    expert_col = jnp.arange(EXPERTS, dtype=jnp.int32)

    def one_device(dev_key):
        noise = jax.random.randint(dev_key, (TOK_DEV, EXPERTS), 0, 1024, dtype=jnp.int32)
        score = (noise + bias[None, :]) * EXPERTS + expert_col[None, :]
        return lax.top_k(score, TOP_K)[1]

    chosen = lax.map(one_device, jax.random.split(key_score, DEVICES))
    return chosen.reshape(TOKENS, TOP_K).astype(jnp.int32)


def setup_inputs(seed: int = 0) -> dict:
    key_list = jax.random.split(jax.random.key(seed), 7)
    x_tok = jax.random.normal(key_list[0], (TOKENS, D_MODEL), jnp.float32)
    dy_tok = jax.random.normal(key_list[1], (TOKENS, D_MODEL), jnp.float32)
    expert_ids = draw_routing(key_list[2])
    route_w = jax.random.uniform(key_list[3], (TOKENS, TOP_K), jnp.float32, 0.1, 1.0)
    w_gate = jax.random.normal(key_list[4], (EXPERTS, D_MODEL, D_FF), jnp.float32) * D_MODEL ** -0.5
    w_up = jax.random.normal(key_list[5], (EXPERTS, D_MODEL, D_FF), jnp.float32) * D_MODEL ** -0.5
    w_down = jax.random.normal(key_list[6], (EXPERTS, D_FF, D_MODEL), jnp.float32) * D_FF ** -0.5
    return {
        "x_tok": x_tok.astype(jnp.bfloat16),
        "dy_tok": dy_tok.astype(jnp.bfloat16),
        "expert_ids": expert_ids,
        "route_w": route_w,
        "w_gate": w_gate.astype(jnp.bfloat16),
        "w_up": w_up.astype(jnp.bfloat16),
        "w_down": w_down.astype(jnp.bfloat16),
    }


def slot_positions(ids_dev):
    onehot = (ids_dev[:, None] == jnp.arange(EXPERTS, dtype=jnp.int32)[None, :]).astype(jnp.int32)
    before = jnp.cumsum(onehot, axis=0) - onehot
    position = jnp.sum(before * onehot, axis=1)
    return jnp.where(position < CAPACITY, ids_dev * CAPACITY + position, SLOTS)


def swiglu_grads(pre_gate, pre_up, grad_hidden):
    sigma = jax.nn.sigmoid(pre_gate)
    grad_gate = grad_hidden * pre_up * sigma * (1.0 + pre_gate * (1.0 - sigma))
    grad_up = grad_hidden * pre_gate * sigma
    return grad_gate.astype(jnp.bfloat16), grad_up.astype(jnp.bfloat16)


def reference(x_tok, dy_tok, expert_ids, route_w, w_gate, w_up, w_down):
    dest_slot = lax.map(slot_positions, expert_ids.reshape(DEVICES, TOK_DEV * TOP_K))
    pair_ids = jnp.arange(TOKENS * TOP_K, dtype=jnp.int32).reshape(DEVICES, TOK_DEV * TOP_K)
    dev_rows = jnp.broadcast_to(jnp.arange(DEVICES, dtype=jnp.int32)[:, None], dest_slot.shape)
    slot_src = jnp.full((DEVICES, SLOTS + 1), TOKENS * TOP_K, jnp.int32)
    slot_src = slot_src.at[dev_rows, dest_slot].set(pair_ids)[:, :SLOTS]
    per_expert = slot_src.reshape(DEVICES, EXPERTS, CAPACITY).transpose(1, 0, 2).reshape(EXPERTS, DEVICES * CAPACITY)
    route_flat = route_w.reshape(-1)

    def expert_step(carry, step_in):
        dx_acc, dr_acc = carry
        pair_src, w_gate_e, w_up_e, w_down_e = step_in
        tok_rows = pair_src // TOP_K
        x_rows = jnp.take(x_tok, tok_rows, axis=0, mode="fill", fill_value=0)
        dy_rows = jnp.take(dy_tok, tok_rows, axis=0, mode="fill", fill_value=0)
        gate_rows = jnp.take(route_flat, pair_src, axis=0, mode="fill", fill_value=0)
        pre_gate = jnp.dot(x_rows, w_gate_e, preferred_element_type=jnp.float32)
        pre_up = jnp.dot(x_rows, w_up_e, preferred_element_type=jnp.float32)
        hidden = (jax.nn.silu(pre_gate) * pre_up).astype(jnp.bfloat16)
        y_rows = jnp.dot(hidden, w_down_e, preferred_element_type=jnp.float32)
        dy_wide = dy_rows.astype(jnp.float32)
        scaled_dy = (gate_rows[:, None] * dy_wide).astype(jnp.bfloat16)
        dr_rows = jnp.sum(dy_wide * y_rows, axis=1)
        grad_hidden = jnp.dot(scaled_dy, w_down_e.T, preferred_element_type=jnp.float32)
        grad_gate, grad_up = swiglu_grads(pre_gate, pre_up, grad_hidden)
        dx_rows = (jnp.dot(grad_gate, w_gate_e.T, preferred_element_type=jnp.float32)
                   + jnp.dot(grad_up, w_up_e.T, preferred_element_type=jnp.float32)).astype(jnp.bfloat16)
        dw_gate = jnp.dot(x_rows.T, grad_gate, preferred_element_type=jnp.float32)
        dw_up = jnp.dot(x_rows.T, grad_up, preferred_element_type=jnp.float32)
        dw_down = jnp.dot(hidden.T, scaled_dy, preferred_element_type=jnp.float32)
        dx_acc = dx_acc.at[tok_rows].add(dx_rows.astype(jnp.float32), mode="drop")
        dr_acc = dr_acc.at[pair_src].set(dr_rows, mode="drop")
        return (dx_acc, dr_acc), (dw_gate, dw_up, dw_down)

    init = (jnp.zeros((TOKENS, D_MODEL), jnp.float32), jnp.zeros((TOKENS * TOP_K,), jnp.float32))
    (dx_acc, dr_acc), (grad_w_gate, grad_w_up, grad_w_down) = lax.scan(
        expert_step, init, (per_expert, w_gate, w_up, w_down))
    grad_x = dx_acc.astype(jnp.bfloat16)
    route_w_grad = dr_acc.reshape(TOKENS, TOP_K)
    return (grad_x, route_w_grad, grad_w_gate, grad_w_up, grad_w_down)
```

```python
import functools

import jax
import jax.numpy as jnp
from jax import lax
from jax.experimental import pallas as pl
from jax.experimental.pallas import tpu as pltpu
from jax.sharding import PartitionSpec as P

MESH = pl.DeviceIdType.MESH
CAP_FACTOR = 3
CHUNKS = 7
F32 = jnp.float32
BF16 = jnp.bfloat16
DIAG = (2, 4, 6)
DIRECT = (1, 2, 4, 6)
B_SLOT = (2, 3, 5, 7)
C_SLOT = (3, 4, 6, 8)


def capacity_of(tok_dev, top_k, experts):
    return max(8, ((CAP_FACTOR * tok_dev * top_k // experts + 7) // 8) * 8)


def flip(p, q):
    for b in (1, 2, 4):
        if q & b:
            p = p + b - 2 * b * lax.rem(lax.div(p, b), 2)
    return p


def dot_nn(a, b):
    return jnp.dot(a, b, preferred_element_type=F32)


def dot_nt(a, b):
    return lax.dot_general(a, b, (((1,), (1,)), ((), ())), preferred_element_type=F32)


def dot_tn(a, b):
    return lax.dot_general(a, b, (((0,), (0,)), ((), ())), preferred_element_type=F32)


def iota_f32(shape, dim):
    return lax.broadcasted_iota(jnp.int32, shape, dim).astype(F32)


def positions(meta, tri, cap):
    ids0, ids1 = meta[0:1, :], meta[1:2, :]
    row = iota_f32((16, meta.shape[1]), 0)
    chosen = jnp.where(ids0 == row, 1.0, 0.0) + jnp.where(ids1 == row, 1.0, 0.0)
    before = dot_nn(chosen.astype(BF16), tri)
    return jnp.where((chosen > 0.0) & (before < cap), before, -1.0)


def pick_row(pos16, e):
    row = iota_f32(pos16.shape, 0)
    return jnp.sum(jnp.where(row == e, pos16, 0.0), axis=0, keepdims=True)


def kernel(cap, n_z, n_p, meta_ref, xd_ref, w_ref, gx_ref, dr_ref, dw0_ref, dw1_ref, dw2_ref,
           xd_all, meta_all, w_all, tri_ref, xc_ref, gc_ref, dyc_ref, xt_ref, gt_ref, y_ref, dx_ref,
           dxs_ref, dxr_ref, drs_ref, drr_ref, gxa_ref,
           s_zt, r_zt, s_zm, r_zm, s_w, r_w, s_p, r_p, s_pm, r_pm, s_r, s_rm,
           s_dx, r_dx, s_dr, r_dr, s_loc):
    z = lax.axis_index("fsdp")
    p = lax.axis_index("ep")
    e_mine = p.astype(F32)
    n_tok, d2 = xd_ref.shape
    d = d2 // 2
    dl = w_ref.shape[1]
    f = w_ref.shape[2]
    fc = f // CHUNKS
    per_h = 4
    n_h = n_p // per_h
    partner = flip(p, 1)

    def plane_of(o):
        m = lax.div(z, 2)
        zz = z + m * (3 - 2 * z)
        if isinstance(o, int):
            jj = (zz, 1 - zz, 2, 3)[o]
        else:
            jj = o + jnp.where(o < 2, zz * (1 - 2 * o), 0)
        return jj + m * (3 - 2 * jj)

    barrier = pltpu.get_barrier_semaphore()
    for q in range(1, n_p):
        pl.semaphore_signal(barrier, inc=1, device_id={"ep": flip(p, q)}, device_id_type=MESH)
    for step in (1, -1):
        nb = z + step

        @pl.when((nb >= 0) & (nb < n_z))
        def _():
            pl.semaphore_signal(barrier, inc=1, device_id={"fsdp": nb}, device_id_type=MESH)

    inner = jnp.where(z > 0, 1, 0) + jnp.where(z < n_z - 1, 1, 0)
    pl.semaphore_wait(barrier, n_p - 1 + inner)

    def remote(src, dst, ssem, rsem, dev):
        return pltpu.make_async_remote_copy(
            src_ref=src, dst_ref=dst, send_sem=ssem, recv_sem=rsem, device_id=dev, device_id_type=MESH)

    def w_block(j, c):
        return w_all.at[:, pl.ds(pl.multiple_of(j * dl, dl), dl), pl.ds(pl.multiple_of(c * fc, fc), fc)]

    def zt_copy(j, way, own):
        dev = {"fsdp": z + 1 - 2 * way}
        return (remote(xd_ref if own else xd_all.at[j, p], xd_all.at[j, p], s_zt.at[way, j], r_zt.at[j], dev),
                remote(meta_ref if own else meta_all.at[j, p], meta_all.at[j, p], s_zm.at[way, j], r_zm.at[j], dev))

    def w_copy(j, c, way, own):
        src = w_ref.at[:, :, pl.ds(pl.multiple_of(c * fc, fc), fc)] if own else w_block(j, c)
        return remote(src, w_block(j, c), s_w.at[way, j, c], r_w.at[j, c], {"fsdp": z + 1 - 2 * way})

    def plane_copy(j, i, own):
        dev = {"ep": flip(p, DIRECT[i])}
        return (remote(xd_ref if own else xd_all.at[j, p], xd_all.at[j, p], s_p.at[j, i], r_p.at[j, p], dev),
                remote(meta_ref if own else meta_all.at[j, p], meta_all.at[j, p], s_pm.at[j, i], r_pm.at[j, p], dev))

    def relay_copy(j, i):
        pp = flip(p, DIAG[i])
        dev = {"ep": partner}
        return (remote(xd_all.at[j, pp], xd_all.at[j, pp], s_r.at[j, i], r_p.at[j, pp], dev),
                remote(meta_all.at[j, pp], meta_all.at[j, pp], s_rm.at[j, i], r_pm.at[j, pp], dev))

    def plane_wait(j, pp):
        remote(xd_all.at[j, pp], xd_all.at[j, pp], s_p.at[j, 0], r_p.at[j, pp], {"ep": partner}).wait_recv()
        remote(meta_all.at[j, pp], meta_all.at[j, pp], s_pm.at[j, 0], r_pm.at[j, pp], {"ep": partner}).wait_recv()

    def valid_z(j):
        return (j >= 0) & (j < n_z)

    def start_all(copies):
        for c in copies:
            c.start()

    for way in (0, 1):
        @pl.when(valid_z(z + 1 - 2 * way))
        def _():
            start_all(zt_copy(z, way, True))
    for i in range(4):
        start_all(plane_copy(z, i, True))
    loc_x = pltpu.make_async_copy(xd_ref, xd_all.at[z, p], s_loc.at[0])
    loc_m = pltpu.make_async_copy(meta_ref, meta_all.at[z, p], s_loc.at[1])
    loc_w = pltpu.make_async_copy(
        w_ref, w_all.at[:, pl.ds(pl.multiple_of(z * dl, dl), dl), :], s_loc.at[2])
    loc_x.start()
    loc_m.start()
    loc_w.start()

    tri_ref[...] = jnp.where(iota_f32((n_tok, n_tok), 0) < iota_f32((n_tok, n_tok), 1), 1.0, 0.0).astype(BF16)
    for ref in (dw0_ref, dw1_ref, dw2_ref, y_ref, dx_ref):
        ref[...] = jnp.zeros_like(ref)
    loc_x.wait()
    loc_m.wait()
    loc_w.wait()

    def rows_of(s):
        return lax.div(s, per_h), pl.ds(pl.multiple_of(lax.rem(s, per_h) * cap, cap), cap)

    def compact(o, j):
        def one(s, carry):
            meta = meta_all[j, s]
            pos = pick_row(positions(meta, tri_ref[...], cap), e_mine)
            hit = iota_f32((cap, n_tok), 0) == pos
            r_row = (jnp.where(meta[0:1, :] == e_mine, meta[2:3, :], 0.0)
                     + jnp.where(meta[1:2, :] == e_mine, meta[3:4, :], 0.0))
            r_col = jnp.sum(jnp.where(hit, r_row, 0.0), axis=1, keepdims=True)
            got = dot_nn(jnp.where(hit, 1.0, 0.0).astype(BF16), xd_all[j, s])
            h, rows = rows_of(s)
            dy = got[:, d:]
            xc_ref[o * n_h + h, rows, :] = got[:, :d].astype(BF16)
            gc_ref[o * n_h + h, rows, :] = (r_col * dy).astype(BF16)

            @pl.when(o == 0)
            def _():
                dyc_ref[h, rows, :] = dy.astype(BF16)

            return carry

        lax.fori_loop(0, n_p, one, 0)

        def turn(h, carry):
            cols = pl.ds(pl.multiple_of(z * dl, dl), dl)
            xt_ref[o * n_h + h] = xc_ref[o * n_h + h, :, cols].T
            gt_ref[o * n_h + h] = gc_ref[o * n_h + h, :, cols].T
            return carry

        lax.fori_loop(0, n_h, turn, 0)

    def cell(o, c, h):
        i = o * n_h + h
        cols = pl.ds(pl.multiple_of(c * fc, fc), fc)
        x, g = xc_ref[i], gc_ref[i]
        w1, w3, w2 = w_all[0, :, cols], w_all[1, :, cols], w_all[2, :, cols]
        h1 = dot_nn(x, w1)
        h3 = dot_nn(x, w3)
        da = dot_nn(g, w2)
        s = jax.nn.sigmoid(h1)
        a = (h1 * s * h3).astype(BF16)
        t = da * s
        dh3 = (t * h1).astype(BF16)
        dh1 = (t * h3 * (1.0 + h1 * (1.0 - s))).astype(BF16)
        dw0_ref[:, cols] += dot_nn(xt_ref[i], dh1)
        dw1_ref[:, cols] += dot_nn(xt_ref[i], dh3)
        dw2_ref[:, cols] += dot_nn(gt_ref[i], a)

        @pl.when(o == 0)
        def _():
            y_ref[h] += dot_nt(a, w2)
            dx_ref[h] += dot_nt(dh1, w1) + dot_nt(dh3, w3)

    def send_back():
        def one(s, carry):
            h, rows = rows_of(s)
            dxs_ref[s] = dx_ref[h, rows, :].astype(BF16)
            dr_col = jnp.sum(dyc_ref[h, rows, :].astype(F32) * y_ref[h, rows, :], axis=1, keepdims=True)
            pos = pick_row(positions(meta_all[z, s], tri_ref[...], cap), e_mine)
            hit = iota_f32((cap, n_tok), 0) == pos
            dr_row = jnp.sum(jnp.where(hit, dr_col, 0.0), axis=0, keepdims=True)
            drs_ref[s] = jnp.broadcast_to(dr_row, (8, n_tok))
            return carry

        lax.fori_loop(0, n_p, one, 0)
        for q in range(1, n_p):
            start_all(back_copy(q))
        for c in own_back():
            c.start()

    def back_copy(q):
        to = flip(p, q)
        return (remote(dxs_ref.at[to], dxr_ref.at[p], s_dx.at[q], r_dx.at[p], {"ep": to}),
                remote(drs_ref.at[to], drr_ref.at[p], s_dr.at[q], r_dr.at[p], {"ep": to}))

    def own_back():
        return (pltpu.make_async_copy(dxs_ref.at[p], dxr_ref.at[p], s_dx.at[0]),
                pltpu.make_async_copy(drs_ref.at[p], drr_ref.at[p], s_dr.at[0]))

    last = CHUNKS + 3

    def slot(k, carry):
        @pl.when(k < n_z)
        def _():
            for way in (0, 1):
                j = z - k * (1 - 2 * way)

                @pl.when(valid_z(j))
                def _():
                    for c in zt_copy(j, way, False):
                        c.wait_recv()

                    @pl.when(valid_z(z + 1 - 2 * way))
                    def _():
                        start_all(zt_copy(j, way, False))

                    for i in range(4):
                        start_all(plane_copy(j, i, False))

        for dist in (2, 1, 3):
            c = k - 1 - dist
            for way in (0, 1):
                j = z - dist * (1 - 2 * way)

                @pl.when(valid_z(j) & (c >= 0) & (c < CHUNKS))
                def _():
                    w_copy(j, c, way, False).wait_recv()

                    @pl.when(valid_z(z + 1 - 2 * way))
                    def _():
                        w_copy(j, c, way, False).start()

        for way in (0, 1):
            @pl.when(valid_z(z + 1 - 2 * way) & (k - 1 < CHUNKS))
            def _():
                w_copy(z, k - 1, way, True).start()

        for o in range(4):
            @pl.when(k == B_SLOT[o])
            def _():
                j = plane_of(o)
                for q in DIAG:
                    plane_wait(j, flip(p, q))
                for i in range(3):
                    start_all(relay_copy(j, i))

        def plane(o, carry):
            at = 3 + o + lax.div(o, 2) + lax.div(o, 3)

            @pl.when(k == at)
            def _():
                j = plane_of(o)
                plane_wait(j, partner)
                for q in DIAG:
                    plane_wait(j, flip(partner, q))
                compact(o, j)

            lo = jnp.where(k == at, 0, jnp.maximum(k - 4, 0))
            hi = jnp.where(k < at, lo, jnp.maximum(k - 3, 0))

            def chunk(c, carry):
                def half(h, carry):
                    cell(o, c, h)
                    return carry

                return lax.fori_loop(0, n_h, half, carry)

            lax.fori_loop(lo, hi, chunk, 0)

            @pl.when((o == 0) & (k == last))
            def _():
                send_back()

            return carry

        return lax.fori_loop(0, n_z, plane, carry)

    lax.fori_loop(1, last + 1, slot, 0)

    for q in range(1, n_p):
        frm = flip(p, q)
        remote(dxs_ref.at[frm], dxr_ref.at[frm], s_dx.at[q], r_dx.at[frm], {"ep": frm}).wait_recv()
        remote(drs_ref.at[frm], drr_ref.at[frm], s_dr.at[q], r_dr.at[frm], {"ep": frm}).wait_recv()
    for c in own_back():
        c.wait()
    meta = meta_ref[...]
    pos16 = positions(meta, tri_ref[...], cap)
    gxa_ref[...] = jnp.zeros_like(gxa_ref)
    dr_ref[...] = jnp.zeros_like(dr_ref)

    def gather(e, carry):
        ef = e.astype(F32)
        pos = pick_row(pos16, ef)
        hit = jnp.where(iota_f32((cap, n_tok), 0) == pos, 1.0, 0.0).astype(BF16)
        gxa_ref[...] += dot_tn(hit, dxr_ref[e])
        dr = drr_ref[e]
        for j in range(2):
            dr_ref[j:j + 1, :] += jnp.where(meta[j:j + 1, :] == ef, dr[0:1, :], 0.0)
        return carry

    lax.fori_loop(0, n_p, gather, 0)
    gx_ref[...] = gxa_ref[...].astype(BF16)

    for q in range(1, n_p):
        for c in back_copy(q):
            c.wait_send()
    for i in range(4):
        for j in range(n_z):
            for c in plane_copy(j, i, False):
                c.wait_send()
    for i in range(3):
        for j in range(n_z):
            for c in relay_copy(j, i):
                c.wait_send()
    for way in (0, 1):
        for dist in range(n_z):
            j = z - dist * (1 - 2 * way)

            @pl.when(valid_z(j) & valid_z(z + 1 - 2 * way))
            def _():
                for c in zt_copy(j, way, False):
                    c.wait_send()

                def drain(c, carry):
                    w_copy(j, c, way, False).wait_send()
                    return carry

                lax.fori_loop(0, CHUNKS, drain, 0)


def solution(mesh):
    n_z, n_p = mesh.shape["fsdp"], mesh.shape["ep"]
    tok_spec = P(("fsdp", "ep"), None)
    spec_in = P("ep", "fsdp", None)
    spec_out = P("ep", None, "fsdp")

    def per_device(x_tok, dy_tok, expert_ids, route_w, w_gate, w_up, w_down):
        n_tok, top_k = expert_ids.shape
        d = x_tok.shape[1]
        dl, f = w_gate.shape[1], w_gate.shape[2]
        cap = capacity_of(n_tok, top_k, n_p)
        xd = jnp.concatenate([x_tok, dy_tok], axis=1)
        meta = jnp.concatenate(
            [expert_ids.astype(F32).T, route_w.T, jnp.zeros((4, n_tok), F32)], axis=0)
        w = jnp.stack([w_gate[0], w_up[0], w_down[0].T])
        rows = 4 * cap
        n_t = n_z * n_p // 4
        sem = pltpu.SemaphoreType.DMA
        vmem = pl.BlockSpec(memory_space=pltpu.VMEM)
        out = jax.ShapeDtypeStruct
        gx, dr, dw0, dw1, dw2 = pl.pallas_call(
            functools.partial(kernel, cap, n_z, n_p),
            out_shape=(out((n_tok, d), BF16), out((8, n_tok), F32),
                       out((dl, f), F32), out((dl, f), F32), out((dl, f), F32)),
            in_specs=[vmem] * 3,
            out_specs=(vmem,) * 5,
            scratch_shapes=[
                pltpu.VMEM((n_z, n_p, n_tok, 2 * d), BF16),
                pltpu.VMEM((n_z, n_p, 8, n_tok), F32),
                pltpu.VMEM((3, n_z * dl, f), BF16),
                pltpu.VMEM((n_tok, n_tok), BF16),
                pltpu.VMEM((n_t, rows, d), BF16),
                pltpu.VMEM((n_t, rows, d), BF16),
                pltpu.VMEM((n_p // 4, rows, d), BF16),
                pltpu.VMEM((n_t, dl, rows), BF16),
                pltpu.VMEM((n_t, dl, rows), BF16),
                pltpu.VMEM((n_p // 4, rows, d), F32),
                pltpu.VMEM((n_p // 4, rows, d), F32),
                pltpu.VMEM((n_p, cap, d), BF16),
                pltpu.VMEM((n_p, cap, d), BF16),
                pltpu.VMEM((n_p, 8, n_tok), F32),
                pltpu.VMEM((n_p, 8, n_tok), F32),
                pltpu.VMEM((n_tok, d), F32),
                sem((2, n_z)), sem((n_z,)), sem((2, n_z)), sem((n_z,)),
                sem((2, n_z, CHUNKS)), sem((n_z, CHUNKS)),
                sem((n_z, 4)), sem((n_z, n_p)), sem((n_z, 4)), sem((n_z, n_p)),
                sem((n_z, 3)), sem((n_z, 3)),
                sem((n_p,)), sem((n_p,)), sem((n_p,)), sem((n_p,)),
                sem((3,)),
            ],
            compiler_params=pltpu.CompilerParams(
                collective_id=0, has_side_effects=True, vmem_limit_bytes=67043328),
        )(meta, xd, w)
        return gx, dr[:top_k].T, dw0[None], dw1[None], dw2.T[None]

    return jax.shard_map(
        per_device, mesh=mesh,
        in_specs=(tok_spec, tok_spec, tok_spec, tok_spec, spec_in, spec_in, spec_out),
        out_specs=(tok_spec, tok_spec, spec_in, spec_in, spec_out),
        check_vma=False)
```

```python
import functools

import jax
import jax.numpy as jnp
from jax import lax
from jax.experimental import pallas as pl
from jax.experimental.pallas import tpu as pltpu
from jax.sharding import PartitionSpec as P

MESH = pl.DeviceIdType.MESH
CAP_FACTOR = 3
CHUNKS = 7
F32 = jnp.float32
BF16 = jnp.bfloat16
DIAG = (2, 4, 6)
DIRECT = (1, 2, 4, 6)
SUB = 3
ORDER = ((0, 1, 2, 3), (1, 0, 2, 3), (2, 1, 3, 0), (3, 2, 1, 0))
STEPS = (
    (0, (0, 0), (0, 0), (0, 0), (0, 0)),
    (-1, (0, 1), (0, 0), (0, 0), (0, 0)),
    (1, (0, 0), (0, 1), (0, 0), (0, 0)),
    (-1, (1, 2), (1, 2), (0, 0), (0, 0)),
    (2, (0, 0), (0, 0), (0, 2), (0, 0)),
    (-1, (2, 3), (2, 3), (2, 3), (0, 0)),
    (-1, (3, 4), (3, 4), (3, 4), (0, 0)),
    (3, (0, 0), (0, 0), (0, 0), (0, 4)),
    (-1, (4, 5), (4, 5), (4, 5), (4, 5)),
    (-1, (5, 6), (5, 6), (5, 6), (5, 6)),
    (-1, (6, 7), (6, 7), (6, 7), (6, 7)),
)


def capacity_of(tok_dev, top_k, experts):
    return max(8, ((CAP_FACTOR * tok_dev * top_k // experts + 7) // 8) * 8)


def flip(p, q):
    for b in (1, 2, 4):
        if q & b:
            p = p + b - 2 * b * lax.rem(lax.div(p, b), 2)
    return p


def dot_nn(a, b):
    return jnp.dot(a, b, preferred_element_type=F32)


def dot_nt(a, b):
    return lax.dot_general(a, b, (((1,), (1,)), ((), ())), preferred_element_type=F32)


def dot_tn(a, b):
    return lax.dot_general(a, b, (((0,), (0,)), ((), ())), preferred_element_type=F32)


def iota_f32(shape, dim):
    return lax.broadcasted_iota(jnp.int32, shape, dim).astype(F32)


def positions(meta, tri, cap):
    ids0, ids1 = meta[0:1, :], meta[1:2, :]
    row = iota_f32((16, meta.shape[1]), 0)
    chosen = jnp.where(ids0 == row, 1.0, 0.0) + jnp.where(ids1 == row, 1.0, 0.0)
    before = dot_nn(chosen.astype(BF16), tri)
    return jnp.where((chosen > 0.0) & (before < cap), before, -1.0)


def pick_row(pos16, e):
    row = iota_f32(pos16.shape, 0)
    return jnp.sum(jnp.where(row == e, pos16, 0.0), axis=0, keepdims=True)


def pick(table, i):
    return sum(jnp.where(i == n, v, 0) for n, v in enumerate(table))


def kernel(cap, n_z, n_p, ids_ref, rw_ref, x_ref, dy_ref, wg_ref, wu_ref, wd_ref,
           gx_ref, dr_ref, dw0_ref, dw1_ref, dw2_ref,
           xd_all, meta_all, w_all, tri_ref, xc_ref, gc_ref, dyc_ref, xt_ref, gt_ref, y_ref, dx_ref,
           dxs_ref, dxr_ref, drs_ref, drr_ref, gxa_ref, dwt_ref,
           s_zt, r_zt, s_zm, r_zm, s_w, r_w, s_p, r_p, s_pm, r_pm, s_r, s_rm,
           s_dx, r_dx, s_dr, r_dr, s_loc):
    z = lax.axis_index("fsdp")
    p = lax.axis_index("ep")
    e_mine = p.astype(F32)
    n_tok, d = x_ref.shape
    dl, f = wg_ref.shape[1:]
    fc = f // CHUNKS
    per_h = 4
    n_h = n_p // per_h
    partner = flip(p, 1)
    own_rows = pl.ds(pl.multiple_of(z * dl, dl), dl)

    def plane_of(o):
        if isinstance(o, int):
            return pick([t[o] for t in ORDER], z)
        return sum(jnp.where(z == n, pick(t, o), 0) for n, t in enumerate(ORDER))

    loads = (
        pltpu.make_async_copy(x_ref, xd_all.at[z, p, :, pl.ds(0, d)], s_loc.at[0]),
        pltpu.make_async_copy(dy_ref, xd_all.at[z, p, :, pl.ds(d, d)], s_loc.at[1]),
        pltpu.make_async_copy(wg_ref.at[0], w_all.at[0, own_rows, :], s_loc.at[2]),
        pltpu.make_async_copy(wu_ref.at[0], w_all.at[1, own_rows, :], s_loc.at[3]),
    )
    for c in loads:
        c.start()

    barrier = pltpu.get_barrier_semaphore()
    for q in range(1, n_p):
        pl.semaphore_signal(barrier, inc=1, device_id={"ep": flip(p, q)}, device_id_type=MESH)
    for step in (1, -1):
        nb = z + step

        @pl.when((nb >= 0) & (nb < n_z))
        def _():
            pl.semaphore_signal(barrier, inc=1, device_id={"fsdp": nb}, device_id_type=MESH)

    for c in range(CHUNKS):
        w_all[2, own_rows, c * fc:(c + 1) * fc] = wd_ref[0, c * fc:(c + 1) * fc, :].T
    meta_all[z, p, 0:2, :] = ids_ref[...].astype(F32)
    meta_all[z, p, 2:4, :] = rw_ref[...]
    meta_all[z, p, 4:8, :] = jnp.zeros((4, n_tok), F32)
    tri_ref[...] = jnp.where(iota_f32((n_tok, n_tok), 0) < iota_f32((n_tok, n_tok), 1), 1.0, 0.0).astype(BF16)
    for ref in (dw0_ref, dw1_ref, dwt_ref, y_ref, dx_ref):
        ref[...] = jnp.zeros_like(ref)
    for c in loads:
        c.wait()
    inner = jnp.where(z > 0, 1, 0) + jnp.where(z < n_z - 1, 1, 0)
    pl.semaphore_wait(barrier, n_p - 1 + inner)

    def remote(src, dst, ssem, rsem, dev):
        return pltpu.make_async_remote_copy(
            src_ref=src, dst_ref=dst, send_sem=ssem, recv_sem=rsem, device_id=dev, device_id_type=MESH)

    def w_block(j, c):
        return w_all.at[:, pl.ds(pl.multiple_of(j * dl, dl), dl), pl.ds(pl.multiple_of(c * fc, fc), fc)]

    def zt_copy(j, way):
        dev = {"fsdp": z + 1 - 2 * way}
        return (remote(meta_all.at[j, p], meta_all.at[j, p], s_zm.at[way, j], r_zm.at[j], dev),
                remote(xd_all.at[j, p], xd_all.at[j, p], s_zt.at[way, j], r_zt.at[j], dev))

    def w_copy(j, c, way):
        return remote(w_block(j, c), w_block(j, c), s_w.at[way, j, c], r_w.at[j, c], {"fsdp": z + 1 - 2 * way})

    def plane_copy(j, i):
        dev = {"ep": flip(p, DIRECT[i])}
        return (remote(meta_all.at[j, p], meta_all.at[j, p], s_pm.at[j, i], r_pm.at[j, p], dev),
                remote(xd_all.at[j, p], xd_all.at[j, p], s_p.at[j, i], r_p.at[j, p], dev))

    def relay_copy(j, i):
        pp = flip(p, DIAG[i])
        dev = {"ep": partner}
        return (remote(meta_all.at[j, pp], meta_all.at[j, pp], s_rm.at[j, i], r_pm.at[j, pp], dev),
                remote(xd_all.at[j, pp], xd_all.at[j, pp], s_r.at[j, i], r_p.at[j, pp], dev))

    def plane_wait(j, pp):
        remote(meta_all.at[j, pp], meta_all.at[j, pp], s_pm.at[j, 0], r_pm.at[j, pp], {"ep": partner}).wait_recv()
        remote(xd_all.at[j, pp], xd_all.at[j, pp], s_p.at[j, 0], r_p.at[j, pp], {"ep": partner}).wait_recv()

    def valid_z(j):
        return (j >= 0) & (j < n_z)

    def start_all(copies):
        for c in copies:
            c.start()

    def link(way):
        return valid_z(z + 1 - 2 * way), (z if way == 0 else n_z - 1 - z)

    def upstream(way, dist):
        return z - dist * (1 - 2 * way)

    def own_w(depths, chunks):
        for way in (0, 1):
            there, depth = link(way)
            for q in depths:
                @pl.when(there & (depth == q))
                def _():
                    for c in chunks:
                        w_copy(z, c, way).start()

    def pass_w(q, dist, c):
        for way in (0, 1):
            there, depth = link(way)

            @pl.when(there & (depth == q))
            def _():
                j = upstream(way, dist)
                w_copy(j, c, way).wait_recv()
                w_copy(j, c, way).start()

    def need_w(c):
        for way in (0, 1):
            there, _ = link(way)
            for dist in range(1, n_z):
                j = upstream(way, dist)

                @pl.when(jnp.logical_not(there) & valid_z(j))
                def _():
                    w_copy(j, c, way).wait_recv()

    def tokens(dist):
        for way in (0, 1):
            there, _ = link(way)
            j = upstream(way, dist)

            @pl.when(valid_z(j))
            def _():
                for c in zt_copy(j, way):
                    c.wait_recv()

                @pl.when(there)
                def _():
                    start_all(zt_copy(j, way))

                for i in range(4):
                    start_all(plane_copy(j, i))

    def relay(o):
        j = plane_of(o)
        for i, q in enumerate(DIAG):
            plane_wait(j, flip(p, q))
            start_all(relay_copy(j, i))

    def landed(j):
        plane_wait(j, partner)
        for q in DIAG:
            plane_wait(j, flip(partner, q))

    def batch(q, c):
        own_w((q,), (c,))
        for dist in range(1, q + 1):
            pass_w(q, dist, c)

    own_w((0, 1, 2), (0,))
    for way in (0, 1):
        there, _ = link(way)

        @pl.when(there)
        def _():
            start_all(zt_copy(z, way))
    for i in range(4):
        start_all(plane_copy(z, i))
    own_w((0,), range(1, CHUNKS))

    def events(k):
        if k == 0:
            pass_w(1, 1, 0)
            pass_w(2, 1, 0)
            tokens(1)
            pass_w(2, 2, 0)
            batch(1, 1)
            relay(0)
        elif k == 1:
            tokens(2)
            batch(1, 2)
            need_w(0)
            own_w((2,), (1,))
        elif k == 2:
            pass_w(2, 1, 1)
            pass_w(2, 2, 1)
            batch(1, 3)
            relay(1)
            tokens(3)
        elif k == 3:
            batch(2, 2)
            batch(1, 4)
            need_w(1)
        elif k == 4:
            batch(2, 3)
            batch(1, 5)
            batch(1, 6)
            relay(2)
        elif k == 5:
            batch(2, 4)
            need_w(2)
        elif k == 6:
            batch(2, 5)
            need_w(3)
        elif k == 7:
            batch(2, 6)
            relay(3)
        else:
            need_w(k - 4)

    def rows_of(s):
        return lax.div(s, per_h), pl.ds(pl.multiple_of(lax.rem(s, per_h) * cap, cap), cap)

    def compact(o, j):
        def one(s, carry):
            meta = meta_all[j, s]
            pos = pick_row(positions(meta, tri_ref[...], cap), e_mine)
            hit = iota_f32((cap, n_tok), 0) == pos
            r_row = (jnp.where(meta[0:1, :] == e_mine, meta[2:3, :], 0.0)
                     + jnp.where(meta[1:2, :] == e_mine, meta[3:4, :], 0.0))
            r_col = jnp.sum(jnp.where(hit, r_row, 0.0), axis=1, keepdims=True)
            got = dot_nn(jnp.where(hit, 1.0, 0.0).astype(BF16), xd_all[j, s])
            h, rows = rows_of(s)
            dy = got[:, d:]
            xc_ref[o * n_h + h, rows, :] = got[:, :d].astype(BF16)
            gc_ref[o * n_h + h, rows, :] = (r_col * dy).astype(BF16)

            @pl.when(o == 0)
            def _():
                dyc_ref[h, rows, :] = dy.astype(BF16)

            return carry

        lax.fori_loop(0, n_p, one, 0)

        def turn(h, carry):
            xt_ref[o * n_h + h] = xc_ref[o * n_h + h, :, own_rows].T
            gt_ref[o * n_h + h] = gc_ref[o * n_h + h, :, own_rows].T
            return carry

        lax.fori_loop(0, n_h, turn, 0)

    def cells(o, c, own):
        cols = pl.ds(pl.multiple_of(c * fc, fc), fc)
        w1, w3, w2 = w_all[0, :, cols], w_all[1, :, cols], w_all[2, :, cols]
        rows = xc_ref.shape[1]
        size = rows // SUB
        subs = [(h, slice(n * size, (n + 1) * size)) for h in range(n_h) for n in range(SUB)]
        sums = [None] * 3
        held = []

        def behind(n):
            h, at = subs[n]
            a, dh1, dh3 = held[n]
            i = o * n_h + h
            for m, (left, right) in enumerate(((xt_ref, dh1), (xt_ref, dh3), (gt_ref, a))):
                term = dot_nn(left[i, :, at], right)
                sums[m] = term if sums[m] is None else sums[m] + term
            if own:
                y_ref[h, at, :] += dot_nt(a, w2)
                dx_ref[h, at, :] += dot_nt(dh1, w1) + dot_nt(dh3, w3)

        for n, (h, at) in enumerate(subs):
            i = o * n_h + h
            h1 = dot_nn(xc_ref[i, at, :], w1)
            h3 = dot_nn(xc_ref[i, at, :], w3)
            da = dot_nn(gc_ref[i, at, :], w2)
            s = jax.nn.sigmoid(h1)
            a = (h1 * s * h3).astype(BF16)
            t = da * s
            dh3 = (t * h1).astype(BF16)
            dh1 = (t * h3 * (1.0 + h1 * (1.0 - s))).astype(BF16)
            held.append((a, dh1, dh3))
            if n:
                behind(n - 1)
        behind(len(subs) - 1)
        for ref, total in zip((dw0_ref, dw1_ref, dwt_ref), sums):
            ref[:, cols] += total

    def send_back():
        def one(s, carry):
            h, rows = rows_of(s)
            dxs_ref[s] = dx_ref[h, rows, :].astype(BF16)
            dr_col = jnp.sum(dyc_ref[h, rows, :].astype(F32) * y_ref[h, rows, :], axis=1, keepdims=True)
            pos = pick_row(positions(meta_all[z, s], tri_ref[...], cap), e_mine)
            hit = iota_f32((cap, n_tok), 0) == pos
            dr_row = jnp.sum(jnp.where(hit, dr_col, 0.0), axis=0, keepdims=True)
            drs_ref[s] = jnp.broadcast_to(dr_row, (8, n_tok))
            return carry

        lax.fori_loop(0, n_p, one, 0)
        for q in range(1, n_p):
            start_all(back_copy(q))
        for c in own_back():
            c.start()

    def back_copy(q):
        to = flip(p, q)
        return (remote(drs_ref.at[to], drr_ref.at[p], s_dr.at[q], r_dr.at[p], {"ep": to}),
                remote(dxs_ref.at[to], dxr_ref.at[p], s_dx.at[q], r_dx.at[p], {"ep": to}))

    def own_back():
        return (pltpu.make_async_copy(dxs_ref.at[p], dxr_ref.at[p], s_dx.at[0]),
                pltpu.make_async_copy(drs_ref.at[p], drr_ref.at[p], s_dr.at[0]))

    n_steps = len(STEPS)

    def step(k, carry):
        for n in range(n_steps):
            @pl.when(k == n)
            def _():
                with jax.named_scope(f"events_{n}"):
                    events(n)

        packed = pick([t[0] for t in STEPS], k)

        @pl.when(packed >= 0)
        def _():
            j = plane_of(packed)
            with jax.named_scope("landed"):
                landed(j)
            with jax.named_scope("compact"):
                compact(packed, j)

        def chunk_own(c, carry):
            with jax.named_scope("cells_own"):
                cells(0, c, True)
            return carry

        lax.fori_loop(pick([t[1][0] for t in STEPS], k), pick([t[1][1] for t in STEPS], k), chunk_own, 0)

        @pl.when(k == n_steps - 1)
        def _():
            with jax.named_scope("send_back"):
                send_back()

        def plane(o, carry):
            def chunk(c, carry):
                with jax.named_scope("cells"):
                    cells(o, c, False)
                return carry

            lo = sum(jnp.where(o == n, pick([t[1 + n][0] for t in STEPS], k), 0) for n in range(1, n_z))
            hi = sum(jnp.where(o == n, pick([t[1 + n][1] for t in STEPS], k), 0) for n in range(1, n_z))
            return lax.fori_loop(lo, hi, chunk, carry)

        return lax.fori_loop(1, n_z, plane, carry)

    lax.fori_loop(0, n_steps, step, 0)

    for c in range(CHUNKS):
        dw2_ref[c * fc:(c + 1) * fc, :] = dwt_ref[:, c * fc:(c + 1) * fc].T
    with jax.named_scope("back_wait"):
        for q in range(1, n_p):
            frm = flip(p, q)
            remote(drs_ref.at[frm], drr_ref.at[frm], s_dr.at[q], r_dr.at[frm], {"ep": frm}).wait_recv()
            remote(dxs_ref.at[frm], dxr_ref.at[frm], s_dx.at[q], r_dx.at[frm], {"ep": frm}).wait_recv()
        for c in own_back():
            c.wait()
    meta = meta_all[z, p]
    pos16 = positions(meta, tri_ref[...], cap)
    gxa_ref[...] = jnp.zeros_like(gxa_ref)
    dr_ref[...] = jnp.zeros_like(dr_ref)

    def gather(e, carry):
        ef = e.astype(F32)
        pos = pick_row(pos16, ef)
        hit = jnp.where(iota_f32((cap, n_tok), 0) == pos, 1.0, 0.0).astype(BF16)
        gxa_ref[...] += dot_tn(hit, dxr_ref[e])
        dr = drr_ref[e]
        dr_ref[...] += jnp.where(meta[0:2, :] == ef, dr[0:1, :], 0.0)
        return carry

    with jax.named_scope("gather"):
        lax.fori_loop(0, n_p, gather, 0)
    gx_ref[...] = gxa_ref[...].astype(BF16)

    with jax.named_scope("drain"):
        for q in range(1, n_p):
            for c in back_copy(q):
                c.wait_send()
        for i in range(4):
            for j in range(n_z):
                for c in plane_copy(j, i):
                    c.wait_send()
        for i in range(3):
            for j in range(n_z):
                for c in relay_copy(j, i):
                    c.wait_send()
        for way in (0, 1):
            there, _ = link(way)
            for dist in range(n_z):
                j = upstream(way, dist)

                @pl.when(valid_z(j) & there)
                def _():
                    for c in zt_copy(j, way):
                        c.wait_send()

                    def drain(c, carry):
                        w_copy(j, c, way).wait_send()
                        return carry

                    lax.fori_loop(0, CHUNKS, drain, 0)


def solution(mesh):
    n_z, n_p = mesh.shape["fsdp"], mesh.shape["ep"]
    tok_spec = P(("fsdp", "ep"), None)
    spec_in = P("ep", "fsdp", None)
    spec_out = P("ep", None, "fsdp")

    def per_device(x_tok, dy_tok, expert_ids, route_w, w_gate, w_up, w_down):
        n_tok, top_k = expert_ids.shape
        d = x_tok.shape[1]
        dl, f = w_gate.shape[1], w_gate.shape[2]
        cap = capacity_of(n_tok, top_k, n_p)
        rows = 4 * cap
        n_t = n_z * n_p // 4
        sem = pltpu.SemaphoreType.DMA
        vmem = pl.BlockSpec(memory_space=pltpu.VMEM)
        hbm = pl.BlockSpec(memory_space=pl.ANY)
        out = jax.ShapeDtypeStruct
        gx, dr, dw0, dw1, dw2 = pl.pallas_call(
            functools.partial(kernel, cap, n_z, n_p),
            out_shape=(out((n_tok, d), BF16), out((top_k, n_tok), F32),
                       out((dl, f), F32), out((dl, f), F32), out((f, dl), F32)),
            in_specs=[vmem] * 2 + [hbm] * 4 + [vmem],
            out_specs=(vmem,) * 5,
            scratch_shapes=[
                pltpu.VMEM((n_z, n_p, n_tok, 2 * d), BF16),
                pltpu.VMEM((n_z, n_p, 8, n_tok), F32),
                pltpu.VMEM((3, n_z * dl, f), BF16),
                pltpu.VMEM((n_tok, n_tok), BF16),
                pltpu.VMEM((n_t, rows, d), BF16),
                pltpu.VMEM((n_t, rows, d), BF16),
                pltpu.VMEM((n_p // 4, rows, d), BF16),
                pltpu.VMEM((n_t, dl, rows), BF16),
                pltpu.VMEM((n_t, dl, rows), BF16),
                pltpu.VMEM((n_p // 4, rows, d), F32),
                pltpu.VMEM((n_p // 4, rows, d), F32),
                pltpu.VMEM((n_p, cap, d), BF16),
                pltpu.VMEM((n_p, cap, d), BF16),
                pltpu.VMEM((n_p, 8, n_tok), F32),
                pltpu.VMEM((n_p, 8, n_tok), F32),
                pltpu.VMEM((n_tok, d), F32),
                pltpu.VMEM((dl, f), F32),
                sem((2, n_z)), sem((n_z,)), sem((2, n_z)), sem((n_z,)),
                sem((2, n_z, CHUNKS)), sem((n_z, CHUNKS)),
                sem((n_z, 4)), sem((n_z, n_p)), sem((n_z, 4)), sem((n_z, n_p)),
                sem((n_z, 3)), sem((n_z, 3)),
                sem((n_p,)), sem((n_p,)), sem((n_p,)), sem((n_p,)),
                sem((4,)),
            ],
            compiler_params=pltpu.CompilerParams(
                collective_id=0, has_side_effects=True, vmem_limit_bytes=67043328),
        )(expert_ids.T, route_w.T, x_tok, dy_tok, w_gate, w_up, w_down)
        return gx, dr.T, dw0[None], dw1[None], dw2[None]

    return jax.shard_map(
        per_device, mesh=mesh,
        in_specs=(tok_spec, tok_spec, tok_spec, tok_spec, spec_in, spec_in, spec_out),
        out_specs=(tok_spec, tok_spec, spec_in, spec_in, spec_out),
        check_vma=False)
```

```python
import functools

import jax
import jax.numpy as jnp
from jax import lax
from jax.experimental import pallas as pl
from jax.experimental.pallas import tpu as pltpu
from jax.sharding import PartitionSpec as P

MESH = pl.DeviceIdType.MESH
CAP_FACTOR = 3
CHUNKS = 7
F32 = jnp.float32
BF16 = jnp.bfloat16
DIAG = (2, 4, 6)
DIRECT = (1, 2, 4, 6)
SUB = 3
RETURN = (6, 4, 7, 5, 2, 3, 1, 0)
ORDER = ((0, 1, 2, 3), (1, 0, 2, 3), (2, 1, 3, 0), (3, 2, 1, 0))
STEPS = (
    (0, (0, 0), (0, 0), (0, 0), (0, 0)),
    (-1, (0, 1), (0, 0), (0, 0), (0, 0)),
    (1, (0, 0), (0, 1), (0, 0), (0, 0)),
    (-1, (1, 2), (1, 2), (0, 0), (0, 0)),
    (2, (0, 0), (0, 0), (0, 2), (0, 0)),
    (-1, (2, 3), (2, 3), (2, 3), (0, 0)),
    (-1, (3, 4), (3, 4), (3, 4), (0, 0)),
    (3, (0, 0), (0, 0), (0, 0), (0, 4)),
    (-1, (4, 5), (0, 0), (0, 0), (0, 0)),
    (-1, (5, 6), (4, 5), (4, 5), (4, 5)),
    (-1, (6, 7), (5, 7), (5, 7), (5, 7)),
)


def capacity_of(tok_dev, top_k, experts):
    return max(8, ((CAP_FACTOR * tok_dev * top_k // experts + 7) // 8) * 8)


def flip(p, q):
    for b in (1, 2, 4):
        turned = b - 2 * b * lax.rem(lax.div(p, b), 2)
        if isinstance(q, int):
            p = p + turned if q & b else p
        else:
            p = p + lax.rem(lax.div(q, b), 2) * turned
    return p


def dot_nn(a, b):
    return jnp.dot(a, b, preferred_element_type=F32)


def dot_nt(a, b):
    return lax.dot_general(a, b, (((1,), (1,)), ((), ())), preferred_element_type=F32)


def dot_tn(a, b):
    return lax.dot_general(a, b, (((0,), (0,)), ((), ())), preferred_element_type=F32)


def iota_f32(shape, dim):
    return lax.broadcasted_iota(jnp.int32, shape, dim).astype(F32)


def earlier(n):
    return jnp.where(iota_f32((n, n), 0) < iota_f32((n, n), 1), 1.0, 0.0).astype(BF16)


def positions(meta, tri, cap):
    ids0, ids1 = meta[0:1, :], meta[1:2, :]
    row = iota_f32((16, meta.shape[1]), 0)
    chosen = jnp.where(ids0 == row, 1.0, 0.0) + jnp.where(ids1 == row, 1.0, 0.0)
    before = dot_nn(chosen.astype(BF16), tri)
    return jnp.where((chosen > 0.0) & (before < cap), before, -1.0)


def pick_row(pos16, e):
    row = iota_f32(pos16.shape, 0)
    return jnp.sum(jnp.where(row == e, pos16, 0.0), axis=0, keepdims=True)


def pick(table, i):
    return sum(jnp.where(i == n, v, 0) for n, v in enumerate(table))


def kernel(cap, n_z, n_p, ids_ref, rw_ref, x_ref, dy_ref, wg_ref, wu_ref, wd_ref,
           dxr_ref, drr_ref, dw0_out, dw1_out, dw2_out,
           xd_all, meta_all, w_all, tri_ref, xc_ref, gc_ref, dyc_ref, xt_ref, gt_ref, dy_y_ref, dx_ref,
           dxs_ref, drs_ref, dw0_ref, dw1_ref, dwt_ref, dw2_ref, wd_own,
           s_zt, r_zt, s_zm, r_zm, s_w, r_w, s_p, r_p, s_pm, r_pm, s_r, s_rm,
           s_dx, r_dx, s_dr, r_dr, s_loc):
    z = lax.axis_index("fsdp")
    p = lax.axis_index("ep")
    e_mine = p.astype(F32)
    n_tok, d = x_ref.shape
    dl, f = wg_ref.shape[1:]
    fc = f // CHUNKS
    per_h = 4
    n_h = n_p // per_h
    partner = flip(p, 1)
    own_rows = pl.ds(pl.multiple_of(z * dl, dl), dl)

    def plane_of(o):
        if isinstance(o, int):
            return pick([t[o] for t in ORDER], z)
        return sum(jnp.where(z == n, pick(t, o), 0) for n, t in enumerate(ORDER))

    barrier = pltpu.get_barrier_semaphore()
    for q in range(1, n_p):
        pl.semaphore_signal(barrier, inc=1, device_id={"ep": flip(p, q)}, device_id_type=MESH)
    for step in (1, -1):
        nb = z + step

        @pl.when((nb >= 0) & (nb < n_z))
        def _():
            pl.semaphore_signal(barrier, inc=1, device_id={"fsdp": nb}, device_id_type=MESH)

    load_wd = pltpu.make_async_copy(wd_ref.at[0], wd_own, s_loc.at[4])
    loads = (
        pltpu.make_async_copy(wg_ref.at[0], w_all.at[0, own_rows, :], s_loc.at[2]),
        pltpu.make_async_copy(wu_ref.at[0], w_all.at[1, own_rows, :], s_loc.at[3]),
        pltpu.make_async_copy(x_ref, xd_all.at[z, p, :, pl.ds(0, d)], s_loc.at[0]),
        pltpu.make_async_copy(dy_ref, xd_all.at[z, p, :, pl.ds(d, d)], s_loc.at[1]),
    )
    load_wd.start()
    for c in loads:
        c.start()
    meta_all[z, p, 0:2, :] = ids_ref[...].astype(F32)
    meta_all[z, p, 2:4, :] = rw_ref[...]
    meta_all[z, p, 4:8, :] = jnp.zeros((4, n_tok), F32)
    load_wd.wait()
    for c in range(CHUNKS):
        w_all[2, own_rows, c * fc:(c + 1) * fc] = wd_own[c * fc:(c + 1) * fc, :].T
    for c in loads:
        c.wait()
    inner = jnp.where(z > 0, 1, 0) + jnp.where(z < n_z - 1, 1, 0)
    pl.semaphore_wait(barrier, n_p - 1 + inner)

    def remote(src, dst, ssem, rsem, dev):
        return pltpu.make_async_remote_copy(
            src_ref=src, dst_ref=dst, send_sem=ssem, recv_sem=rsem, device_id=dev, device_id_type=MESH)

    def w_block(j, c):
        return w_all.at[:, pl.ds(pl.multiple_of(j * dl, dl), dl), pl.ds(pl.multiple_of(c * fc, fc), fc)]

    def zt_copy(j, way):
        dev = {"fsdp": z + 1 - 2 * way}
        return (remote(meta_all.at[j, p], meta_all.at[j, p], s_zm.at[way, j], r_zm.at[j], dev),
                remote(xd_all.at[j, p], xd_all.at[j, p], s_zt.at[way, j], r_zt.at[j], dev))

    def w_copy(j, c, way):
        return remote(w_block(j, c), w_block(j, c), s_w.at[way, j, c], r_w.at[j, c], {"fsdp": z + 1 - 2 * way})

    def plane_copy(j, i):
        dev = {"ep": flip(p, DIRECT[i])}
        return (remote(meta_all.at[j, p], meta_all.at[j, p], s_pm.at[j, i], r_pm.at[j, p], dev),
                remote(xd_all.at[j, p], xd_all.at[j, p], s_p.at[j, i], r_p.at[j, p], dev))

    def relay_copy(j, i):
        pp = flip(p, DIAG[i])
        dev = {"ep": partner}
        return (remote(meta_all.at[j, pp], meta_all.at[j, pp], s_rm.at[j, i], r_pm.at[j, pp], dev),
                remote(xd_all.at[j, pp], xd_all.at[j, pp], s_r.at[j, i], r_p.at[j, pp], dev))

    def plane_wait(j, pp):
        remote(meta_all.at[j, pp], meta_all.at[j, pp], s_pm.at[j, 0], r_pm.at[j, pp], {"ep": partner}).wait_recv()
        remote(xd_all.at[j, pp], xd_all.at[j, pp], s_p.at[j, 0], r_p.at[j, pp], {"ep": partner}).wait_recv()

    def valid_z(j):
        return (j >= 0) & (j < n_z)

    def start_all(copies):
        for c in copies:
            c.start()

    def link(way):
        return valid_z(z + 1 - 2 * way), (z if way == 0 else n_z - 1 - z)

    def upstream(way, dist):
        return z - dist * (1 - 2 * way)

    def own_w(depths, chunks):
        for way in (0, 1):
            there, depth = link(way)
            for q in depths:
                @pl.when(there & (depth == q))
                def _():
                    for c in chunks:
                        w_copy(z, c, way).start()

    def pass_w(q, dist, c):
        for way in (0, 1):
            there, depth = link(way)

            @pl.when(there & (depth == q))
            def _():
                j = upstream(way, dist)
                w_copy(j, c, way).wait_recv()
                w_copy(j, c, way).start()

    def need_w(c):
        for way in (0, 1):
            there, _ = link(way)
            for dist in range(1, n_z):
                j = upstream(way, dist)

                @pl.when(jnp.logical_not(there) & valid_z(j))
                def _():
                    w_copy(j, c, way).wait_recv()

    def tokens(dist):
        for way in (0, 1):
            there, _ = link(way)
            j = upstream(way, dist)

            @pl.when(valid_z(j))
            def _():
                for c in zt_copy(j, way):
                    c.wait_recv()

                @pl.when(there)
                def _():
                    start_all(zt_copy(j, way))

                for i in range(4):
                    start_all(plane_copy(j, i))

    def relay(o):
        j = plane_of(o)
        for i, q in enumerate(DIAG):
            plane_wait(j, flip(p, q))
            start_all(relay_copy(j, i))

    def landed(j):
        plane_wait(j, partner)
        for q in DIAG:
            plane_wait(j, flip(partner, q))

    def batch(q, c):
        own_w((q,), (c,))
        for dist in range(1, q + 1):
            pass_w(q, dist, c)

    own_w((0, 1, 2), (0,))
    for way in (0, 1):
        there, _ = link(way)

        @pl.when(there)
        def _():
            start_all(zt_copy(z, way))
    for i in range(4):
        start_all(plane_copy(z, i))
    own_w((0,), range(1, CHUNKS))
    tri_ref[...] = earlier(n_tok)
    for ref in (dw0_ref, dw1_ref, dwt_ref, dy_y_ref, dx_ref):
        ref[...] = jnp.zeros_like(ref)

    def events(k):
        if k == 0:
            pass_w(1, 1, 0)
            pass_w(2, 1, 0)
            tokens(1)
            pass_w(2, 2, 0)
            batch(1, 1)
            relay(0)
        elif k == 1:
            tokens(2)
            batch(1, 2)
            need_w(0)
            own_w((2,), (1,))
        elif k == 2:
            pass_w(2, 1, 1)
            pass_w(2, 2, 1)
            batch(1, 3)
            relay(1)
            tokens(3)
        elif k == 3:
            batch(2, 2)
            batch(1, 4)
            need_w(1)
        elif k == 4:
            batch(2, 3)
            batch(1, 5)
            batch(1, 6)
            relay(2)
        elif k == 5:
            batch(2, 4)
            need_w(2)
        elif k == 6:
            batch(2, 5)
            need_w(3)
        elif k == 7:
            batch(2, 6)
            relay(3)
        else:
            need_w(k - 4)

    def rows_of(s):
        return lax.div(s, per_h), pl.ds(pl.multiple_of(lax.rem(s, per_h) * cap, cap), cap)

    def compact(o, j):
        def one(s, carry):
            meta = meta_all[j, s]
            pos = pick_row(positions(meta, tri_ref[...], cap), e_mine)
            hit = iota_f32((cap, n_tok), 0) == pos
            r_row = (jnp.where(meta[0:1, :] == e_mine, meta[2:3, :], 0.0)
                     + jnp.where(meta[1:2, :] == e_mine, meta[3:4, :], 0.0))
            r_col = jnp.sum(jnp.where(hit, r_row, 0.0), axis=1, keepdims=True)
            got = dot_nn(jnp.where(hit, 1.0, 0.0).astype(BF16), xd_all[j, s])
            h, rows = rows_of(s)
            dy = got[:, d:]
            xc_ref[o * n_h + h, rows, :] = got[:, :d].astype(BF16)
            gc_ref[o * n_h + h, rows, :] = (r_col * dy).astype(BF16)

            @pl.when(o == 0)
            def _():
                dyc_ref[h, rows, :] = dy.astype(BF16)

            return carry

        lax.fori_loop(0, n_p, one, 0)

        def turn(h, carry):
            xt_ref[o * n_h + h] = xc_ref[o * n_h + h, :, own_rows].T
            gt_ref[o * n_h + h] = gc_ref[o * n_h + h, :, own_rows].T
            return carry

        lax.fori_loop(0, n_h, turn, 0)

    def cells(o, c, own):
        cols = pl.ds(pl.multiple_of(c * fc, fc), fc)
        w1, w3, w2 = w_all[0, :, cols], w_all[1, :, cols], w_all[2, :, cols]
        rows = xc_ref.shape[1]
        size = rows // SUB
        subs = [(h, slice(n * size, (n + 1) * size)) for h in range(n_h) for n in range(SUB)]
        sums = [None] * 3
        held = []

        def behind(n):
            h, at = subs[n]
            a, dh1, dh3 = held[n]
            i = o * n_h + h
            for m, (left, right) in enumerate(((xt_ref, dh1), (xt_ref, dh3), (gt_ref, a))):
                term = dot_nn(left[i, :, at], right)
                sums[m] = term if sums[m] is None else sums[m] + term
            if own:
                grown = dyc_ref[h, at, :].astype(F32) * dot_nt(a, w2)
                wide = dy_y_ref.shape[2]
                dy_y_ref[h, at, :] += sum(grown[:, m:m + wide] for m in range(0, d, wide))
                dx_ref[h, at, :] += dot_nt(dh1, w1) + dot_nt(dh3, w3)

        for n, (h, at) in enumerate(subs):
            i = o * n_h + h
            h1 = dot_nn(xc_ref[i, at, :], w1)
            h3 = dot_nn(xc_ref[i, at, :], w3)
            da = dot_nn(gc_ref[i, at, :], w2)
            s = jax.nn.sigmoid(h1)
            a = (h1 * s * h3).astype(BF16)
            t = da * s
            dh3 = (t * h1).astype(BF16)
            dh1 = (t * h3 * (1.0 + h1 * (1.0 - s))).astype(BF16)
            held.append((a, dh1, dh3))
            if n:
                behind(n - 1)
        behind(len(subs) - 1)
        for ref, total in zip((dw0_ref, dw1_ref, dwt_ref), sums):
            ref[:, cols] += total

    def send_back():
        def leave(n):
            to = flip(p, pick(RETURN, n))

            @pl.when(to != p)
            def _():
                start_all(back_copy(to))

            @pl.when(to == p)
            def _():
                start_all(own_back())

        def one(n, carry):
            s = flip(p, pick(RETURN, n))
            h, rows = rows_of(s)
            dxs_ref[s] = dx_ref[h, rows, :].astype(BF16)
            dr_col = jnp.sum(dy_y_ref[h, rows, :], axis=1, keepdims=True)
            pos = pick_row(positions(meta_all[z, s], tri_ref[...], cap), e_mine)
            hit = iota_f32((cap, n_tok), 0) == pos
            dr_row = jnp.sum(jnp.where(hit, dr_col, 0.0), axis=0, keepdims=True)
            drs_ref[s] = jnp.broadcast_to(dr_row, (8, n_tok))

            @pl.when(n > 0)
            def _():
                leave(n - 1)

            return carry

        lax.fori_loop(0, n_p, one, 0)
        leave(n_p - 1)

    def back_copy(to):
        return (remote(drs_ref.at[to], drr_ref.at[p], s_dr.at[to], r_dr.at[p], {"ep": to}),
                remote(dxs_ref.at[to], dxr_ref.at[p], s_dx.at[to], r_dx.at[p], {"ep": to}))

    def own_back():
        return (pltpu.make_async_copy(drs_ref.at[p], drr_ref.at[p], s_dr.at[p]),
                pltpu.make_async_copy(dxs_ref.at[p], dxr_ref.at[p], s_dx.at[p]))

    n_steps = len(STEPS)

    def step(k, carry):
        for n in range(n_steps):
            @pl.when(k == n)
            def _():
                with jax.named_scope(f"events_{n}"):
                    events(n)

        packed = pick([t[0] for t in STEPS], k)

        @pl.when(packed >= 0)
        def _():
            j = plane_of(packed)
            with jax.named_scope("landed"):
                landed(j)
            with jax.named_scope("compact"):
                compact(packed, j)

        def chunk_own(c, carry):
            with jax.named_scope("cells_own"):
                cells(0, c, True)
            return carry

        lax.fori_loop(pick([t[1][0] for t in STEPS], k), pick([t[1][1] for t in STEPS], k), chunk_own, 0)

        @pl.when(k == n_steps - 1)
        def _():
            with jax.named_scope("send_back"):
                send_back()

        def plane(o, carry):
            def chunk(c, carry):
                with jax.named_scope("cells"):
                    cells(o, c, False)
                return carry

            lo = sum(jnp.where(o == n, pick([t[1 + n][0] for t in STEPS], k), 0) for n in range(1, n_z))
            hi = sum(jnp.where(o == n, pick([t[1 + n][1] for t in STEPS], k), 0) for n in range(1, n_z))
            return lax.fori_loop(lo, hi, chunk, carry)

        return lax.fori_loop(1, n_z, plane, carry)

    lax.fori_loop(0, n_steps, step, 0)

    stores = [pltpu.make_async_copy(dw0_ref, dw0_out, s_loc.at[0]),
              pltpu.make_async_copy(dw1_ref, dw1_out, s_loc.at[1]),
              pltpu.make_async_copy(dw2_ref, dw2_out, s_loc.at[2])]
    for c in range(CHUNKS):
        dw2_ref[c * fc:(c + 1) * fc, :] = dwt_ref[:, c * fc:(c + 1) * fc].T
    for c in stores:
        c.start()
    with jax.named_scope("back_wait"):
        for q in range(1, n_p):
            frm = flip(p, q)
            remote(drs_ref.at[frm], drr_ref.at[frm], s_dr.at[frm], r_dr.at[frm], {"ep": frm}).wait_recv()
            remote(dxs_ref.at[frm], dxr_ref.at[frm], s_dx.at[frm], r_dx.at[frm], {"ep": frm}).wait_recv()
        for c in own_back():
            c.wait()
    for c in stores:
        c.wait()

    with jax.named_scope("drain"):
        for q in range(1, n_p):
            for c in back_copy(flip(p, q)):
                c.wait_send()
        for i in range(4):
            for j in range(n_z):
                for c in plane_copy(j, i):
                    c.wait_send()
        for i in range(3):
            for j in range(n_z):
                for c in relay_copy(j, i):
                    c.wait_send()
        for way in (0, 1):
            there, _ = link(way)
            for dist in range(n_z):
                j = upstream(way, dist)

                @pl.when(valid_z(j) & there)
                def _():
                    for c in zt_copy(j, way):
                        c.wait_send()

                    def drain(c, carry):
                        w_copy(j, c, way).wait_send()
                        return carry

                    lax.fori_loop(0, CHUNKS, drain, 0)


def finish(cap, n_p, ids_ref, dxr_hbm, drr_hbm, dw0_in, dw1_in, dw2_in,
           gx_ref, dr_ref, dw0_out, dw1_out, dw2_out,
           dxr_ref, drr_ref, dw0_ref, dw1_ref, dw2_ref, gxa_ref, s_in, s_out):
    n_tok = ids_ref.shape[1]
    rows_in = (pltpu.make_async_copy(dxr_hbm, dxr_ref, s_in.at[0]),
               pltpu.make_async_copy(drr_hbm, drr_ref, s_in.at[1]))
    moves = tuple(
        (pltpu.make_async_copy(src, mid, s_in.at[2 + n]), pltpu.make_async_copy(mid, dst, s_out.at[n]))
        for n, (src, mid, dst) in enumerate(
            ((dw0_in, dw0_ref, dw0_out), (dw1_in, dw1_ref, dw1_out), (dw2_in, dw2_ref, dw2_out))))
    for c in rows_in:
        c.start()
    for c, _ in moves:
        c.start()
    ids = ids_ref[...].astype(F32)
    pos16 = positions(ids, earlier(n_tok), cap)
    gxa_ref[...] = jnp.zeros_like(gxa_ref)
    dr_ref[...] = jnp.zeros_like(dr_ref)
    for c in rows_in:
        c.wait()
    for c_in, c_out in moves:
        c_in.wait()
        c_out.start()

    def gather(e, carry):
        ef = e.astype(F32)
        pos = pick_row(pos16, ef)
        hit = jnp.where(iota_f32((cap, n_tok), 0) == pos, 1.0, 0.0).astype(BF16)
        gxa_ref[...] += dot_tn(hit, dxr_ref[e])
        dr = drr_ref[e]
        dr_ref[...] += jnp.where(ids == ef, dr[0:1, :], 0.0)
        return carry

    lax.fori_loop(0, n_p, gather, 0)
    gx_ref[...] = gxa_ref[...].astype(BF16)
    for _, c in moves:
        c.wait()


def solution(mesh):
    n_z, n_p = mesh.shape["fsdp"], mesh.shape["ep"]
    tok_spec = P(("fsdp", "ep"), None)
    spec_in = P("ep", "fsdp", None)
    spec_out = P("ep", None, "fsdp")

    def per_device(x_tok, dy_tok, expert_ids, route_w, w_gate, w_up, w_down):
        n_tok, top_k = expert_ids.shape
        d = x_tok.shape[1]
        dl, f = w_gate.shape[1], w_gate.shape[2]
        cap = capacity_of(n_tok, top_k, n_p)
        rows = 4 * cap
        n_t = n_z * n_p // 4
        sem = pltpu.SemaphoreType.DMA
        vmem = pl.BlockSpec(memory_space=pltpu.VMEM)
        hbm = pl.BlockSpec(memory_space=pl.ANY)
        out = jax.ShapeDtypeStruct
        ids, rw = expert_ids.T, route_w.T
        dw_shapes = (out((dl, f), F32), out((dl, f), F32), out((f, dl), F32))
        back = pl.pallas_call(
            functools.partial(kernel, cap, n_z, n_p),
            out_shape=(out((n_p, cap, d), BF16), out((n_p, 8, n_tok), F32)) + dw_shapes,
            in_specs=[vmem] * 2 + [hbm] * 5,
            out_specs=(hbm,) * 5,
            scratch_shapes=[
                pltpu.VMEM((n_z, n_p, n_tok, 2 * d), BF16),
                pltpu.VMEM((n_z, n_p, 8, n_tok), F32),
                pltpu.VMEM((3, n_z * dl, f), BF16),
                pltpu.VMEM((n_tok, n_tok), BF16),
                pltpu.VMEM((n_t, rows, d), BF16),
                pltpu.VMEM((n_t, rows, d), BF16),
                pltpu.VMEM((n_p // 4, rows, d), BF16),
                pltpu.VMEM((n_t, dl, rows), BF16),
                pltpu.VMEM((n_t, dl, rows), BF16),
                pltpu.VMEM((n_p // 4, rows, min(128, d)), F32),
                pltpu.VMEM((n_p // 4, rows, d), F32),
                pltpu.VMEM((n_p, cap, d), BF16),
                pltpu.VMEM((n_p, 8, n_tok), F32),
                pltpu.VMEM((dl, f), F32),
                pltpu.VMEM((dl, f), F32),
                pltpu.VMEM((dl, f), F32),
                pltpu.VMEM((f, dl), F32),
                pltpu.VMEM((f, dl), BF16),
                sem((2, n_z)), sem((n_z,)), sem((2, n_z)), sem((n_z,)),
                sem((2, n_z, CHUNKS)), sem((n_z, CHUNKS)),
                sem((n_z, 4)), sem((n_z, n_p)), sem((n_z, 4)), sem((n_z, n_p)),
                sem((n_z, 3)), sem((n_z, 3)),
                sem((n_p,)), sem((n_p,)), sem((n_p,)), sem((n_p,)),
                sem((5,)),
            ],
            compiler_params=pltpu.CompilerParams(
                collective_id=0, has_side_effects=True, vmem_limit_bytes=67043328),
        )(ids, rw, x_tok, dy_tok, w_gate, w_up, w_down)
        gx, dr, dw0, dw1, dw2 = pl.pallas_call(
            functools.partial(finish, cap, n_p),
            out_shape=(out((n_tok, d), BF16), out((top_k, n_tok), F32)) + dw_shapes,
            in_specs=[vmem] + [hbm] * 5,
            out_specs=(vmem,) * 2 + (hbm,) * 3,
            scratch_shapes=[
                pltpu.VMEM((n_p, cap, d), BF16),
                pltpu.VMEM((n_p, 8, n_tok), F32),
                pltpu.VMEM((dl, f), F32),
                pltpu.VMEM((dl, f), F32),
                pltpu.VMEM((f, dl), F32),
                pltpu.VMEM((n_tok, d), F32),
                sem((5,)), sem((3,)),
            ],
        )(ids, *back)
        return gx, dr.T, dw0[None], dw1[None], dw2[None]

    return jax.shard_map(
        per_device, mesh=mesh,
        in_specs=(tok_spec, tok_spec, tok_spec, tok_spec, spec_in, spec_in, spec_out),
        out_specs=(tok_spec, tok_spec, spec_in, spec_in, spec_out),
        check_vma=False)
```

```python
import functools

import jax
import jax.numpy as jnp
from jax import lax
from jax.experimental import pallas as pl
from jax.experimental.pallas import tpu as pltpu
from jax.sharding import PartitionSpec as P

MESH = pl.DeviceIdType.MESH
CAP_FACTOR = 3
CHUNKS = 7
F32 = jnp.float32
BF16 = jnp.bfloat16
DIAG = (2, 4, 6)
DIRECT = (1, 2, 4, 6)
SUB = 3
RETURN = (6, 4, 7, 5, 2, 3, 1, 0)
ORDER = ((0, 1, 2, 3), (1, 0, 2, 3), (2, 3, 1, 0), (3, 2, 1, 0))
NONE = (0, 0)
END_STEPS = (
    (0, NONE, NONE, NONE, NONE),
    (-1, (0, 1), NONE, NONE, NONE),
    (1, NONE, (0, 1), NONE, NONE),
    (-1, (1, 2), (1, 2), NONE, NONE),
    (2, NONE, NONE, (0, 2), NONE),
    (-1, (2, 3), (2, 3), (2, 3), NONE),
    (-1, (3, 4), (3, 4), (3, 4), NONE),
    (3, NONE, NONE, NONE, (0, 4)),
    (-1, (4, 5), (4, 5), (4, 5), (4, 5)),
    (-1, (5, 6), (5, 6), (5, 6), (5, 6)),
    (-1, (6, 7), (6, 7), (6, 7), (6, 7)),
)
MID_STEPS = (
    (0, (0, 1), NONE, NONE, NONE),
    (-1, (1, 2), NONE, NONE, NONE),
    (1, (2, 3), (0, 1), NONE, NONE),
    (-1, (3, 4), (1, 4), NONE, NONE),
    (-1, (4, 5), (4, 5), NONE, NONE),
    (-1, (5, 6), (5, 6), NONE, NONE),
    (-1, (6, 7), (6, 7), NONE, NONE),
    (2, NONE, NONE, (0, 7), NONE),
    (3, NONE, NONE, NONE, NONE),
    (-1, NONE, NONE, NONE, (0, 7)),
    (-1, NONE, NONE, NONE, NONE),
)
SEND_STEP = 6
GATHER_STEP = 9


def capacity_of(tok_dev, top_k, experts):
    return max(8, ((CAP_FACTOR * tok_dev * top_k // experts + 7) // 8) * 8)


def flip(p, q):
    for b in (1, 2, 4):
        turned = b - 2 * b * lax.rem(lax.div(p, b), 2)
        if isinstance(q, int):
            p = p + turned if q & b else p
        else:
            p = p + lax.rem(lax.div(q, b), 2) * turned
    return p


def dot_nn(a, b):
    return jnp.dot(a, b, preferred_element_type=F32)


def dot_nt(a, b):
    return lax.dot_general(a, b, (((1,), (1,)), ((), ())), preferred_element_type=F32)


def dot_tn(a, b):
    return lax.dot_general(a, b, (((0,), (0,)), ((), ())), preferred_element_type=F32)


def iota_f32(shape, dim):
    return lax.broadcasted_iota(jnp.int32, shape, dim).astype(F32)


def earlier(n):
    return jnp.where(iota_f32((n, n), 0) < iota_f32((n, n), 1), 1.0, 0.0).astype(BF16)


def positions(meta, tri, cap):
    ids0, ids1 = meta[0:1, :], meta[1:2, :]
    row = iota_f32((16, meta.shape[1]), 0)
    chosen = jnp.where(ids0 == row, 1.0, 0.0) + jnp.where(ids1 == row, 1.0, 0.0)
    before = dot_nn(chosen.astype(BF16), tri)
    return jnp.where((chosen > 0.0) & (before < cap), before, -1.0)


def pick_row(pos16, e):
    row = iota_f32(pos16.shape, 0)
    return jnp.sum(jnp.where(row == e, pos16, 0.0), axis=0, keepdims=True)


def pick(table, i):
    return sum(jnp.where(i == n, v, 0) for n, v in enumerate(table))


def kernel(cap, n_z, n_p, ids_ref, rw_ref, x_ref, dy_ref, wg_ref, wu_ref, wd_ref,
           gx_out, dr_out, dw0_out, dw1_out, dw2_out,
           xd_all, meta_all, w_all, tri_ref, xc_ref, gc_ref, dyc_ref, xt_ref, gt_ref, dy_y_ref, dx_ref,
           dxs_ref, drs_ref, dxr_ref, drr_ref, gxa_ref, gx_ref, dr_ref,
           dw0_ref, dw1_ref, dwt_ref, dw2_ref, wd_own,
           s_zt, r_zt, s_zm, r_zm, s_w, r_w, s_p, r_p, s_pm, r_pm, s_r, s_rm,
           s_dx, r_dx, s_dr, r_dr, s_gx, r_gx, s_loc):
    z = lax.axis_index("fsdp")
    p = lax.axis_index("ep")
    e_mine = p.astype(F32)
    n_tok, d = x_ref.shape
    dl, f = wg_ref.shape[1:]
    fc = f // CHUNKS
    per_h = 4
    n_h = n_p // per_h
    partner = flip(p, 1)
    mid = (z > 0) & (z < n_z - 1)
    own_rows = pl.ds(pl.multiple_of(z * dl, dl), dl)

    def plane_of(o):
        if isinstance(o, int):
            return pick([t[o] for t in ORDER], z)
        return sum(jnp.where(z == n, pick(t, o), 0) for n, t in enumerate(ORDER))

    barrier = pltpu.get_barrier_semaphore()
    for q in range(1, n_p):
        pl.semaphore_signal(barrier, inc=1, device_id={"ep": flip(p, q)}, device_id_type=MESH)
    for step in (1, -1):
        nb = z + step

        @pl.when((nb >= 0) & (nb < n_z))
        def _():
            pl.semaphore_signal(barrier, inc=1, device_id={"fsdp": nb}, device_id_type=MESH)

    load_wd = pltpu.make_async_copy(wd_ref.at[0], wd_own, s_loc.at[4])
    loads = (
        pltpu.make_async_copy(wg_ref.at[0], w_all.at[0, own_rows, :], s_loc.at[2]),
        pltpu.make_async_copy(wu_ref.at[0], w_all.at[1, own_rows, :], s_loc.at[3]),
        pltpu.make_async_copy(x_ref, xd_all.at[z, p, :, pl.ds(0, d)], s_loc.at[0]),
        pltpu.make_async_copy(dy_ref, xd_all.at[z, p, :, pl.ds(d, d)], s_loc.at[1]),
    )
    load_wd.start()
    for c in loads:
        c.start()
    meta_all[z, p, 0:2, :] = ids_ref[...].astype(F32)
    meta_all[z, p, 2:4, :] = rw_ref[...]
    meta_all[z, p, 4:8, :] = jnp.zeros((4, n_tok), F32)
    load_wd.wait()
    for c in range(CHUNKS):
        w_all[2, own_rows, c * fc:(c + 1) * fc] = wd_own[c * fc:(c + 1) * fc, :].T
    for c in loads:
        c.wait()
    inner = jnp.where(z > 0, 1, 0) + jnp.where(z < n_z - 1, 1, 0)
    pl.semaphore_wait(barrier, n_p - 1 + inner)

    def remote(src, dst, ssem, rsem, dev):
        return pltpu.make_async_remote_copy(
            src_ref=src, dst_ref=dst, send_sem=ssem, recv_sem=rsem, device_id=dev, device_id_type=MESH)

    def w_block(j, c):
        return w_all.at[:, pl.ds(pl.multiple_of(j * dl, dl), dl), pl.ds(pl.multiple_of(c * fc, fc), fc)]

    def zt_copy(j, way):
        dev = {"fsdp": z + 1 - 2 * way}
        return (remote(meta_all.at[j, p], meta_all.at[j, p], s_zm.at[way, j], r_zm.at[j], dev),
                remote(xd_all.at[j, p], xd_all.at[j, p], s_zt.at[way, j], r_zt.at[j], dev))

    def w_copy(j, c, way):
        return remote(w_block(j, c), w_block(j, c), s_w.at[way, j, c], r_w.at[j, c], {"fsdp": z + 1 - 2 * way})

    def plane_copy(j, i):
        dev = {"ep": flip(p, DIRECT[i])}
        return (remote(meta_all.at[j, p], meta_all.at[j, p], s_pm.at[j, i], r_pm.at[j, p], dev),
                remote(xd_all.at[j, p], xd_all.at[j, p], s_p.at[j, i], r_p.at[j, p], dev))

    def relay_copy(j, i):
        pp = flip(p, DIAG[i])
        dev = {"ep": partner}
        return (remote(meta_all.at[j, pp], meta_all.at[j, pp], s_rm.at[j, i], r_pm.at[j, pp], dev),
                remote(xd_all.at[j, pp], xd_all.at[j, pp], s_r.at[j, i], r_p.at[j, pp], dev))

    def plane_wait(j, pp):
        remote(meta_all.at[j, pp], meta_all.at[j, pp], s_pm.at[j, 0], r_pm.at[j, pp], {"ep": partner}).wait_recv()
        remote(xd_all.at[j, pp], xd_all.at[j, pp], s_p.at[j, 0], r_p.at[j, pp], {"ep": partner}).wait_recv()

    def valid_z(j):
        return (j >= 0) & (j < n_z)

    def start_all(copies):
        for c in copies:
            c.start()

    def link(way):
        return valid_z(z + 1 - 2 * way), (z if way == 0 else n_z - 1 - z)

    def upstream(way, dist):
        return z - dist * (1 - 2 * way)

    def own_w(depths, chunks):
        for way in (0, 1):
            there, depth = link(way)
            for q in depths:
                @pl.when(there & (depth == q))
                def _():
                    for c in chunks:
                        w_copy(z, c, way).start()

    def pass_w(q, dist, c):
        for way in (0, 1):
            there, depth = link(way)

            @pl.when(there & (depth == q))
            def _():
                j = upstream(way, dist)
                w_copy(j, c, way).wait_recv()
                w_copy(j, c, way).start()

    def need_w(c):
        for way in (0, 1):
            there, _ = link(way)
            for dist in range(1, n_z):
                j = upstream(way, dist)

                @pl.when(jnp.logical_not(there) & valid_z(j))
                def _():
                    w_copy(j, c, way).wait_recv()

    def tokens(dist):
        for way, turn in ((0, z < 2), (1, z >= 0), (0, z >= 2)):
            there, _ = link(way)
            j = upstream(way, dist)

            @pl.when(turn & valid_z(j))
            def _():
                for c in zt_copy(j, way):
                    c.wait_recv()

                @pl.when(there)
                def _():
                    start_all(zt_copy(j, way))

                for i in range(4):
                    start_all(plane_copy(j, i))

    def relay(o):
        j = plane_of(o)
        for i, q in enumerate(DIAG):
            plane_wait(j, flip(p, q))
            start_all(relay_copy(j, i))

    def landed(j):
        plane_wait(j, partner)
        for q in DIAG:
            plane_wait(j, flip(partner, q))

    def batch(q, c):
        own_w((q,), (c,))
        for dist in range(1, q + 1):
            pass_w(q, dist, c)

    own_w((0, 1, 2), (0,))
    for way in (0, 1):
        there, _ = link(way)

        @pl.when(there)
        def _():
            start_all(zt_copy(z, way))
    for i in range(4):
        start_all(plane_copy(z, i))
    own_w((0,), range(1, CHUNKS))
    tri_ref[...] = earlier(n_tok)
    for ref in (dw0_ref, dw1_ref, dwt_ref, dy_y_ref, dx_ref):
        ref[...] = jnp.zeros_like(ref)

    def end_events(k):
        if k == 0:
            tokens(1)
            relay(0)
        elif k == 1:
            tokens(2)
            need_w(0)
        elif k == 2:
            relay(1)
            tokens(3)
        elif k == 3:
            need_w(1)
        elif k == 4:
            relay(2)
        elif k in (5, 6):
            need_w(k - 3)
        elif k == 7:
            relay(3)
        else:
            need_w(k - 4)

    def mid_events(k):
        if k == 0:
            pass_w(1, 1, 0)
            pass_w(2, 1, 0)
            tokens(1)
            pass_w(2, 2, 0)
            batch(1, 1)
            relay(0)
        elif k == 1:
            tokens(2)
            batch(1, 2)
            batch(2, 1)
        elif k == 2:
            batch(1, 3)
            relay(1)
            batch(2, 2)
        elif k == 3:
            batch(2, 3)
            batch(1, 4)
            batch(1, 5)
            batch(1, 6)
        elif k == 4:
            relay(2)
            batch(2, 4)
        elif k in (5, 6):
            batch(2, k)
        elif k == 7:
            relay(3)

    def rows_of(s):
        return lax.div(s, per_h), pl.ds(pl.multiple_of(lax.rem(s, per_h) * cap, cap), cap)

    def compact(o, j, keep_dy):
        def one(s, carry):
            meta = meta_all[j, s]
            pos = pick_row(positions(meta, tri_ref[...], cap), e_mine)
            hit = iota_f32((cap, n_tok), 0) == pos
            r_row = (jnp.where(meta[0:1, :] == e_mine, meta[2:3, :], 0.0)
                     + jnp.where(meta[1:2, :] == e_mine, meta[3:4, :], 0.0))
            r_col = jnp.sum(jnp.where(hit, r_row, 0.0), axis=1, keepdims=True)
            got = dot_nn(jnp.where(hit, 1.0, 0.0).astype(BF16), xd_all[j, s])
            h, rows = rows_of(s)
            dy = got[:, d:]
            xc_ref[o * n_h + h, rows, :] = got[:, :d].astype(BF16)
            gc_ref[o * n_h + h, rows, :] = (r_col * dy).astype(BF16)

            if keep_dy:
                dyc_ref[o, h, rows, :] = dy.astype(BF16)
            return carry

        lax.fori_loop(0, n_p, one, 0, unroll=2)

        def turn(h, carry):
            xt_ref[o * n_h + h] = xc_ref[o * n_h + h, :, own_rows].T
            gt_ref[o * n_h + h] = gc_ref[o * n_h + h, :, own_rows].T
            return carry

        lax.fori_loop(0, n_h, turn, 0)

    def cells(o, c, own):
        cols = pl.ds(pl.multiple_of(c * fc, fc), fc)
        w1, w3, w2 = w_all[0, :, cols], w_all[1, :, cols], w_all[2, :, cols]
        rows = xc_ref.shape[1]
        size = rows // SUB
        subs = [(h, slice(n * size, (n + 1) * size)) for h in range(n_h) for n in range(SUB)]
        sums = [None] * 3
        held = []

        def behind(n):
            h, at = subs[n]
            a, dh1, dh3 = held[n]
            i = o * n_h + h
            for m, (left, right) in enumerate(((xt_ref, dh1), (xt_ref, dh3), (gt_ref, a))):
                term = dot_nn(left[i, :, at], right)
                sums[m] = term if sums[m] is None else sums[m] + term
            if own:
                grown = dyc_ref[o, h, at, :].astype(F32) * dot_nt(a, w2)
                wide = dy_y_ref.shape[-1]
                dy_y_ref[o, h, at, :] += sum(grown[:, m:m + wide] for m in range(0, d, wide))
                dx_ref[o, h, at, :] += dot_nt(dh1, w1) + dot_nt(dh3, w3)

        for n, (h, at) in enumerate(subs):
            i = o * n_h + h
            h1 = dot_nn(xc_ref[i, at, :], w1)
            h3 = dot_nn(xc_ref[i, at, :], w3)
            da = dot_nn(gc_ref[i, at, :], w2)
            s = jax.nn.sigmoid(h1)
            a = (h1 * s * h3).astype(BF16)
            t = da * s
            dh3 = (t * h1).astype(BF16)
            dh1 = (t * h3 * (1.0 + h1 * (1.0 - s))).astype(BF16)
            held.append((a, dh1, dh3))
            if n:
                behind(n - 1)
        behind(len(subs) - 1)
        for ref, total in zip((dw0_ref, dw1_ref, dwt_ref), sums):
            ref[:, cols] += total

    def send_back(o):
        j = plane_of(o)

        def leave(n):
            to = flip(p, pick(RETURN, n))

            @pl.when(to != p)
            def _():
                start_all(back_copy(o, to))

            @pl.when(to == p)
            def _():
                start_all(own_back(o))

        def one(n, carry):
            s = flip(p, pick(RETURN, n))
            h, rows = rows_of(s)
            dxs_ref[o, s] = dx_ref[o, h, rows, :].astype(BF16)
            dr_col = jnp.sum(dy_y_ref[o, h, rows, :], axis=1, keepdims=True)
            pos = pick_row(positions(meta_all[j, s], tri_ref[...], cap), e_mine)
            hit = iota_f32((cap, n_tok), 0) == pos
            dr_row = jnp.sum(jnp.where(hit, dr_col, 0.0), axis=0, keepdims=True)
            drs_ref[o, s] = jnp.broadcast_to(dr_row, (8, n_tok))

            @pl.when(n > 0)
            def _():
                leave(n - 1)

            return carry

        lax.fori_loop(0, n_p, one, 0)
        leave(n_p - 1)

    def back_copy(o, to):
        return (remote(drs_ref.at[o, to], drr_ref.at[o, p], s_dr.at[o, to], r_dr.at[o, p], {"ep": to}),
                remote(dxs_ref.at[o, to], dxr_ref.at[o, p], s_dx.at[o, to], r_dx.at[o, p], {"ep": to}))

    def own_back(o):
        return (pltpu.make_async_copy(drs_ref.at[o, p], drr_ref.at[o, p], s_dr.at[o, p]),
                pltpu.make_async_copy(dxs_ref.at[o, p], dxr_ref.at[o, p], s_dx.at[o, p]))

    def gather(o):
        meta = meta_all[plane_of(o), p]
        pos16 = positions(meta, tri_ref[...], cap)
        gxa_ref[...] = jnp.zeros_like(gxa_ref)
        dr_ref[o] = jnp.zeros_like(dr_ref[o])

        def one(n, carry):
            e = flip(p, pick(RETURN, n))

            @pl.when(e != p)
            def _():
                remote(drs_ref.at[o, e], drr_ref.at[o, e], s_dr.at[o, e], r_dr.at[o, e], {"ep": e}).wait_recv()
                remote(dxs_ref.at[o, e], dxr_ref.at[o, e], s_dx.at[o, e], r_dx.at[o, e], {"ep": e}).wait_recv()

            @pl.when(e == p)
            def _():
                for c in own_back(o):
                    c.wait()

            ef = e.astype(F32)
            pos = pick_row(pos16, ef)
            hit = jnp.where(iota_f32((cap, n_tok), 0) == pos, 1.0, 0.0).astype(BF16)
            gxa_ref[...] += dot_tn(hit, dxr_ref[o, e])
            dr = drr_ref[o, e]
            dr_ref[o] += jnp.where(meta == ef, dr[0:1, :], 0.0)
            return carry

        lax.fori_loop(0, n_p, one, 0)
        gx_ref[o] = gxa_ref[...].astype(BF16)

    def sums_out(way):
        dev = {"fsdp": z + 1 - 2 * way}
        return (remote(dr_ref.at[1], dr_out, s_gx.at[0], r_gx.at[0], dev),
                remote(gx_ref.at[1], gx_out, s_gx.at[1], r_gx.at[1], dev))

    n_steps = len(END_STEPS)

    def chosen(of, k):
        return jnp.where(mid, pick([of(t) for t in MID_STEPS], k), pick([of(t) for t in END_STEPS], k))

    def step(k, carry):
        for n in range(n_steps):
            @pl.when((k == n) & mid)
            def _():
                with jax.named_scope(f"mid_{n}"):
                    mid_events(n)

            @pl.when((k == n) & jnp.logical_not(mid))
            def _():
                with jax.named_scope(f"end_{n}"):
                    end_events(n)

        packed = chosen(lambda t: t[0], k)

        @pl.when(packed >= 0)
        def _():
            j = plane_of(packed)
            with jax.named_scope("landed"):
                landed(j)

            @pl.when(mid & (packed < 2))
            def _():
                with jax.named_scope("compact"):
                    compact(packed, j, True)

            @pl.when(jnp.logical_not(mid & (packed < 2)))
            def _():
                with jax.named_scope("compact"):
                    compact(packed, j, False)

        @pl.when(mid & (k == GATHER_STEP))
        def _():
            with jax.named_scope("gather"):
                gather(1)
            for way in (0, 1):
                @pl.when((z == 2) if way == 0 else (z == 1))
                def _():
                    start_all(sums_out(way))

        def dx_plane(m, carry):
            o = 1 - m

            def chunk(c, carry):
                with jax.named_scope("cells_own"):
                    cells(o, c, True)
                return carry

            lo = pick([chosen(lambda t, n=n: t[1 + n][0], k) for n in range(2)], o)
            hi = pick([chosen(lambda t, n=n: t[1 + n][1], k) for n in range(2)], o)
            lax.fori_loop(lo, hi, chunk, 0)

            @pl.when(k == SEND_STEP)
            def _():
                with jax.named_scope("send_back"):
                    send_back(o)

            return carry

        lax.fori_loop(0, jnp.where(mid, 2, 0), dx_plane, 0)

        def plane(o, carry):
            def chunk(c, carry):
                with jax.named_scope("cells"):
                    cells(o, c, False)
                return carry

            lo = pick([chosen(lambda t, n=n: t[1 + n][0], k) for n in range(n_z)], o)
            hi = pick([chosen(lambda t, n=n: t[1 + n][1], k) for n in range(n_z)], o)
            return lax.fori_loop(lo, hi, chunk, carry)

        return lax.fori_loop(jnp.where(mid, 2, 0), n_z, plane, carry)

    lax.fori_loop(0, n_steps, step, 0)

    stores = [pltpu.make_async_copy(dw0_ref, dw0_out, s_loc.at[0]),
              pltpu.make_async_copy(dw1_ref, dw1_out, s_loc.at[1]),
              pltpu.make_async_copy(dw2_ref, dw2_out, s_loc.at[2])]
    for c in range(CHUNKS):
        dw2_ref[c * fc:(c + 1) * fc, :] = dwt_ref[:, c * fc:(c + 1) * fc].T
    for c in stores:
        c.start()

    @pl.when(mid)
    def _():
        with jax.named_scope("gather"):
            gather(0)
        own_sums = (pltpu.make_async_copy(gx_ref.at[0], gx_out, s_loc.at[3]),
                    pltpu.make_async_copy(dr_ref.at[0], dr_out, s_loc.at[4]))
        start_all(own_sums)
        for c in own_sums:
            c.wait()
        for way in (0, 1):
            @pl.when((z == 2) if way == 0 else (z == 1))
            def _():
                for c in sums_out(way):
                    c.wait_send()

    @pl.when(jnp.logical_not(mid))
    def _():
        with jax.named_scope("sums_wait"):
            for c in sums_out(0):
                c.wait_recv()

    for c in stores:
        c.wait()

    with jax.named_scope("drain"):
        @pl.when(mid)
        def _():
            for o in range(2):
                for q in range(1, n_p):
                    for c in back_copy(o, flip(p, q)):
                        c.wait_send()

        for i in range(4):
            for j in range(n_z):
                for c in plane_copy(j, i):
                    c.wait_send()
        for i in range(3):
            for j in range(n_z):
                for c in relay_copy(j, i):
                    c.wait_send()
        for way in (0, 1):
            there, _ = link(way)
            for dist in range(n_z):
                j = upstream(way, dist)

                @pl.when(valid_z(j) & there)
                def _():
                    for c in zt_copy(j, way):
                        c.wait_send()

                    def drain(c, carry):
                        w_copy(j, c, way).wait_send()
                        return carry

                    lax.fori_loop(0, CHUNKS, drain, 0)


def finish(gx_in, dr_ref, dw0_in, dw1_in, dw2_in, gx_out, drt_ref, dw0_out, dw1_out, dw2_out,
           gx_ref, dw0_ref, dw1_ref, dw2_ref, s_in, s_out):
    moves = tuple(
        (pltpu.make_async_copy(src, mid, s_in.at[n]), pltpu.make_async_copy(mid, dst, s_out.at[n]))
        for n, (src, mid, dst) in enumerate(
            ((gx_in, gx_ref, gx_out), (dw0_in, dw0_ref, dw0_out), (dw1_in, dw1_ref, dw1_out),
             (dw2_in, dw2_ref, dw2_out))))
    for c, _ in moves:
        c.start()
    drt_ref[0:1, :] = dr_ref[0:1, :]
    drt_ref[1:2, :] = dr_ref[1:2, :]
    for c_in, c_out in moves:
        c_in.wait()
        c_out.start()
    for _, c in moves:
        c.wait()


def solution(mesh):
    n_z, n_p = mesh.shape["fsdp"], mesh.shape["ep"]
    tok_spec = P(("fsdp", "ep"), None)
    spec_in = P("ep", "fsdp", None)
    spec_out = P("ep", None, "fsdp")

    def per_device(x_tok, dy_tok, expert_ids, route_w, w_gate, w_up, w_down):
        n_tok, top_k = expert_ids.shape
        d = x_tok.shape[1]
        dl, f = w_gate.shape[1], w_gate.shape[2]
        cap = capacity_of(n_tok, top_k, n_p)
        rows = 4 * cap
        n_t = n_z * n_p // 4
        sem = pltpu.SemaphoreType.DMA
        vmem = pl.BlockSpec(memory_space=pltpu.VMEM)
        hbm = pl.BlockSpec(memory_space=pl.ANY)
        out = jax.ShapeDtypeStruct
        ids, rw = expert_ids.T, route_w.T
        dw_shapes = (out((dl, f), F32), out((dl, f), F32), out((f, dl), F32))
        back = pl.pallas_call(
            functools.partial(kernel, cap, n_z, n_p),
            out_shape=(out((n_tok, d), BF16), out((8, n_tok), F32)) + dw_shapes,
            in_specs=[vmem] * 2 + [hbm] * 5,
            out_specs=(hbm,) * 5,
            scratch_shapes=[
                pltpu.VMEM((n_z, n_p, n_tok, 2 * d), BF16),
                pltpu.VMEM((n_z, n_p, 8, n_tok), F32),
                pltpu.VMEM((3, n_z * dl, f), BF16),
                pltpu.VMEM((n_tok, n_tok), BF16),
                pltpu.VMEM((n_t, rows, d), BF16),
                pltpu.VMEM((n_t, rows, d), BF16),
                pltpu.VMEM((2, n_p // 4, rows, d), BF16),
                pltpu.VMEM((n_t, dl, rows), BF16),
                pltpu.VMEM((n_t, dl, rows), BF16),
                pltpu.VMEM((2, n_p // 4, rows, min(128, d)), F32),
                pltpu.VMEM((2, n_p // 4, rows, d), F32),
                pltpu.VMEM((2, n_p, cap, d), BF16),
                pltpu.VMEM((2, n_p, 8, n_tok), F32),
                pltpu.VMEM((2, n_p, cap, d), BF16),
                pltpu.VMEM((2, n_p, 8, n_tok), F32),
                pltpu.VMEM((n_tok, d), F32),
                pltpu.VMEM((2, n_tok, d), BF16),
                pltpu.VMEM((2, 8, n_tok), F32),
                pltpu.VMEM((dl, f), F32),
                pltpu.VMEM((dl, f), F32),
                pltpu.VMEM((dl, f), F32),
                pltpu.VMEM((f, dl), F32),
                pltpu.VMEM((f, dl), BF16),
                sem((2, n_z)), sem((n_z,)), sem((2, n_z)), sem((n_z,)),
                sem((2, n_z, CHUNKS)), sem((n_z, CHUNKS)),
                sem((n_z, 4)), sem((n_z, n_p)), sem((n_z, 4)), sem((n_z, n_p)),
                sem((n_z, 3)), sem((n_z, 3)),
                sem((2, n_p)), sem((2, n_p)), sem((2, n_p)), sem((2, n_p)), sem((2,)), sem((2,)),
                sem((5,)),
            ],
            compiler_params=pltpu.CompilerParams(
                collective_id=0, has_side_effects=True, vmem_limit_bytes=67043328),
        )(ids, rw, x_tok, dy_tok, w_gate, w_up, w_down)
        gx, dr, dw0, dw1, dw2 = pl.pallas_call(
            finish,
            out_shape=(out((n_tok, d), BF16), out((top_k, n_tok), F32)) + dw_shapes,
            in_specs=[hbm, vmem] + [hbm] * 3,
            out_specs=(hbm, vmem) + (hbm,) * 3,
            scratch_shapes=[
                pltpu.VMEM((n_tok, d), BF16),
                pltpu.VMEM((dl, f), F32),
                pltpu.VMEM((dl, f), F32),
                pltpu.VMEM((f, dl), F32),
                sem((4,)), sem((4,)),
            ],
        )(*back)
        return gx, dr.T, dw0[None], dw1[None], dw2[None]

    return jax.shard_map(
        per_device, mesh=mesh,
        in_specs=(tok_spec, tok_spec, tok_spec, tok_spec, spec_in, spec_in, spec_out),
        out_specs=(tok_spec, tok_spec, spec_in, spec_in, spec_out),
        check_vma=False)
```

```python
import functools

import jax
import jax.numpy as jnp
from jax import lax
from jax.experimental import pallas as pl
from jax.experimental.pallas import tpu as pltpu
from jax.sharding import PartitionSpec as P

MESH = pl.DeviceIdType.MESH
CAP_FACTOR = 3
CHUNKS = 7
F32 = jnp.float32
BF16 = jnp.bfloat16
DIAG = (2, 4, 6)
DIRECT = (1, 2, 4, 6)
SUB = 3
RETURN = (6, 4, 7, 5, 2, 3, 1, 0)
ORDER = ((0, 1, 2, 3), (1, 0, 2, 3), (2, 3, 1, 0), (3, 2, 1, 0))
SKIP = -1
NONE = (0, 0)
PAIR = (0, 2)
FULL = (0, CHUNKS)
ONE = tuple((c, c + 1) for c in range(CHUNKS))
END_STEPS = (
    (0, NONE, NONE, NONE, NONE),
    (SKIP, ONE[0], NONE, NONE, NONE),
    (1, ONE[1], PAIR, NONE, NONE),
    (SKIP, NONE, NONE, NONE, NONE),
    (2, NONE, NONE, PAIR, NONE),
    (SKIP, ONE[2], ONE[2], ONE[2], NONE),
    (SKIP, ONE[3], ONE[3], ONE[3], NONE),
    (3, NONE, NONE, NONE, (0, 4)),
) + tuple((SKIP, c, c, c, c) for c in ONE[4:])
MID_STEPS = (
    (0, ONE[0], NONE, NONE, NONE),
    (SKIP, ONE[1], NONE, NONE, NONE),
    (SKIP, ONE[2], NONE, NONE, NONE),
    (1, NONE, PAIR, NONE, NONE),
    (SKIP, ONE[3], (2, 4), NONE, NONE),
) + tuple((SKIP, c, c, NONE, NONE) for c in ONE[4:]) + (
    (2, NONE, NONE, FULL, NONE),
    (3, NONE, NONE, NONE, NONE),
    (SKIP, NONE, NONE, NONE, FULL),
)
SEND_STEP = 7
GATHER_STEP = 10


def capacity_of(tok_dev, top_k, experts):
    return max(8, ((CAP_FACTOR * tok_dev * top_k // experts + 7) // 8) * 8)


def flip(p, q):
    for b in (1, 2, 4):
        turned = b - 2 * b * lax.rem(lax.div(p, b), 2)
        if isinstance(q, int):
            p = p + turned if q & b else p
        else:
            p = p + lax.rem(lax.div(q, b), 2) * turned
    return p


def dot_nn(a, b):
    return jnp.dot(a, b, preferred_element_type=F32)


def dot_nt(a, b):
    return lax.dot_general(a, b, (((1,), (1,)), ((), ())), preferred_element_type=F32)


def dot_tn(a, b):
    return lax.dot_general(a, b, (((0,), (0,)), ((), ())), preferred_element_type=F32)


def iota_f32(shape, dim):
    return lax.broadcasted_iota(jnp.int32, shape, dim).astype(F32)


def earlier(n):
    return jnp.where(iota_f32((n, n), 0) < iota_f32((n, n), 1), 1.0, 0.0).astype(BF16)


def positions(meta, tri, cap):
    ids0, ids1 = meta[0:1, :], meta[1:2, :]
    row = iota_f32((16, meta.shape[1]), 0)
    chosen = jnp.where(ids0 == row, 1.0, 0.0) + jnp.where(ids1 == row, 1.0, 0.0)
    before = dot_nn(chosen.astype(BF16), tri)
    return jnp.where((chosen > 0.0) & (before < cap), before, -1.0)


def pick_row(pos16, e):
    row = iota_f32(pos16.shape, 0)
    return jnp.sum(jnp.where(row == e, pos16, 0.0), axis=0, keepdims=True)


def pick(table, i):
    return sum(jnp.where(i == n, v, 0) for n, v in enumerate(table))


def kernel(cap, n_z, n_p, ids_ref, rw_ref, x_ref, dy_ref, wg_ref, wu_ref, wd_ref,
           gx_out, dr_out, dw0_out, dw1_out, dw2_out,
           xd_all, meta_all, w_all, tri_ref, xc_ref, gc_ref, dyc_ref, xt_ref, gt_ref, dy_y_ref, dx_ref,
           dxs_ref, drs_ref, dxr_ref, drr_ref, gxa_ref, gx_ref, dr_ref,
           dw0_ref, dw1_ref, dwt_ref, dw2_ref, wd_own,
           s_zt, r_zt, s_zm, r_zm, s_w, r_w, s_p, r_p, s_pm, r_pm, s_r, s_rm,
           s_dx, r_dx, s_dr, r_dr, s_gx, r_gx, s_loc):
    z = lax.axis_index("fsdp")
    p = lax.axis_index("ep")
    e_mine = p.astype(F32)
    n_tok, d = x_ref.shape
    dl, f = wg_ref.shape[1:]
    fc = f // CHUNKS
    per_h = 4
    n_h = n_p // per_h
    partner = flip(p, 1)
    mid = (z > 0) & (z < n_z - 1)
    own_rows = pl.ds(pl.multiple_of(z * dl, dl), dl)

    def plane_of(o):
        if isinstance(o, int):
            return pick([t[o] for t in ORDER], z)
        return sum(jnp.where(z == n, pick(t, o), 0) for n, t in enumerate(ORDER))

    barrier = pltpu.get_barrier_semaphore()
    for q in range(1, n_p):
        pl.semaphore_signal(barrier, inc=1, device_id={"ep": flip(p, q)}, device_id_type=MESH)
    for step in (1, -1):
        nb = z + step

        @pl.when((nb >= 0) & (nb < n_z))
        def _():
            pl.semaphore_signal(barrier, inc=1, device_id={"fsdp": nb}, device_id_type=MESH)

    load_wd = pltpu.make_async_copy(wd_ref.at[0], wd_own, s_loc.at[4])
    loads = (
        pltpu.make_async_copy(wg_ref.at[0], w_all.at[0, own_rows, :], s_loc.at[2]),
        pltpu.make_async_copy(wu_ref.at[0], w_all.at[1, own_rows, :], s_loc.at[3]),
        pltpu.make_async_copy(x_ref, xd_all.at[z, p, :, pl.ds(0, d)], s_loc.at[0]),
        pltpu.make_async_copy(dy_ref, xd_all.at[z, p, :, pl.ds(d, d)], s_loc.at[1]),
    )
    load_wd.start()
    for c in loads:
        c.start()
    meta_all[z, p, 0:2, :] = ids_ref[...].astype(F32)
    meta_all[z, p, 2:4, :] = rw_ref[...]
    meta_all[z, p, 4:8, :] = jnp.zeros((4, n_tok), F32)
    load_wd.wait()
    for c in range(CHUNKS):
        w_all[2, own_rows, c * fc:(c + 1) * fc] = wd_own[c * fc:(c + 1) * fc, :].T
    for c in loads:
        c.wait()
    inner = jnp.where(z > 0, 1, 0) + jnp.where(z < n_z - 1, 1, 0)
    pl.semaphore_wait(barrier, n_p - 1 + inner)

    def remote(src, dst, ssem, rsem, dev):
        return pltpu.make_async_remote_copy(
            src_ref=src, dst_ref=dst, send_sem=ssem, recv_sem=rsem, device_id=dev, device_id_type=MESH)

    def w_block(j, c):
        return w_all.at[:, pl.ds(pl.multiple_of(j * dl, dl), dl), pl.ds(pl.multiple_of(c * fc, fc), fc)]

    def zt_copy(j, way):
        dev = {"fsdp": z + 1 - 2 * way}
        return (remote(meta_all.at[j, p], meta_all.at[j, p], s_zm.at[way, j], r_zm.at[j], dev),
                remote(xd_all.at[j, p], xd_all.at[j, p], s_zt.at[way, j], r_zt.at[j], dev))

    def w_copy(j, c, way):
        return remote(w_block(j, c), w_block(j, c), s_w.at[way, j, c], r_w.at[j, c], {"fsdp": z + 1 - 2 * way})

    def plane_copy(j, i):
        dev = {"ep": flip(p, DIRECT[i])}
        return (remote(meta_all.at[j, p], meta_all.at[j, p], s_pm.at[j, i], r_pm.at[j, p], dev),
                remote(xd_all.at[j, p], xd_all.at[j, p], s_p.at[j, i], r_p.at[j, p], dev))

    def relay_copy(j, i):
        pp = flip(p, DIAG[i])
        dev = {"ep": partner}
        return (remote(meta_all.at[j, pp], meta_all.at[j, pp], s_rm.at[j, i], r_pm.at[j, pp], dev),
                remote(xd_all.at[j, pp], xd_all.at[j, pp], s_r.at[j, i], r_p.at[j, pp], dev))

    def plane_wait(j, pp):
        remote(meta_all.at[j, pp], meta_all.at[j, pp], s_pm.at[j, 0], r_pm.at[j, pp], {"ep": partner}).wait_recv()
        remote(xd_all.at[j, pp], xd_all.at[j, pp], s_p.at[j, 0], r_p.at[j, pp], {"ep": partner}).wait_recv()

    def valid_z(j):
        return (j >= 0) & (j < n_z)

    def start_all(copies):
        for c in copies:
            c.start()

    def link(way):
        return valid_z(z + 1 - 2 * way), (z if way == 0 else n_z - 1 - z)

    def upstream(way, dist):
        return z - dist * (1 - 2 * way)

    def own_w(depths, chunks):
        for way in (0, 1):
            there, depth = link(way)
            for q in depths:
                @pl.when(there & (depth == q))
                def _():
                    for c in chunks:
                        w_copy(z, c, way).start()

    def pass_w(q, dist, c, wait=True, send=True):
        for way in (0, 1):
            there, depth = link(way)

            @pl.when(there & (depth == q))
            def _():
                j = upstream(way, dist)
                if wait:
                    w_copy(j, c, way).wait_recv()
                if send:
                    w_copy(j, c, way).start()

    def pass_tokens(q, dist):
        for way in (0, 1):
            there, depth = link(way)

            @pl.when(there & (depth == q))
            def _():
                start_all(zt_copy(upstream(way, dist), way))

    def need_w(c):
        for way in (0, 1):
            there, _ = link(way)
            for dist in range(1, n_z):
                j = upstream(way, dist)

                @pl.when(jnp.logical_not(there) & valid_z(j))
                def _():
                    w_copy(j, c, way).wait_recv()

    def tokens(dist):
        for way, turn in ((0, z < 2), (1, z >= 0), (0, z >= 2)):
            there, depth = link(way)
            j = upstream(way, dist)

            @pl.when(turn & valid_z(j))
            def _():
                for c in zt_copy(j, way):
                    c.wait_recv()

                @pl.when(there & (depth == n_z - 2))
                def _():
                    start_all(zt_copy(j, way))

                for i in range(4):
                    start_all(plane_copy(j, i))

    def relay(o):
        j = plane_of(o)
        for i, q in enumerate(DIAG):
            plane_wait(j, flip(p, q))
            start_all(relay_copy(j, i))

    def landed(j):
        plane_wait(j, partner)
        for q in DIAG:
            plane_wait(j, flip(partner, q))

    def batch(q, c):
        own_w((q,), (c,))
        for dist in range(1, q + 1):
            pass_w(q, dist, c)

    own_w((0, 1, 2), (0,))
    for way in (0, 1):
        there, _ = link(way)

        @pl.when(there)
        def _():
            start_all(zt_copy(z, way))
    for i in range(4):
        start_all(plane_copy(z, i))
    own_w((1,), (1,))
    own_w((0,), range(1, CHUNKS))
    tri_ref[...] = earlier(n_tok)
    for ref in (dw0_ref, dw1_ref, dwt_ref, dy_y_ref, dx_ref):
        ref[...] = jnp.zeros_like(ref)

    def end_events(k):
        if k == 0:
            tokens(1)
            relay(0)
        elif k == 1:
            tokens(2)
            need_w(0)
        elif k == 2:
            relay(1)
            need_w(1)
        elif k == 3:
            tokens(3)
        elif k == 4:
            relay(2)
        elif k in (5, 6):
            need_w(k - 3)
        elif k == 7:
            relay(3)
        else:
            need_w(k - 4)

    def mid_events(k):
        if k == 0:
            pass_w(1, 1, 0)
            pass_w(2, 1, 0)
            tokens(1)
            pass_w(1, 1, 1)
            own_w((1,), (2,))
            relay(0)
            pass_w(1, 1, 2)
            pass_tokens(1, 1)
            pass_w(2, 2, 0)
        elif k == 1:
            batch(2, 1)
            batch(1, 3)
        elif k == 2:
            own_w((2,), (2,))
            pass_w(2, 1, 2, send=False)
            pass_w(2, 2, 2, send=False)
        elif k == 3:
            relay(1)
            tokens(2)
            pass_w(2, 1, 2, wait=False)
            pass_w(2, 2, 2, wait=False)
            batch(1, 4)
            batch(1, 5)
            batch(1, 6)
        elif k == 4:
            batch(2, 3)
        elif k == 5:
            batch(2, 4)
            relay(2)
        elif k in (6, 7):
            batch(2, k - 1)
        elif k == 8:
            relay(3)

    def rows_of(s):
        return lax.div(s, per_h), pl.ds(pl.multiple_of(lax.rem(s, per_h) * cap, cap), cap)

    def compact(o, j, keep_dy):
        def one(s, carry):
            meta = meta_all[j, s]
            pos = pick_row(positions(meta, tri_ref[...], cap), e_mine)
            hit = iota_f32((cap, n_tok), 0) == pos
            r_row = (jnp.where(meta[0:1, :] == e_mine, meta[2:3, :], 0.0)
                     + jnp.where(meta[1:2, :] == e_mine, meta[3:4, :], 0.0))
            r_col = jnp.sum(jnp.where(hit, r_row, 0.0), axis=1, keepdims=True)
            got = dot_nn(jnp.where(hit, 1.0, 0.0).astype(BF16), xd_all[j, s])
            h, rows = rows_of(s)
            dy = got[:, d:]
            xc_ref[o * n_h + h, rows, :] = got[:, :d].astype(BF16)
            gc_ref[o * n_h + h, rows, :] = (r_col * dy).astype(BF16)

            if keep_dy:
                dyc_ref[o, h, rows, :] = dy.astype(BF16)
            return carry

        lax.fori_loop(0, n_p, one, 0, unroll=4)

        def turn(h, carry):
            xt_ref[o * n_h + h] = xc_ref[o * n_h + h, :, own_rows].T
            gt_ref[o * n_h + h] = gc_ref[o * n_h + h, :, own_rows].T
            return carry

        lax.fori_loop(0, n_h, turn, 0)

    def cells(o, c, own):
        cols = pl.ds(pl.multiple_of(c * fc, fc), fc)
        w1, w3, w2 = w_all[0, :, cols], w_all[1, :, cols], w_all[2, :, cols]
        rows = xc_ref.shape[1]
        size = rows // SUB
        subs = [(h, slice(n * size, (n + 1) * size)) for h in range(n_h) for n in range(SUB)]
        sums = [None] * 3
        held = []

        def behind(n):
            h, at = subs[n]
            a, dh1, dh3 = held[n]
            i = o * n_h + h
            for m, (left, right) in enumerate(((xt_ref, dh1), (xt_ref, dh3), (gt_ref, a))):
                term = dot_nn(left[i, :, at], right)
                sums[m] = term if sums[m] is None else sums[m] + term
            if own:
                grown = dyc_ref[o, h, at, :].astype(F32) * dot_nt(a, w2)
                wide = dy_y_ref.shape[-1]
                dy_y_ref[o, h, at, :] += sum(grown[:, m:m + wide] for m in range(0, d, wide))
                dx_ref[o, h, at, :] += dot_nt(dh1, w1) + dot_nt(dh3, w3)

        for n, (h, at) in enumerate(subs):
            i = o * n_h + h
            h1 = dot_nn(xc_ref[i, at, :], w1)
            h3 = dot_nn(xc_ref[i, at, :], w3)
            da = dot_nn(gc_ref[i, at, :], w2)
            s = jax.nn.sigmoid(h1)
            a = (h1 * s * h3).astype(BF16)
            t = da * s
            dh3 = (t * h1).astype(BF16)
            dh1 = (t * h3 * (1.0 + h1 * (1.0 - s))).astype(BF16)
            held.append((a, dh1, dh3))
            if n:
                behind(n - 1)
        behind(len(subs) - 1)
        for ref, total in zip((dw0_ref, dw1_ref, dwt_ref), sums):
            ref[:, cols] += total

    def send_back(o):
        j = plane_of(o)

        def leave(n):
            to = flip(p, pick(RETURN, n))

            @pl.when(to != p)
            def _():
                start_all(back_copy(o, to))

            @pl.when(to == p)
            def _():
                start_all(own_back(o))

        def one(n):
            s = flip(p, pick(RETURN, n))
            h, rows = rows_of(s)
            dxs_ref[o, s] = dx_ref[o, h, rows, :].astype(BF16)
            dr_col = jnp.sum(dy_y_ref[o, h, rows, :], axis=1, keepdims=True)
            pos = pick_row(positions(meta_all[j, s], tri_ref[...], cap), e_mine)
            hit = iota_f32((cap, n_tok), 0) == pos
            dr_row = jnp.sum(jnp.where(hit, dr_col, 0.0), axis=0, keepdims=True)
            drs_ref[o, s] = jnp.broadcast_to(dr_row, (8, n_tok))

        def pair(n, carry):
            one(2 * n)
            one(2 * n + 1)

            @pl.when(n > 0)
            def _():
                leave(2 * n - 2)
                leave(2 * n - 1)

            return carry

        lax.fori_loop(0, n_p // 2, pair, 0)
        leave(n_p - 2)
        leave(n_p - 1)

    def back_copy(o, to):
        return (remote(drs_ref.at[o, to], drr_ref.at[o, p], s_dr.at[o, to], r_dr.at[o, p], {"ep": to}),
                remote(dxs_ref.at[o, to], dxr_ref.at[o, p], s_dx.at[o, to], r_dx.at[o, p], {"ep": to}))

    def own_back(o):
        return (pltpu.make_async_copy(drs_ref.at[o, p], drr_ref.at[o, p], s_dr.at[o, p]),
                pltpu.make_async_copy(dxs_ref.at[o, p], dxr_ref.at[o, p], s_dx.at[o, p]))

    def gather(o):
        meta = meta_all[plane_of(o), p]
        pos16 = positions(meta, tri_ref[...], cap)
        gxa_ref[...] = jnp.zeros_like(gxa_ref)
        dr_ref[o] = jnp.zeros_like(dr_ref[o])

        for q in range(1, n_p):
            e = flip(p, q)
            remote(drs_ref.at[o, e], drr_ref.at[o, e], s_dr.at[o, e], r_dr.at[o, e], {"ep": e}).wait_recv()
            remote(dxs_ref.at[o, e], dxr_ref.at[o, e], s_dx.at[o, e], r_dx.at[o, e], {"ep": e}).wait_recv()
        for c in own_back(o):
            c.wait()

        def one(e, carry):
            ef = e.astype(F32)
            pos = pick_row(pos16, ef)
            hit = jnp.where(iota_f32((cap, n_tok), 0) == pos, 1.0, 0.0).astype(BF16)
            gxa_ref[...] += dot_tn(hit, dxr_ref[o, e])
            dr = drr_ref[o, e]
            dr_ref[o] += jnp.where(meta == ef, dr[0:1, :], 0.0)
            return carry

        lax.fori_loop(0, n_p, one, 0, unroll=4)
        gx_ref[o] = gxa_ref[...].astype(BF16)

    def sums_out(way):
        dev = {"fsdp": z + 1 - 2 * way}
        return (remote(dr_ref.at[1], dr_out, s_gx.at[0], r_gx.at[0], dev),
                remote(gx_ref.at[1], gx_out, s_gx.at[1], r_gx.at[1], dev))

    n_steps = len(END_STEPS)

    def chosen(of, k):
        return jnp.where(mid, pick([of(t) for t in MID_STEPS], k), pick([of(t) for t in END_STEPS], k))

    def step(k, carry):
        for n in range(n_steps):
            @pl.when((k == n) & mid)
            def _():
                with jax.named_scope(f"mid_{n}"):
                    mid_events(n)

            @pl.when((k == n) & jnp.logical_not(mid))
            def _():
                with jax.named_scope(f"end_{n}"):
                    end_events(n)

        packed = chosen(lambda t: t[0], k)

        @pl.when(packed >= 0)
        def _():
            j = plane_of(packed)
            with jax.named_scope("landed"):
                landed(j)

            @pl.when(mid & (packed < 2))
            def _():
                with jax.named_scope("compact"):
                    compact(packed, j, True)

            @pl.when(jnp.logical_not(mid & (packed < 2)))
            def _():
                with jax.named_scope("compact"):
                    compact(packed, j, False)

        @pl.when(mid & (k == GATHER_STEP))
        def _():
            with jax.named_scope("gather"):
                gather(1)
            for way in (0, 1):
                @pl.when((z == 2) if way == 0 else (z == 1))
                def _():
                    start_all(sums_out(way))

        def dx_plane(m, carry):
            o = 1 - m

            def chunk(c, carry):
                with jax.named_scope("cells_own"):
                    cells(o, c, True)
                return carry

            lo = pick([chosen(lambda t, n=n: t[1 + n][0], k) for n in range(2)], o)
            hi = pick([chosen(lambda t, n=n: t[1 + n][1], k) for n in range(2)], o)
            lax.fori_loop(lo, hi, chunk, 0)

            @pl.when(k == SEND_STEP)
            def _():
                with jax.named_scope("send_back"):
                    send_back(o)

            return carry

        lax.fori_loop(0, jnp.where(mid, 2, 0), dx_plane, 0)

        def plane(o, carry):
            def chunk(c, carry):
                with jax.named_scope("cells"):
                    cells(o, c, False)
                return carry

            lo = pick([chosen(lambda t, n=n: t[1 + n][0], k) for n in range(n_z)], o)
            hi = pick([chosen(lambda t, n=n: t[1 + n][1], k) for n in range(n_z)], o)
            return lax.fori_loop(lo, hi, chunk, carry)

        return lax.fori_loop(jnp.where(mid, 2, 0), n_z, plane, carry)

    lax.fori_loop(0, n_steps, step, 0)

    stores = [pltpu.make_async_copy(dw0_ref, dw0_out, s_loc.at[0]),
              pltpu.make_async_copy(dw1_ref, dw1_out, s_loc.at[1]),
              pltpu.make_async_copy(dw2_ref, dw2_out, s_loc.at[2])]
    for c in range(CHUNKS):
        dw2_ref[c * fc:(c + 1) * fc, :] = dwt_ref[:, c * fc:(c + 1) * fc].T
    for c in stores:
        c.start()

    @pl.when(mid)
    def _():
        with jax.named_scope("gather"):
            gather(0)
        own_sums = (pltpu.make_async_copy(gx_ref.at[0], gx_out, s_loc.at[3]),
                    pltpu.make_async_copy(dr_ref.at[0], dr_out, s_loc.at[4]))
        start_all(own_sums)
        for c in own_sums:
            c.wait()
        for way in (0, 1):
            @pl.when((z == 2) if way == 0 else (z == 1))
            def _():
                for c in sums_out(way):
                    c.wait_send()

    @pl.when(jnp.logical_not(mid))
    def _():
        with jax.named_scope("sums_wait"):
            for c in sums_out(0):
                c.wait_recv()

    for c in stores:
        c.wait()

    with jax.named_scope("drain"):
        @pl.when(mid)
        def _():
            for o in range(2):
                for q in range(1, n_p):
                    for c in back_copy(o, flip(p, q)):
                        c.wait_send()

        for i in range(4):
            for j in range(n_z):
                for c in plane_copy(j, i):
                    c.wait_send()
        for i in range(3):
            for j in range(n_z):
                for c in relay_copy(j, i):
                    c.wait_send()
        for way in (0, 1):
            there, _ = link(way)
            for dist in range(n_z):
                j = upstream(way, dist)

                @pl.when(valid_z(j) & there)
                def _():
                    for c in zt_copy(j, way):
                        c.wait_send()

                    def drain(c, carry):
                        w_copy(j, c, way).wait_send()
                        return carry

                    lax.fori_loop(0, CHUNKS, drain, 0)


def finish(gx_in, dr_ref, dw0_in, dw1_in, dw2_in, gx_out, drt_ref, dw0_out, dw1_out, dw2_out,
           gx_ref, dw0_ref, dw1_ref, dw2_ref, s_in, s_out):
    moves = tuple(
        (pltpu.make_async_copy(src, mid, s_in.at[n]), pltpu.make_async_copy(mid, dst, s_out.at[n]))
        for n, (src, mid, dst) in enumerate(
            ((gx_in, gx_ref, gx_out), (dw0_in, dw0_ref, dw0_out), (dw1_in, dw1_ref, dw1_out),
             (dw2_in, dw2_ref, dw2_out))))
    for c, _ in moves:
        c.start()
    drt_ref[0:1, :] = dr_ref[0:1, :]
    drt_ref[1:2, :] = dr_ref[1:2, :]
    for c_in, c_out in moves:
        c_in.wait()
        c_out.start()
    for _, c in moves:
        c.wait()


def solution(mesh):
    n_z, n_p = mesh.shape["fsdp"], mesh.shape["ep"]
    tok_spec = P(("fsdp", "ep"), None)
    spec_in = P("ep", "fsdp", None)
    spec_out = P("ep", None, "fsdp")

    def per_device(x_tok, dy_tok, expert_ids, route_w, w_gate, w_up, w_down):
        n_tok, top_k = expert_ids.shape
        d = x_tok.shape[1]
        dl, f = w_gate.shape[1], w_gate.shape[2]
        cap = capacity_of(n_tok, top_k, n_p)
        rows = 4 * cap
        n_t = n_z * n_p // 4
        sem = pltpu.SemaphoreType.DMA
        vmem = pl.BlockSpec(memory_space=pltpu.VMEM)
        hbm = pl.BlockSpec(memory_space=pl.ANY)
        out = jax.ShapeDtypeStruct
        ids, rw = expert_ids.T, route_w.T
        dw_shapes = (out((dl, f), F32), out((dl, f), F32), out((f, dl), F32))
        back = pl.pallas_call(
            functools.partial(kernel, cap, n_z, n_p),
            out_shape=(out((n_tok, d), BF16), out((8, n_tok), F32)) + dw_shapes,
            in_specs=[vmem] * 2 + [hbm] * 5,
            out_specs=(hbm,) * 5,
            scratch_shapes=[
                pltpu.VMEM((n_z, n_p, n_tok, 2 * d), BF16),
                pltpu.VMEM((n_z, n_p, 8, n_tok), F32),
                pltpu.VMEM((3, n_z * dl, f), BF16),
                pltpu.VMEM((n_tok, n_tok), BF16),
                pltpu.VMEM((n_t, rows, d), BF16),
                pltpu.VMEM((n_t, rows, d), BF16),
                pltpu.VMEM((2, n_p // 4, rows, d), BF16),
                pltpu.VMEM((n_t, dl, rows), BF16),
                pltpu.VMEM((n_t, dl, rows), BF16),
                pltpu.VMEM((2, n_p // 4, rows, min(128, d)), F32),
                pltpu.VMEM((2, n_p // 4, rows, d), F32),
                pltpu.VMEM((2, n_p, cap, d), BF16),
                pltpu.VMEM((2, n_p, 8, n_tok), F32),
                pltpu.VMEM((2, n_p, cap, d), BF16),
                pltpu.VMEM((2, n_p, 8, n_tok), F32),
                pltpu.VMEM((n_tok, d), F32),
                pltpu.VMEM((2, n_tok, d), BF16),
                pltpu.VMEM((2, 8, n_tok), F32),
                pltpu.VMEM((dl, f), F32),
                pltpu.VMEM((dl, f), F32),
                pltpu.VMEM((dl, f), F32),
                pltpu.VMEM((f, dl), F32),
                pltpu.VMEM((f, dl), BF16),
                sem((2, n_z)), sem((n_z,)), sem((2, n_z)), sem((n_z,)),
                sem((2, n_z, CHUNKS)), sem((n_z, CHUNKS)),
                sem((n_z, 4)), sem((n_z, n_p)), sem((n_z, 4)), sem((n_z, n_p)),
                sem((n_z, 3)), sem((n_z, 3)),
                sem((2, n_p)), sem((2, n_p)), sem((2, n_p)), sem((2, n_p)), sem((2,)), sem((2,)),
                sem((5,)),
            ],
            compiler_params=pltpu.CompilerParams(
                collective_id=0, has_side_effects=True, vmem_limit_bytes=67043328),
        )(ids, rw, x_tok, dy_tok, w_gate, w_up, w_down)
        gx, dr, dw0, dw1, dw2 = pl.pallas_call(
            finish,
            out_shape=(out((n_tok, d), BF16), out((top_k, n_tok), F32)) + dw_shapes,
            in_specs=[hbm, vmem] + [hbm] * 3,
            out_specs=(hbm, vmem) + (hbm,) * 3,
            scratch_shapes=[
                pltpu.VMEM((n_tok, d), BF16),
                pltpu.VMEM((dl, f), F32),
                pltpu.VMEM((dl, f), F32),
                pltpu.VMEM((f, dl), F32),
                sem((4,)), sem((4,)),
            ],
        )(*back)
        return gx, dr.T, dw0[None], dw1[None], dw2[None]

    return jax.shard_map(
        per_device, mesh=mesh,
        in_specs=(tok_spec, tok_spec, tok_spec, tok_spec, spec_in, spec_in, spec_out),
        out_specs=(tok_spec, tok_spec, spec_in, spec_in, spec_out),
        check_vma=False)
```

```python
import functools

import jax
import jax.numpy as jnp
from jax import lax
from jax.experimental import pallas as pl
from jax.experimental.pallas import tpu as pltpu
from jax.sharding import PartitionSpec as P

MESH = pl.DeviceIdType.MESH
CAP_FACTOR = 3
CHUNKS = 7
F32 = jnp.float32
BF16 = jnp.bfloat16
DIAG = (2, 4, 6)
DIRECT = (1, 2, 4, 6)
SUB = 3
PIECES = 4
RETURN = (6, 4, 7, 5, 2, 3, 1, 0)
ORDER = ((0, 1, 2, 3), (1, 0, 2, 3), (2, 3, 1, 0), (3, 2, 1, 0))
SKIP = -1
NONE = (0, 0)
PAIR = (0, 2)
FULL = (0, CHUNKS)
ONE = tuple((c, c + 1) for c in range(CHUNKS))
END_STEPS = (
    (0, NONE, NONE, NONE, NONE),
    (SKIP, ONE[0], NONE, NONE, NONE),
    (1, ONE[1], PAIR, NONE, NONE),
    (SKIP, NONE, NONE, NONE, NONE),
    (2, NONE, NONE, PAIR, NONE),
    (SKIP, ONE[2], ONE[2], ONE[2], NONE),
    (SKIP, ONE[3], ONE[3], ONE[3], NONE),
    (3, NONE, NONE, NONE, (0, 4)),
) + tuple((SKIP, c, c, c, c) for c in ONE[4:])
MID_STEPS = (
    (0, ONE[0], NONE, NONE, NONE),
    (SKIP, ONE[1], NONE, NONE, NONE),
    (SKIP, ONE[2], NONE, NONE, NONE),
    (1, NONE, PAIR, NONE, NONE),
    (SKIP, ONE[3], (2, 4), NONE, NONE),
) + tuple((SKIP, c, c, NONE, NONE) for c in ONE[4:]) + (
    (2, NONE, NONE, FULL, NONE),
    (3, NONE, NONE, NONE, NONE),
    (SKIP, NONE, NONE, NONE, FULL),
)
SEND_STEP = 7
GATHER_STEP = 10


def capacity_of(tok_dev, top_k, experts):
    return max(8, ((CAP_FACTOR * tok_dev * top_k // experts + 7) // 8) * 8)


def flip(p, q):
    for b in (1, 2, 4):
        turned = b - 2 * b * lax.rem(lax.div(p, b), 2)
        if isinstance(q, int):
            p = p + turned if q & b else p
        else:
            p = p + lax.rem(lax.div(q, b), 2) * turned
    return p


def dot_nn(a, b):
    return jnp.dot(a, b, preferred_element_type=F32)


def dot_nt(a, b):
    return lax.dot_general(a, b, (((1,), (1,)), ((), ())), preferred_element_type=F32)


def dot_tn(a, b):
    return lax.dot_general(a, b, (((0,), (0,)), ((), ())), preferred_element_type=F32)


def iota_f32(shape, dim):
    return lax.broadcasted_iota(jnp.int32, shape, dim).astype(F32)


def earlier(n):
    return jnp.where(iota_f32((n, n), 0) < iota_f32((n, n), 1), 1.0, 0.0).astype(BF16)


def positions(meta, tri, cap):
    ids0, ids1 = meta[0:1, :], meta[1:2, :]
    row = iota_f32((16, meta.shape[1]), 0)
    chosen = jnp.where(ids0 == row, 1.0, 0.0) + jnp.where(ids1 == row, 1.0, 0.0)
    before = dot_nn(chosen.astype(BF16), tri)
    return jnp.where((chosen > 0.0) & (before < cap), before, -1.0)


def pick_row(pos16, e):
    row = iota_f32(pos16.shape, 0)
    return jnp.sum(jnp.where(row == e, pos16, 0.0), axis=0, keepdims=True)


def pick(table, i):
    return sum(jnp.where(i == n, v, 0) for n, v in enumerate(table))


def kernel(cap, n_z, n_p, ids_ref, rw_ref, x_ref, dy_ref, wg_ref, wu_ref, wd_ref,
           gx_out, dr_out, dw0_out, dw1_out, dw2_out,
           xd_all, meta_all, w_all, tri_ref, xc_ref, gc_ref, dyc_ref, xt_ref, gt_ref, dy_y_ref, dx_ref,
           dxs_ref, drs_ref, dxr_ref, drr_ref, gxa_ref, gx_ref, dr_ref,
           dw0_ref, dw1_ref, dwt_ref, dw2_ref, wd_own, ids_own, rw_own,
           s_zt, r_zt, s_zm, r_zm, s_w, r_w, s_p, r_p, s_pm, r_pm, s_r, s_rm,
           s_dx, r_dx, s_dr, r_dr, s_gx, r_gx, s_dw, s_loc):
    z = lax.axis_index("fsdp")
    p = lax.axis_index("ep")
    e_mine = p.astype(F32)
    n_tok, d = x_ref.shape
    dl, f = wg_ref.shape[1:]
    fc = f // CHUNKS
    per_h = 4
    n_h = n_p // per_h
    partner = flip(p, 1)
    mid = (z > 0) & (z < n_z - 1)
    own_rows = pl.ds(pl.multiple_of(z * dl, dl), dl)

    def plane_of(o):
        if isinstance(o, int):
            return pick([t[o] for t in ORDER], z)
        return sum(jnp.where(z == n, pick(t, o), 0) for n, t in enumerate(ORDER))

    barrier = pltpu.get_barrier_semaphore()
    for q in range(1, n_p):
        pl.semaphore_signal(barrier, inc=1, device_id={"ep": flip(p, q)}, device_id_type=MESH)
    for step in (1, -1):
        nb = z + step

        @pl.when((nb >= 0) & (nb < n_z))
        def _():
            pl.semaphore_signal(barrier, inc=1, device_id={"fsdp": nb}, device_id_type=MESH)

    load_wd = pltpu.make_async_copy(wd_ref.at[0], wd_own, s_loc.at[4])
    loads = (
        pltpu.make_async_copy(wg_ref.at[0], w_all.at[0, own_rows, :], s_loc.at[2]),
        pltpu.make_async_copy(wu_ref.at[0], w_all.at[1, own_rows, :], s_loc.at[3]),
        pltpu.make_async_copy(x_ref, xd_all.at[z, p, :, pl.ds(0, d)], s_loc.at[0]),
        pltpu.make_async_copy(dy_ref, xd_all.at[z, p, :, pl.ds(d, d)], s_loc.at[1]),
    )
    small = (pltpu.make_async_copy(ids_ref, ids_own, s_loc.at[5]),
             pltpu.make_async_copy(rw_ref, rw_own, s_loc.at[6]))
    load_wd.start()
    for c in small + loads:
        c.start()
    for c in small:
        c.wait()
    meta_all[z, p, 0:2, :] = ids_own[...].astype(F32)
    meta_all[z, p, 2:4, :] = rw_own[...]
    meta_all[z, p, 4:8, :] = jnp.zeros((4, n_tok), F32)
    load_wd.wait()
    for c in range(CHUNKS):
        w_all[2, own_rows, c * fc:(c + 1) * fc] = wd_own[c * fc:(c + 1) * fc, :].T
    for c in loads:
        c.wait()
    inner = jnp.where(z > 0, 1, 0) + jnp.where(z < n_z - 1, 1, 0)
    pl.semaphore_wait(barrier, n_p - 1 + inner)

    def remote(src, dst, ssem, rsem, dev):
        return pltpu.make_async_remote_copy(
            src_ref=src, dst_ref=dst, send_sem=ssem, recv_sem=rsem, device_id=dev, device_id_type=MESH)

    def w_block(j, c):
        return w_all.at[:, pl.ds(pl.multiple_of(j * dl, dl), dl), pl.ds(pl.multiple_of(c * fc, fc), fc)]

    def zt_copy(j, way):
        dev = {"fsdp": z + 1 - 2 * way}
        return (remote(meta_all.at[j, p], meta_all.at[j, p], s_zm.at[way, j], r_zm.at[j], dev),
                remote(xd_all.at[j, p], xd_all.at[j, p], s_zt.at[way, j], r_zt.at[j], dev))

    def w_copy(j, c, way):
        return remote(w_block(j, c), w_block(j, c), s_w.at[way, j, c], r_w.at[j, c], {"fsdp": z + 1 - 2 * way})

    def plane_copy(j, i):
        dev = {"ep": flip(p, DIRECT[i])}
        return (remote(meta_all.at[j, p], meta_all.at[j, p], s_pm.at[j, i], r_pm.at[j, p], dev),
                remote(xd_all.at[j, p], xd_all.at[j, p], s_p.at[j, i], r_p.at[j, p], dev))

    def relay_copy(j, i):
        pp = flip(p, DIAG[i])
        dev = {"ep": partner}
        return (remote(meta_all.at[j, pp], meta_all.at[j, pp], s_rm.at[j, i], r_pm.at[j, pp], dev),
                remote(xd_all.at[j, pp], xd_all.at[j, pp], s_r.at[j, i], r_p.at[j, pp], dev))

    def plane_wait(j, pp):
        remote(meta_all.at[j, pp], meta_all.at[j, pp], s_pm.at[j, 0], r_pm.at[j, pp], {"ep": partner}).wait_recv()
        remote(xd_all.at[j, pp], xd_all.at[j, pp], s_p.at[j, 0], r_p.at[j, pp], {"ep": partner}).wait_recv()

    def valid_z(j):
        return (j >= 0) & (j < n_z)

    def start_all(copies):
        for c in copies:
            c.start()

    def link(way):
        return valid_z(z + 1 - 2 * way), (z if way == 0 else n_z - 1 - z)

    def upstream(way, dist):
        return z - dist * (1 - 2 * way)

    def own_w(depths, chunks):
        for way in (0, 1):
            there, depth = link(way)
            for q in depths:
                @pl.when(there & (depth == q))
                def _():
                    for c in chunks:
                        w_copy(z, c, way).start()

    def pass_w(q, dist, c, wait=True, send=True):
        for way in (0, 1):
            there, depth = link(way)

            @pl.when(there & (depth == q))
            def _():
                j = upstream(way, dist)
                if wait:
                    w_copy(j, c, way).wait_recv()
                if send:
                    w_copy(j, c, way).start()

    def pass_tokens(q, dist):
        for way in (0, 1):
            there, depth = link(way)

            @pl.when(there & (depth == q))
            def _():
                start_all(zt_copy(upstream(way, dist), way))

    def need_w(c):
        for way in (0, 1):
            there, _ = link(way)
            for dist in range(1, n_z):
                j = upstream(way, dist)

                @pl.when(jnp.logical_not(there) & valid_z(j))
                def _():
                    w_copy(j, c, way).wait_recv()

    def tokens(dist):
        for way, turn in ((0, z < 2), (1, z >= 0), (0, z >= 2)):
            there, depth = link(way)
            j = upstream(way, dist)

            @pl.when(turn & valid_z(j))
            def _():
                for c in zt_copy(j, way):
                    c.wait_recv()

                @pl.when(there & (depth == n_z - 2))
                def _():
                    start_all(zt_copy(j, way))

                for i in range(4):
                    start_all(plane_copy(j, i))

    def relay(o):
        j = plane_of(o)
        for i, q in enumerate(DIAG):
            plane_wait(j, flip(p, q))
            start_all(relay_copy(j, i))

    def landed(j):
        plane_wait(j, partner)
        for q in DIAG:
            plane_wait(j, flip(partner, q))

    def batch(q, c):
        own_w((q,), (c,))
        for dist in range(1, q + 1):
            pass_w(q, dist, c)

    own_w((0, 1, 2), (0,))
    for way in (0, 1):
        there, _ = link(way)

        @pl.when(there)
        def _():
            start_all(zt_copy(z, way))
    for i in range(4):
        start_all(plane_copy(z, i))
    own_w((1,), (1,))
    own_w((0,), range(1, CHUNKS))
    tri_ref[...] = earlier(n_tok)
    for ref in (dw0_ref, dw1_ref, dwt_ref, dy_y_ref, dx_ref):
        ref[...] = jnp.zeros_like(ref)

    def end_events(k):
        if k == 0:
            tokens(1)
            relay(0)
        elif k == 1:
            tokens(2)
            need_w(0)
        elif k == 2:
            relay(1)
            need_w(1)
        elif k == 3:
            tokens(3)
        elif k == 4:
            relay(2)
        elif k in (5, 6):
            need_w(k - 3)
        elif k == 7:
            relay(3)
        else:
            need_w(k - 4)

    def mid_events(k):
        if k == 0:
            pass_w(1, 1, 0)
            pass_w(2, 1, 0)
            tokens(1)
            pass_w(1, 1, 1)
            own_w((1,), (2,))
            relay(0)
            pass_w(1, 1, 2)
            pass_tokens(1, 1)
            pass_w(2, 2, 0)
        elif k == 1:
            batch(2, 1)
            batch(1, 3)
        elif k == 2:
            own_w((2,), (2,))
            pass_w(2, 1, 2, send=False)
            pass_w(2, 2, 2, send=False)
        elif k == 3:
            relay(1)
            tokens(2)
            pass_w(2, 1, 2, wait=False)
            pass_w(2, 2, 2, wait=False)
            batch(1, 4)
            batch(1, 5)
            batch(1, 6)
        elif k == 4:
            batch(2, 3)
        elif k == 5:
            batch(2, 4)
            relay(2)
        elif k in (6, 7):
            batch(2, k - 1)
        elif k == 8:
            relay(3)

    def rows_of(s):
        return lax.div(s, per_h), pl.ds(pl.multiple_of(lax.rem(s, per_h) * cap, cap), cap)

    def compact(o, j, keep_dy):
        def one(s, carry):
            meta = meta_all[j, s]
            pos = pick_row(positions(meta, tri_ref[...], cap), e_mine)
            hit = iota_f32((cap, n_tok), 0) == pos
            r_row = (jnp.where(meta[0:1, :] == e_mine, meta[2:3, :], 0.0)
                     + jnp.where(meta[1:2, :] == e_mine, meta[3:4, :], 0.0))
            r_col = jnp.sum(jnp.where(hit, r_row, 0.0), axis=1, keepdims=True)
            got = dot_nn(jnp.where(hit, 1.0, 0.0).astype(BF16), xd_all[j, s])
            h, rows = rows_of(s)
            dy = got[:, d:]
            xc_ref[o * n_h + h, rows, :] = got[:, :d].astype(BF16)
            gc_ref[o * n_h + h, rows, :] = (r_col * dy).astype(BF16)

            if keep_dy:
                dyc_ref[o, h, rows, :] = dy.astype(BF16)
            return carry

        lax.fori_loop(0, n_p, one, 0, unroll=4)

        def turn(h, carry):
            xt_ref[o * n_h + h] = xc_ref[o * n_h + h, :, own_rows].T
            gt_ref[o * n_h + h] = gc_ref[o * n_h + h, :, own_rows].T
            return carry

        lax.fori_loop(0, n_h, turn, 0)

    def cells(o, c, own):
        cols = pl.ds(pl.multiple_of(c * fc, fc), fc)
        w1, w3, w2 = w_all[0, :, cols], w_all[1, :, cols], w_all[2, :, cols]
        rows = xc_ref.shape[1]
        size = rows // SUB
        subs = [(h, slice(n * size, (n + 1) * size)) for h in range(n_h) for n in range(SUB)]
        sums = [None] * 3
        held = []

        def behind(n):
            h, at = subs[n]
            a, dh1, dh3 = held[n]
            i = o * n_h + h
            for m, (left, right) in enumerate(((xt_ref, dh1), (xt_ref, dh3), (gt_ref, a))):
                term = dot_nn(left[i, :, at], right)
                sums[m] = term if sums[m] is None else sums[m] + term
            if own:
                grown = dyc_ref[o, h, at, :].astype(F32) * dot_nt(a, w2)
                wide = dy_y_ref.shape[-1]
                dy_y_ref[o, h, at, :] += sum(grown[:, m:m + wide] for m in range(0, d, wide))
                dx_ref[o, h, at, :] += dot_nt(dh1, w1) + dot_nt(dh3, w3)

        for n, (h, at) in enumerate(subs):
            i = o * n_h + h
            h1 = dot_nn(xc_ref[i, at, :], w1)
            h3 = dot_nn(xc_ref[i, at, :], w3)
            da = dot_nn(gc_ref[i, at, :], w2)
            s = jax.nn.sigmoid(h1)
            a = (h1 * s * h3).astype(BF16)
            t = da * s
            dh3 = (t * h1).astype(BF16)
            dh1 = (t * h3 * (1.0 + h1 * (1.0 - s))).astype(BF16)
            held.append((a, dh1, dh3))
            if n:
                behind(n - 1)
        behind(len(subs) - 1)
        for ref, total in zip((dw0_ref, dw1_ref, dwt_ref), sums):
            ref[:, cols] += total

    def send_back(o):
        j = plane_of(o)

        def leave(n):
            to = flip(p, pick(RETURN, n))

            @pl.when(to != p)
            def _():
                start_all(back_copy(o, to))

            @pl.when(to == p)
            def _():
                start_all(own_back(o))

        def one(n):
            s = flip(p, pick(RETURN, n))
            h, rows = rows_of(s)
            dxs_ref[o, s] = dx_ref[o, h, rows, :].astype(BF16)
            dr_col = jnp.sum(dy_y_ref[o, h, rows, :], axis=1, keepdims=True)
            pos = pick_row(positions(meta_all[j, s], tri_ref[...], cap), e_mine)
            hit = iota_f32((cap, n_tok), 0) == pos
            dr_row = jnp.sum(jnp.where(hit, dr_col, 0.0), axis=0, keepdims=True)
            drs_ref[o, s] = jnp.broadcast_to(dr_row, (8, n_tok))

        def pair(n, carry):
            one(2 * n)
            one(2 * n + 1)

            @pl.when(n > 0)
            def _():
                leave(2 * n - 2)
                leave(2 * n - 1)

            return carry

        lax.fori_loop(0, n_p // 2, pair, 0)
        leave(n_p - 2)
        leave(n_p - 1)

    def back_copy(o, to):
        return (remote(drs_ref.at[o, to], drr_ref.at[o, p], s_dr.at[o, to], r_dr.at[o, p], {"ep": to}),
                remote(dxs_ref.at[o, to], dxr_ref.at[o, p], s_dx.at[o, to], r_dx.at[o, p], {"ep": to}))

    def own_back(o):
        return (pltpu.make_async_copy(drs_ref.at[o, p], drr_ref.at[o, p], s_dr.at[o, p]),
                pltpu.make_async_copy(dxs_ref.at[o, p], dxr_ref.at[o, p], s_dx.at[o, p]))

    def gather(o):
        meta = meta_all[plane_of(o), p]
        pos16 = positions(meta, tri_ref[...], cap)
        gxa_ref[...] = jnp.zeros_like(gxa_ref)
        dr_ref[o] = jnp.zeros_like(dr_ref[o])

        for q in range(1, n_p):
            e = flip(p, q)
            remote(drs_ref.at[o, e], drr_ref.at[o, e], s_dr.at[o, e], r_dr.at[o, e], {"ep": e}).wait_recv()
            remote(dxs_ref.at[o, e], dxr_ref.at[o, e], s_dx.at[o, e], r_dx.at[o, e], {"ep": e}).wait_recv()
        for c in own_back(o):
            c.wait()

        def one(e, carry):
            ef = e.astype(F32)
            pos = pick_row(pos16, ef)
            hit = jnp.where(iota_f32((cap, n_tok), 0) == pos, 1.0, 0.0).astype(BF16)
            gxa_ref[...] += dot_tn(hit, dxr_ref[o, e])
            dr = drr_ref[o, e]
            dr_ref[o] += jnp.where(meta == ef, dr[0:1, :], 0.0)
            return carry

        lax.fori_loop(0, n_p, one, 0, unroll=4)
        gx_ref[o] = gxa_ref[...].astype(BF16)

    def sums_out(way):
        dev = {"fsdp": z + 1 - 2 * way}
        return (remote(dr_ref.at[1], dr_out, s_gx.at[0], r_gx.at[0], dev),
                remote(gx_ref.at[1], gx_out, s_gx.at[1], r_gx.at[1], dev))

    n_steps = len(END_STEPS)

    def stores(c):
        cols = pl.ds(pl.multiple_of(c * fc, fc), fc)
        return (pltpu.make_async_copy(dw0_ref.at[:, cols], dw0_out.at[:, cols], s_dw.at[0, c]),
                pltpu.make_async_copy(dw1_ref.at[:, cols], dw1_out.at[:, cols], s_dw.at[1, c]),
                pltpu.make_async_copy(dw2_ref.at[cols, :], dw2_out.at[cols, :], s_dw.at[2, c]))

    def chosen(of, k):
        return jnp.where(mid, pick([of(t) for t in MID_STEPS], k), pick([of(t) for t in END_STEPS], k))

    def step(k, carry):
        for n in range(n_steps):
            @pl.when((k == n) & mid)
            def _():
                with jax.named_scope(f"mid_{n}"):
                    mid_events(n)

            @pl.when((k == n) & jnp.logical_not(mid))
            def _():
                with jax.named_scope(f"end_{n}"):
                    end_events(n)

        packed = chosen(lambda t: t[0], k)

        @pl.when(packed >= 0)
        def _():
            j = plane_of(packed)
            with jax.named_scope("landed"):
                landed(j)

            @pl.when(mid & (packed < 2))
            def _():
                with jax.named_scope("compact"):
                    compact(packed, j, True)

            @pl.when(jnp.logical_not(mid & (packed < 2)))
            def _():
                with jax.named_scope("compact"):
                    compact(packed, j, False)

        @pl.when(mid & (k == GATHER_STEP))
        def _():
            with jax.named_scope("gather"):
                gather(1)
            for way in (0, 1):
                @pl.when((z == 2) if way == 0 else (z == 1))
                def _():
                    start_all(sums_out(way))

        def dx_plane(m, carry):
            o = 1 - m

            def chunk(c, carry):
                with jax.named_scope("cells_own"):
                    cells(o, c, True)
                return carry

            lo = pick([chosen(lambda t, n=n: t[1 + n][0], k) for n in range(2)], o)
            hi = pick([chosen(lambda t, n=n: t[1 + n][1], k) for n in range(2)], o)
            lax.fori_loop(lo, hi, chunk, 0)

            @pl.when(k == SEND_STEP)
            def _():
                with jax.named_scope("send_back"):
                    send_back(o)

            return carry

        lax.fori_loop(0, jnp.where(mid, 2, 0), dx_plane, 0)

        def plane(o, carry):
            def chunk(c, carry):
                with jax.named_scope("cells"):
                    cells(o, c, False)

                @pl.when(o == n_z - 1)
                def _():
                    cols = pl.ds(pl.multiple_of(c * fc, fc), fc)
                    dw2_ref[cols, :] = dwt_ref[:, cols].T
                    start_all(stores(c))

                return carry

            lo = pick([chosen(lambda t, n=n: t[1 + n][0], k) for n in range(n_z)], o)
            hi = pick([chosen(lambda t, n=n: t[1 + n][1], k) for n in range(n_z)], o)
            return lax.fori_loop(lo, hi, chunk, carry)

        return lax.fori_loop(jnp.where(mid, 2, 0), n_z, plane, carry)

    lax.fori_loop(0, n_steps, step, 0)

    @pl.when(mid)
    def _():
        with jax.named_scope("gather"):
            gather(0)
        own_sums = (pltpu.make_async_copy(gx_ref.at[0], gx_out, s_loc.at[3]),
                    pltpu.make_async_copy(dr_ref.at[0], dr_out, s_loc.at[4]))
        start_all(own_sums)
        for c in own_sums:
            c.wait()
        for way in (0, 1):
            @pl.when((z == 2) if way == 0 else (z == 1))
            def _():
                for c in sums_out(way):
                    c.wait_send()

    @pl.when(jnp.logical_not(mid))
    def _():
        with jax.named_scope("sums_wait"):
            for c in sums_out(0):
                c.wait_recv()

    def stored(c, carry):
        for copy in stores(c):
            copy.wait()
        return carry

    lax.fori_loop(0, CHUNKS, stored, 0)

    with jax.named_scope("drain"):
        @pl.when(mid)
        def _():
            for o in range(2):
                for q in range(1, n_p):
                    for c in back_copy(o, flip(p, q)):
                        c.wait_send()

        for i in range(4):
            for j in range(n_z):
                for c in plane_copy(j, i):
                    c.wait_send()
        for i in range(3):
            for j in range(n_z):
                for c in relay_copy(j, i):
                    c.wait_send()
        for way in (0, 1):
            there, _ = link(way)
            for dist in range(n_z):
                j = upstream(way, dist)

                @pl.when(valid_z(j) & there)
                def _():
                    for c in zt_copy(j, way):
                        c.wait_send()

                    def drain(c, carry):
                        w_copy(j, c, way).wait_send()
                        return carry

                    lax.fori_loop(0, CHUNKS, drain, 0)


def finish(gx_in, dr_in, dw0_in, dw1_in, dw2_in, gx_out, dr_out, dw0_out, dw1_out, dw2_out,
           gx_ref, dr_ref, drt_ref, dw0_ref, dw1_ref, dw2_ref, s_in, s_out):
    moves = []
    for src, via, dst in ((dw0_in, dw0_ref, dw0_out), (dw1_in, dw1_ref, dw1_out), (dw2_in, dw2_ref, dw2_out),
                          (gx_in, gx_ref, gx_out)):
        rows = src.shape[0] // PIECES
        for at in [pl.ds(i * rows, rows) for i in range(PIECES)]:
            n = len(moves)
            moves.append((pltpu.make_async_copy(src.at[at, :], via.at[at, :], s_in.at[n]),
                          pltpu.make_async_copy(via.at[at, :], dst.at[at, :], s_out.at[n])))
    dr_load = pltpu.make_async_copy(dr_in, dr_ref, s_in.at[len(moves)])
    dr_store = pltpu.make_async_copy(drt_ref, dr_out, s_out.at[len(moves)])
    dr_load.start()
    for c, _ in moves:
        c.start()
    dr_load.wait()
    drt_ref[...] = dr_ref[: drt_ref.shape[0], :]
    for c_in, c_out in moves:
        c_in.wait()
        c_out.start()
    dr_store.start()
    for _, c in moves:
        c.wait()
    dr_store.wait()


def solution(mesh):
    n_z, n_p = mesh.shape["fsdp"], mesh.shape["ep"]
    tok_spec = P(("fsdp", "ep"), None)
    spec_in = P("ep", "fsdp", None)
    spec_out = P("ep", None, "fsdp")

    def per_device(x_tok, dy_tok, expert_ids, route_w, w_gate, w_up, w_down):
        n_tok, top_k = expert_ids.shape
        d = x_tok.shape[1]
        dl, f = w_gate.shape[1], w_gate.shape[2]
        cap = capacity_of(n_tok, top_k, n_p)
        rows = 4 * cap
        n_t = n_z * n_p // 4
        sem = pltpu.SemaphoreType.DMA
        hbm = pl.BlockSpec(memory_space=pl.ANY)
        out = jax.ShapeDtypeStruct
        ids, rw = expert_ids.T, route_w.T
        dw_shapes = (out((dl, f), F32), out((dl, f), F32), out((f, dl), F32))
        back = pl.pallas_call(
            functools.partial(kernel, cap, n_z, n_p),
            out_shape=(out((n_tok, d), BF16), out((8, n_tok), F32)) + dw_shapes,
            in_specs=[hbm] * 7,
            out_specs=(hbm,) * 5,
            scratch_shapes=[
                pltpu.VMEM((n_z, n_p, n_tok, 2 * d), BF16),
                pltpu.VMEM((n_z, n_p, 8, n_tok), F32),
                pltpu.VMEM((3, n_z * dl, f), BF16),
                pltpu.VMEM((n_tok, n_tok), BF16),
                pltpu.VMEM((n_t, rows, d), BF16),
                pltpu.VMEM((n_t, rows, d), BF16),
                pltpu.VMEM((2, n_p // 4, rows, d), BF16),
                pltpu.VMEM((n_t, dl, rows), BF16),
                pltpu.VMEM((n_t, dl, rows), BF16),
                pltpu.VMEM((2, n_p // 4, rows, min(128, d)), F32),
                pltpu.VMEM((2, n_p // 4, rows, d), F32),
                pltpu.VMEM((2, n_p, cap, d), BF16),
                pltpu.VMEM((2, n_p, 8, n_tok), F32),
                pltpu.VMEM((2, n_p, cap, d), BF16),
                pltpu.VMEM((2, n_p, 8, n_tok), F32),
                pltpu.VMEM((n_tok, d), F32),
                pltpu.VMEM((2, n_tok, d), BF16),
                pltpu.VMEM((2, 8, n_tok), F32),
                pltpu.VMEM((dl, f), F32),
                pltpu.VMEM((dl, f), F32),
                pltpu.VMEM((dl, f), F32),
                pltpu.VMEM((f, dl), F32),
                pltpu.VMEM((f, dl), BF16),
                pltpu.VMEM((top_k, n_tok), jnp.int32),
                pltpu.VMEM((top_k, n_tok), F32),
                sem((2, n_z)), sem((n_z,)), sem((2, n_z)), sem((n_z,)),
                sem((2, n_z, CHUNKS)), sem((n_z, CHUNKS)),
                sem((n_z, 4)), sem((n_z, n_p)), sem((n_z, 4)), sem((n_z, n_p)),
                sem((n_z, 3)), sem((n_z, 3)),
                sem((2, n_p)), sem((2, n_p)), sem((2, n_p)), sem((2, n_p)), sem((2,)), sem((2,)),
                sem((3, CHUNKS)),
                sem((7,)),
            ],
            compiler_params=pltpu.CompilerParams(
                collective_id=0, has_side_effects=True, vmem_limit_bytes=67043328),
        )(ids, rw, x_tok, dy_tok, w_gate, w_up, w_down)
        gx, dr, dw0, dw1, dw2 = pl.pallas_call(
            finish,
            out_shape=(out((n_tok, d), BF16), out((top_k, n_tok), F32)) + dw_shapes,
            in_specs=[hbm] * 5,
            out_specs=(hbm,) * 5,
            scratch_shapes=[
                pltpu.VMEM((n_tok, d), BF16),
                pltpu.VMEM((8, n_tok), F32),
                pltpu.VMEM((top_k, n_tok), F32),
                pltpu.VMEM((dl, f), F32),
                pltpu.VMEM((dl, f), F32),
                pltpu.VMEM((f, dl), F32),
                sem((4 * PIECES + 1,)), sem((4 * PIECES + 1,)),
            ],
        )(*back)
        return gx, dr.T, dw0[None], dw1[None], dw2[None]

    return jax.shard_map(
        per_device, mesh=mesh,
        in_specs=(tok_spec, tok_spec, tok_spec, tok_spec, spec_in, spec_in, spec_out),
        out_specs=(tok_spec, tok_spec, spec_in, spec_in, spec_out),
        check_vma=False)
```

```python
import functools

import jax
import jax.numpy as jnp
from jax import lax
from jax.experimental import pallas as pl
from jax.experimental.pallas import tpu as pltpu
from jax.sharding import PartitionSpec as P

MESH = pl.DeviceIdType.MESH
CAP_FACTOR = 3
CHUNKS = 7
F32 = jnp.float32
BF16 = jnp.bfloat16
DIAG = (2, 4, 6)
DIRECT = (1, 2, 4, 6)
SUB = 3
PIECES = 4
EARLY = (0, 1, 2, 3, 4, 5)
LATE = (6, 7)
RETURN = (6, 4, 7, 5, 2, 3, 1, 0)
ORDER = ((0, 1, 2, 3), (1, 0, 2, 3), (2, 3, 1, 0), (3, 2, 1, 0))
SKIP = -1
NONE = (0, 0)
PAIR = (0, 2)
FULL = (0, CHUNKS)
ONE = tuple((c, c + 1) for c in range(CHUNKS))
END_STEPS = (
    (0, NONE, NONE, NONE, NONE),
    (SKIP, ONE[0], NONE, NONE, NONE),
    (1, ONE[1], PAIR, NONE, NONE),
    (SKIP, NONE, NONE, NONE, NONE),
    (2, NONE, NONE, PAIR, NONE),
    (SKIP, ONE[2], ONE[2], ONE[2], NONE),
    (SKIP, ONE[3], ONE[3], ONE[3], NONE),
    (3, NONE, NONE, NONE, (0, 4)),
) + tuple((SKIP, c, c, c, c) for c in ONE[4:])
MID_STEPS = (
    (0, ONE[0], NONE, NONE, NONE),
    (SKIP, ONE[1], NONE, NONE, NONE),
    (SKIP, ONE[2], NONE, NONE, NONE),
    (1, NONE, PAIR, NONE, NONE),
    (SKIP, ONE[3], (2, 4), NONE, NONE),
) + tuple((SKIP, c, c, NONE, NONE) for c in ONE[4:]) + (
    (2, NONE, NONE, FULL, NONE),
    (3, NONE, NONE, NONE, NONE),
    (SKIP, NONE, NONE, NONE, FULL),
)
SEND_STEP = 7
GATHER_STEP = 10


def capacity_of(tok_dev, top_k, experts):
    return max(8, ((CAP_FACTOR * tok_dev * top_k // experts + 7) // 8) * 8)


def flip(p, q):
    for b in (1, 2, 4):
        turned = b - 2 * b * lax.rem(lax.div(p, b), 2)
        if isinstance(q, int):
            p = p + turned if q & b else p
        else:
            p = p + lax.rem(lax.div(q, b), 2) * turned
    return p


def dot_nn(a, b):
    return jnp.dot(a, b, preferred_element_type=F32)


def dot_nt(a, b):
    return lax.dot_general(a, b, (((1,), (1,)), ((), ())), preferred_element_type=F32)


def dot_tn(a, b):
    return lax.dot_general(a, b, (((0,), (0,)), ((), ())), preferred_element_type=F32)


def iota_f32(shape, dim):
    return lax.broadcasted_iota(jnp.int32, shape, dim).astype(F32)


def earlier(n):
    return jnp.where(iota_f32((n, n), 0) < iota_f32((n, n), 1), 1.0, 0.0).astype(BF16)


def positions(meta, tri, cap):
    ids0, ids1 = meta[0:1, :], meta[1:2, :]
    row = iota_f32((16, meta.shape[1]), 0)
    chosen = jnp.where(ids0 == row, 1.0, 0.0) + jnp.where(ids1 == row, 1.0, 0.0)
    before = dot_nn(chosen.astype(BF16), tri)
    return jnp.where((chosen > 0.0) & (before < cap), before, -1.0)


def pick_row(pos16, e):
    row = iota_f32(pos16.shape, 0)
    return jnp.sum(jnp.where(row == e, pos16, 0.0), axis=0, keepdims=True)


def pick(table, i):
    return sum(jnp.where(i == n, v, 0) for n, v in enumerate(table))


def kernel(cap, n_z, n_p, ids_ref, rw_ref, x_ref, dy_ref, wg_ref, wu_ref, wd_ref,
           gx_out, dr_out, dw0_out, dw1_out, dw2_out,
           xd_all, meta_all, w_all, tri_ref, xc_ref, gc_ref, dyc_ref, xt_ref, gt_ref, dy_y_ref, dx_ref,
           dxs_ref, drs_ref, dxr_ref, drr_ref, gxa_ref, gx_ref, dr_ref,
           dw0_ref, dw1_ref, dwt_ref, dw2_ref, wd_own, ids_own, rw_own,
           s_zt, r_zt, s_zm, r_zm, s_w, r_w, s_p, r_p, s_pm, r_pm, s_r, s_rm,
           s_dx, r_dx, s_dr, r_dr, s_gx, r_gx, s_dw, s_loc):
    z = lax.axis_index("fsdp")
    p = lax.axis_index("ep")
    e_mine = p.astype(F32)
    n_tok, d = x_ref.shape
    dl, f = wg_ref.shape[1:]
    fc = f // CHUNKS
    per_h = 4
    n_h = n_p // per_h
    partner = flip(p, 1)
    mid = (z > 0) & (z < n_z - 1)
    own_rows = pl.ds(pl.multiple_of(z * dl, dl), dl)

    def plane_of(o):
        if isinstance(o, int):
            return pick([t[o] for t in ORDER], z)
        return sum(jnp.where(z == n, pick(t, o), 0) for n, t in enumerate(ORDER))

    barrier = pltpu.get_barrier_semaphore()
    for q in range(1, n_p):
        pl.semaphore_signal(barrier, inc=1, device_id={"ep": flip(p, q)}, device_id_type=MESH)
    for step in (1, -1):
        nb = z + step

        @pl.when((nb >= 0) & (nb < n_z))
        def _():
            pl.semaphore_signal(barrier, inc=1, device_id={"fsdp": nb}, device_id_type=MESH)

    load_wd = pltpu.make_async_copy(wd_ref.at[0], wd_own, s_loc.at[4])
    loads = (
        pltpu.make_async_copy(wg_ref.at[0], w_all.at[0, own_rows, :], s_loc.at[2]),
        pltpu.make_async_copy(wu_ref.at[0], w_all.at[1, own_rows, :], s_loc.at[3]),
        pltpu.make_async_copy(x_ref, xd_all.at[z, p, :, pl.ds(0, d)], s_loc.at[0]),
        pltpu.make_async_copy(dy_ref, xd_all.at[z, p, :, pl.ds(d, d)], s_loc.at[1]),
    )
    small = (pltpu.make_async_copy(ids_ref, ids_own, s_loc.at[5]),
             pltpu.make_async_copy(rw_ref, rw_own, s_loc.at[6]))
    load_wd.start()
    for c in small + loads:
        c.start()
    for c in small:
        c.wait()
    meta_all[z, p, 0:2, :] = ids_own[...].astype(F32)
    meta_all[z, p, 2:4, :] = rw_own[...]
    meta_all[z, p, 4:8, :] = jnp.zeros((4, n_tok), F32)
    load_wd.wait()
    for c in range(CHUNKS):
        w_all[2, own_rows, c * fc:(c + 1) * fc] = wd_own[c * fc:(c + 1) * fc, :].T
    for c in loads:
        c.wait()
    inner = jnp.where(z > 0, 1, 0) + jnp.where(z < n_z - 1, 1, 0)
    pl.semaphore_wait(barrier, n_p - 1 + inner)

    def remote(src, dst, ssem, rsem, dev):
        return pltpu.make_async_remote_copy(
            src_ref=src, dst_ref=dst, send_sem=ssem, recv_sem=rsem, device_id=dev, device_id_type=MESH)

    def w_block(j, c):
        return w_all.at[:, pl.ds(pl.multiple_of(j * dl, dl), dl), pl.ds(pl.multiple_of(c * fc, fc), fc)]

    def zt_copy(j, way):
        dev = {"fsdp": z + 1 - 2 * way}
        return (remote(meta_all.at[j, p], meta_all.at[j, p], s_zm.at[way, j], r_zm.at[j], dev),
                remote(xd_all.at[j, p], xd_all.at[j, p], s_zt.at[way, j], r_zt.at[j], dev))

    def w_copy(j, c, way):
        return remote(w_block(j, c), w_block(j, c), s_w.at[way, j, c], r_w.at[j, c], {"fsdp": z + 1 - 2 * way})

    def plane_copy(j, i):
        dev = {"ep": flip(p, DIRECT[i])}
        return (remote(meta_all.at[j, p], meta_all.at[j, p], s_pm.at[j, i], r_pm.at[j, p], dev),
                remote(xd_all.at[j, p], xd_all.at[j, p], s_p.at[j, i], r_p.at[j, p], dev))

    def relay_copy(j, i):
        pp = flip(p, DIAG[i])
        dev = {"ep": partner}
        return (remote(meta_all.at[j, pp], meta_all.at[j, pp], s_rm.at[j, i], r_pm.at[j, pp], dev),
                remote(xd_all.at[j, pp], xd_all.at[j, pp], s_r.at[j, i], r_p.at[j, pp], dev))

    def plane_wait(j, pp):
        remote(meta_all.at[j, pp], meta_all.at[j, pp], s_pm.at[j, 0], r_pm.at[j, pp], {"ep": partner}).wait_recv()
        remote(xd_all.at[j, pp], xd_all.at[j, pp], s_p.at[j, 0], r_p.at[j, pp], {"ep": partner}).wait_recv()

    def valid_z(j):
        return (j >= 0) & (j < n_z)

    def start_all(copies):
        for c in copies:
            c.start()

    def link(way):
        return valid_z(z + 1 - 2 * way), (z if way == 0 else n_z - 1 - z)

    def upstream(way, dist):
        return z - dist * (1 - 2 * way)

    def own_w(depths, chunks):
        for way in (0, 1):
            there, depth = link(way)
            for q in depths:
                @pl.when(there & (depth == q))
                def _():
                    for c in chunks:
                        w_copy(z, c, way).start()

    def pass_w(q, dist, c, wait=True, send=True):
        for way in (0, 1):
            there, depth = link(way)

            @pl.when(there & (depth == q))
            def _():
                j = upstream(way, dist)
                if wait:
                    w_copy(j, c, way).wait_recv()
                if send:
                    w_copy(j, c, way).start()

    def pass_tokens(q, dist):
        for way in (0, 1):
            there, depth = link(way)

            @pl.when(there & (depth == q))
            def _():
                start_all(zt_copy(upstream(way, dist), way))

    def need_w(c):
        for way in (0, 1):
            there, _ = link(way)
            for dist in range(1, n_z):
                j = upstream(way, dist)

                @pl.when(jnp.logical_not(there) & valid_z(j))
                def _():
                    w_copy(j, c, way).wait_recv()

    def tokens(dist):
        for way, turn in ((0, z < 2), (1, z >= 0), (0, z >= 2)):
            there, depth = link(way)
            j = upstream(way, dist)

            @pl.when(turn & valid_z(j))
            def _():
                for c in zt_copy(j, way):
                    c.wait_recv()

                @pl.when(there & (depth == n_z - 2))
                def _():
                    start_all(zt_copy(j, way))

                for i in range(4):
                    start_all(plane_copy(j, i))

    def relay(o, which=(0, 1, 2)):
        j = plane_of(o)
        for i in which:
            plane_wait(j, flip(p, DIAG[i]))
            start_all(relay_copy(j, i))

    def landed(j, sources=DIRECT):
        for q in sources:
            plane_wait(j, partner if q == 1 else flip(partner, q))

    def early_pack(o):
        relay(o, (0, 1))
        landed(plane_of(o), DIRECT[:3])
        with jax.named_scope("compact_early"):
            pack(o, plane_of(o), EARLY, 3, True)
        relay(o, (2,))

    def batch(q, c):
        own_w((q,), (c,))
        for dist in range(1, q + 1):
            pass_w(q, dist, c)

    own_w((0, 1, 2), (0,))
    for way in (0, 1):
        there, _ = link(way)

        @pl.when(there)
        def _():
            start_all(zt_copy(z, way))
    for i in range(4):
        start_all(plane_copy(z, i))
    own_w((1,), (1,))
    own_w((0,), range(1, CHUNKS))
    tri_ref[...] = earlier(n_tok)
    for ref in (dw0_ref, dw1_ref, dwt_ref, dy_y_ref, dx_ref):
        ref[...] = jnp.zeros_like(ref)

    def end_events(k):
        if k == 0:
            tokens(1)
            relay(0)
        elif k == 1:
            tokens(2)
            need_w(0)
        elif k == 2:
            relay(1)
            need_w(1)
        elif k == 3:
            tokens(3)
        elif k == 4:
            relay(2)
        elif k in (5, 6):
            need_w(k - 3)
        elif k == 7:
            relay(3)
        else:
            need_w(k - 4)

    def mid_events(k):
        if k == 0:
            pass_w(1, 1, 0)
            pass_w(2, 1, 0)
            tokens(1)
            pass_w(1, 1, 1)
            own_w((1,), (2,))
            early_pack(0)
            pass_w(1, 1, 2)
            pass_tokens(1, 1)
            pass_w(2, 2, 0)
        elif k == 1:
            batch(2, 1)
            batch(1, 3)
        elif k == 2:
            own_w((2,), (2,))
            pass_w(2, 1, 2, send=False)
            pass_w(2, 2, 2, send=False)
        elif k == 3:
            early_pack(1)
            tokens(2)
            pass_w(2, 1, 2, wait=False)
            pass_w(2, 2, 2, wait=False)
            batch(1, 4)
            batch(1, 5)
            batch(1, 6)
        elif k == 4:
            batch(2, 3)
        elif k == 5:
            batch(2, 4)
            relay(2)
        elif k in (6, 7):
            batch(2, k - 1)
        elif k == 8:
            relay(3)

    def rows_of(s):
        return lax.div(s, per_h), pl.ds(pl.multiple_of(lax.rem(s, per_h) * cap, cap), cap)

    def pack(o, j, sources, unroll, keep_dy):
        def one(n, carry):
            s = flip(p, pick(sources, n))
            meta = meta_all[j, s]
            pos = pick_row(positions(meta, tri_ref[...], cap), e_mine)
            hit = iota_f32((cap, n_tok), 0) == pos
            r_row = (jnp.where(meta[0:1, :] == e_mine, meta[2:3, :], 0.0)
                     + jnp.where(meta[1:2, :] == e_mine, meta[3:4, :], 0.0))
            r_col = jnp.sum(jnp.where(hit, r_row, 0.0), axis=1, keepdims=True)
            got = dot_nn(jnp.where(hit, 1.0, 0.0).astype(BF16), xd_all[j, s])
            h, rows = rows_of(s)
            dy = got[:, d:]
            xc_ref[o * n_h + h, rows, :] = got[:, :d].astype(BF16)
            gc_ref[o * n_h + h, rows, :] = (r_col * dy).astype(BF16)

            if keep_dy:
                dyc_ref[o, h, rows, :] = dy.astype(BF16)
            return carry

        lax.fori_loop(0, len(sources), one, 0, unroll=unroll)

    def turned(o):
        def turn(h, carry):
            xt_ref[o * n_h + h] = xc_ref[o * n_h + h, :, own_rows].T
            gt_ref[o * n_h + h] = gc_ref[o * n_h + h, :, own_rows].T
            return carry

        lax.fori_loop(0, n_h, turn, 0)

    def cells(o, c, own):
        cols = pl.ds(pl.multiple_of(c * fc, fc), fc)
        w1, w3, w2 = w_all[0, :, cols], w_all[1, :, cols], w_all[2, :, cols]
        rows = xc_ref.shape[1]
        size = rows // SUB
        subs = [(h, slice(n * size, (n + 1) * size)) for h in range(n_h) for n in range(SUB)]
        sums = [None] * 3
        held = []

        def behind(n):
            h, at = subs[n]
            a, dh1, dh3 = held[n]
            i = o * n_h + h
            for m, (left, right) in enumerate(((xt_ref, dh1), (xt_ref, dh3), (gt_ref, a))):
                term = dot_nn(left[i, :, at], right)
                sums[m] = term if sums[m] is None else sums[m] + term
            if own:
                grown = dyc_ref[o, h, at, :].astype(F32) * dot_nt(a, w2)
                wide = dy_y_ref.shape[-1]
                dy_y_ref[o, h, at, :] += sum(grown[:, m:m + wide] for m in range(0, d, wide))
                dx_ref[o, h, at, :] += dot_nt(dh1, w1) + dot_nt(dh3, w3)

        for n, (h, at) in enumerate(subs):
            i = o * n_h + h
            h1 = dot_nn(xc_ref[i, at, :], w1)
            h3 = dot_nn(xc_ref[i, at, :], w3)
            da = dot_nn(gc_ref[i, at, :], w2)
            s = jax.nn.sigmoid(h1)
            a = (h1 * s * h3).astype(BF16)
            t = da * s
            dh3 = (t * h1).astype(BF16)
            dh1 = (t * h3 * (1.0 + h1 * (1.0 - s))).astype(BF16)
            held.append((a, dh1, dh3))
            if n:
                behind(n - 1)
        behind(len(subs) - 1)
        for ref, total in zip((dw0_ref, dw1_ref, dwt_ref), sums):
            ref[:, cols] += total

    def send_back(o):
        j = plane_of(o)

        def leave(n):
            to = flip(p, pick(RETURN, n))

            @pl.when(to != p)
            def _():
                start_all(back_copy(o, to))

            @pl.when(to == p)
            def _():
                start_all(own_back(o))

        def one(n):
            s = flip(p, pick(RETURN, n))
            h, rows = rows_of(s)
            dxs_ref[o, s] = dx_ref[o, h, rows, :].astype(BF16)
            dr_col = jnp.sum(dy_y_ref[o, h, rows, :], axis=1, keepdims=True)
            pos = pick_row(positions(meta_all[j, s], tri_ref[...], cap), e_mine)
            hit = iota_f32((cap, n_tok), 0) == pos
            dr_row = jnp.sum(jnp.where(hit, dr_col, 0.0), axis=0, keepdims=True)
            drs_ref[o, s] = jnp.broadcast_to(dr_row, (8, n_tok))

        def pair(n, carry):
            one(2 * n)
            one(2 * n + 1)

            @pl.when(n > 0)
            def _():
                leave(2 * n - 2)
                leave(2 * n - 1)

            return carry

        lax.fori_loop(0, n_p // 2, pair, 0)
        leave(n_p - 2)
        leave(n_p - 1)

    def back_copy(o, to):
        return (remote(drs_ref.at[o, to], drr_ref.at[o, p], s_dr.at[o, to], r_dr.at[o, p], {"ep": to}),
                remote(dxs_ref.at[o, to], dxr_ref.at[o, p], s_dx.at[o, to], r_dx.at[o, p], {"ep": to}))

    def own_back(o):
        return (pltpu.make_async_copy(drs_ref.at[o, p], drr_ref.at[o, p], s_dr.at[o, p]),
                pltpu.make_async_copy(dxs_ref.at[o, p], dxr_ref.at[o, p], s_dx.at[o, p]))

    def gather(o):
        meta = meta_all[plane_of(o), p]
        pos16 = positions(meta, tri_ref[...], cap)
        gxa_ref[...] = jnp.zeros_like(gxa_ref)
        dr_ref[o] = jnp.zeros_like(dr_ref[o])

        for q in range(1, n_p):
            e = flip(p, q)
            remote(drs_ref.at[o, e], drr_ref.at[o, e], s_dr.at[o, e], r_dr.at[o, e], {"ep": e}).wait_recv()
            remote(dxs_ref.at[o, e], dxr_ref.at[o, e], s_dx.at[o, e], r_dx.at[o, e], {"ep": e}).wait_recv()
        for c in own_back(o):
            c.wait()

        def one(e, carry):
            ef = e.astype(F32)
            pos = pick_row(pos16, ef)
            hit = jnp.where(iota_f32((cap, n_tok), 0) == pos, 1.0, 0.0).astype(BF16)
            gxa_ref[...] += dot_tn(hit, dxr_ref[o, e])
            dr = drr_ref[o, e]
            dr_ref[o] += jnp.where(meta == ef, dr[0:1, :], 0.0)
            return carry

        lax.fori_loop(0, n_p, one, 0, unroll=4)
        gx_ref[o] = gxa_ref[...].astype(BF16)

    def sums_out(way):
        dev = {"fsdp": z + 1 - 2 * way}
        return (remote(dr_ref.at[1], dr_out, s_gx.at[0], r_gx.at[0], dev),
                remote(gx_ref.at[1], gx_out, s_gx.at[1], r_gx.at[1], dev))

    n_steps = len(END_STEPS)

    def stores(c):
        cols = pl.ds(pl.multiple_of(c * fc, fc), fc)
        return (pltpu.make_async_copy(dw0_ref.at[:, cols], dw0_out.at[:, cols], s_dw.at[0, c]),
                pltpu.make_async_copy(dw1_ref.at[:, cols], dw1_out.at[:, cols], s_dw.at[1, c]),
                pltpu.make_async_copy(dw2_ref.at[cols, :], dw2_out.at[cols, :], s_dw.at[2, c]))

    def chosen(of, k):
        return jnp.where(mid, pick([of(t) for t in MID_STEPS], k), pick([of(t) for t in END_STEPS], k))

    def step(k, carry):
        for n in range(n_steps):
            @pl.when((k == n) & mid)
            def _():
                with jax.named_scope(f"mid_{n}"):
                    mid_events(n)

            @pl.when((k == n) & jnp.logical_not(mid))
            def _():
                with jax.named_scope(f"end_{n}"):
                    end_events(n)

        packed = chosen(lambda t: t[0], k)

        @pl.when(packed >= 0)
        def _():
            j = plane_of(packed)
            @pl.when(mid & (packed < 2))
            def _():
                landed(j, DIRECT[3:])
                with jax.named_scope("compact"):
                    pack(packed, j, LATE, 2, True)

            @pl.when(jnp.logical_not(mid & (packed < 2)))
            def _():
                landed(j)
                with jax.named_scope("compact"):
                    pack(packed, j, EARLY + LATE, 4, False)

            turned(packed)

        @pl.when(mid & (k == GATHER_STEP))
        def _():
            with jax.named_scope("gather"):
                gather(1)
            for way in (0, 1):
                @pl.when((z == 2) if way == 0 else (z == 1))
                def _():
                    start_all(sums_out(way))

        def dx_plane(m, carry):
            o = 1 - m

            def chunk(c, carry):
                with jax.named_scope("cells_own"):
                    cells(o, c, True)
                return carry

            lo = pick([chosen(lambda t, n=n: t[1 + n][0], k) for n in range(2)], o)
            hi = pick([chosen(lambda t, n=n: t[1 + n][1], k) for n in range(2)], o)
            lax.fori_loop(lo, hi, chunk, 0)

            @pl.when(k == SEND_STEP)
            def _():
                with jax.named_scope("send_back"):
                    send_back(o)

            return carry

        lax.fori_loop(0, jnp.where(mid, 2, 0), dx_plane, 0)

        def plane(o, carry):
            def chunk(c, carry):
                with jax.named_scope("cells"):
                    cells(o, c, False)

                @pl.when(o == n_z - 1)
                def _():
                    cols = pl.ds(pl.multiple_of(c * fc, fc), fc)
                    dw2_ref[cols, :] = dwt_ref[:, cols].T
                    start_all(stores(c))

                return carry

            lo = pick([chosen(lambda t, n=n: t[1 + n][0], k) for n in range(n_z)], o)
            hi = pick([chosen(lambda t, n=n: t[1 + n][1], k) for n in range(n_z)], o)
            return lax.fori_loop(lo, hi, chunk, carry)

        return lax.fori_loop(jnp.where(mid, 2, 0), n_z, plane, carry)

    lax.fori_loop(0, n_steps, step, 0)

    @pl.when(mid)
    def _():
        with jax.named_scope("gather"):
            gather(0)
        own_sums = (pltpu.make_async_copy(gx_ref.at[0], gx_out, s_loc.at[3]),
                    pltpu.make_async_copy(dr_ref.at[0], dr_out, s_loc.at[4]))
        start_all(own_sums)
        for c in own_sums:
            c.wait()
        for way in (0, 1):
            @pl.when((z == 2) if way == 0 else (z == 1))
            def _():
                for c in sums_out(way):
                    c.wait_send()

    @pl.when(jnp.logical_not(mid))
    def _():
        with jax.named_scope("sums_wait"):
            for c in sums_out(0):
                c.wait_recv()

    def stored(c, carry):
        for copy in stores(c):
            copy.wait()
        return carry

    lax.fori_loop(0, CHUNKS, stored, 0)

    with jax.named_scope("drain"):
        @pl.when(mid)
        def _():
            for o in range(2):
                for q in range(1, n_p):
                    for c in back_copy(o, flip(p, q)):
                        c.wait_send()

        for i in range(4):
            for j in range(n_z):
                for c in plane_copy(j, i):
                    c.wait_send()
        for i in range(3):
            for j in range(n_z):
                for c in relay_copy(j, i):
                    c.wait_send()
        for way in (0, 1):
            there, _ = link(way)
            for dist in range(n_z):
                j = upstream(way, dist)

                @pl.when(valid_z(j) & there)
                def _():
                    for c in zt_copy(j, way):
                        c.wait_send()

                    def drain(c, carry):
                        w_copy(j, c, way).wait_send()
                        return carry

                    lax.fori_loop(0, CHUNKS, drain, 0)


def finish(gx_in, dr_in, dw0_in, dw1_in, dw2_in, gx_out, dr_out, dw0_out, dw1_out, dw2_out,
           gx_ref, dr_ref, drt_ref, dw0_ref, dw1_ref, dw2_ref, s_in, s_out):
    moves = []
    for src, via, dst in ((dw0_in, dw0_ref, dw0_out), (dw1_in, dw1_ref, dw1_out), (dw2_in, dw2_ref, dw2_out),
                          (gx_in, gx_ref, gx_out)):
        rows = src.shape[0] // PIECES
        for at in [pl.ds(i * rows, rows) for i in range(PIECES)]:
            n = len(moves)
            moves.append((pltpu.make_async_copy(src.at[at, :], via.at[at, :], s_in.at[n]),
                          pltpu.make_async_copy(via.at[at, :], dst.at[at, :], s_out.at[n])))
    dr_load = pltpu.make_async_copy(dr_in, dr_ref, s_in.at[len(moves)])
    dr_store = pltpu.make_async_copy(drt_ref, dr_out, s_out.at[len(moves)])
    dr_load.start()
    for c, _ in moves:
        c.start()
    dr_load.wait()
    drt_ref[...] = dr_ref[: drt_ref.shape[0], :]
    for c_in, c_out in moves:
        c_in.wait()
        c_out.start()
    dr_store.start()
    for _, c in moves:
        c.wait()
    dr_store.wait()


def solution(mesh):
    n_z, n_p = mesh.shape["fsdp"], mesh.shape["ep"]
    tok_spec = P(("fsdp", "ep"), None)
    spec_in = P("ep", "fsdp", None)
    spec_out = P("ep", None, "fsdp")

    def per_device(x_tok, dy_tok, expert_ids, route_w, w_gate, w_up, w_down):
        n_tok, top_k = expert_ids.shape
        d = x_tok.shape[1]
        dl, f = w_gate.shape[1], w_gate.shape[2]
        cap = capacity_of(n_tok, top_k, n_p)
        rows = 4 * cap
        n_t = n_z * n_p // 4
        sem = pltpu.SemaphoreType.DMA
        hbm = pl.BlockSpec(memory_space=pl.ANY)
        out = jax.ShapeDtypeStruct
        ids, rw = expert_ids.T, route_w.T
        dw_shapes = (out((dl, f), F32), out((dl, f), F32), out((f, dl), F32))
        back = pl.pallas_call(
            functools.partial(kernel, cap, n_z, n_p),
            out_shape=(out((n_tok, d), BF16), out((8, n_tok), F32)) + dw_shapes,
            in_specs=[hbm] * 7,
            out_specs=(hbm,) * 5,
            scratch_shapes=[
                pltpu.VMEM((n_z, n_p, n_tok, 2 * d), BF16),
                pltpu.VMEM((n_z, n_p, 8, n_tok), F32),
                pltpu.VMEM((3, n_z * dl, f), BF16),
                pltpu.VMEM((n_tok, n_tok), BF16),
                pltpu.VMEM((n_t, rows, d), BF16),
                pltpu.VMEM((n_t, rows, d), BF16),
                pltpu.VMEM((2, n_p // 4, rows, d), BF16),
                pltpu.VMEM((n_t, dl, rows), BF16),
                pltpu.VMEM((n_t, dl, rows), BF16),
                pltpu.VMEM((2, n_p // 4, rows, min(128, d)), F32),
                pltpu.VMEM((2, n_p // 4, rows, d), F32),
                pltpu.VMEM((2, n_p, cap, d), BF16),
                pltpu.VMEM((2, n_p, 8, n_tok), F32),
                pltpu.VMEM((2, n_p, cap, d), BF16),
                pltpu.VMEM((2, n_p, 8, n_tok), F32),
                pltpu.VMEM((n_tok, d), F32),
                pltpu.VMEM((2, n_tok, d), BF16),
                pltpu.VMEM((2, 8, n_tok), F32),
                pltpu.VMEM((dl, f), F32),
                pltpu.VMEM((dl, f), F32),
                pltpu.VMEM((dl, f), F32),
                pltpu.VMEM((f, dl), F32),
                pltpu.VMEM((f, dl), BF16),
                pltpu.VMEM((top_k, n_tok), jnp.int32),
                pltpu.VMEM((top_k, n_tok), F32),
                sem((2, n_z)), sem((n_z,)), sem((2, n_z)), sem((n_z,)),
                sem((2, n_z, CHUNKS)), sem((n_z, CHUNKS)),
                sem((n_z, 4)), sem((n_z, n_p)), sem((n_z, 4)), sem((n_z, n_p)),
                sem((n_z, 3)), sem((n_z, 3)),
                sem((2, n_p)), sem((2, n_p)), sem((2, n_p)), sem((2, n_p)), sem((2,)), sem((2,)),
                sem((3, CHUNKS)),
                sem((7,)),
            ],
            compiler_params=pltpu.CompilerParams(
                collective_id=0, has_side_effects=True, vmem_limit_bytes=67043328),
        )(ids, rw, x_tok, dy_tok, w_gate, w_up, w_down)
        gx, dr, dw0, dw1, dw2 = pl.pallas_call(
            finish,
            out_shape=(out((n_tok, d), BF16), out((top_k, n_tok), F32)) + dw_shapes,
            in_specs=[hbm] * 5,
            out_specs=(hbm,) * 5,
            scratch_shapes=[
                pltpu.VMEM((n_tok, d), BF16),
                pltpu.VMEM((8, n_tok), F32),
                pltpu.VMEM((top_k, n_tok), F32),
                pltpu.VMEM((dl, f), F32),
                pltpu.VMEM((dl, f), F32),
                pltpu.VMEM((f, dl), F32),
                sem((4 * PIECES + 1,)), sem((4 * PIECES + 1,)),
            ],
        )(*back)
        return gx, dr.T, dw0[None], dw1[None], dw2[None]

    return jax.shard_map(
        per_device, mesh=mesh,
        in_specs=(tok_spec, tok_spec, tok_spec, tok_spec, spec_in, spec_in, spec_out),
        out_specs=(tok_spec, tok_spec, spec_in, spec_in, spec_out),
        check_vma=False)
```

```python
import functools

import jax
import jax.numpy as jnp
from jax import lax
from jax.experimental import pallas as pl
from jax.experimental.pallas import tpu as pltpu
from jax.sharding import PartitionSpec as P

MESH = pl.DeviceIdType.MESH
CAP_FACTOR = 3
CHUNKS = 7
F32 = jnp.float32
BF16 = jnp.bfloat16
DIAG = (2, 4, 6)
DIRECT = (1, 2, 4, 6)
SUB = 3
PIECES = 4
EARLY = (0, 1, 2, 3, 4, 5)
LATE = (6, 7)
RETURN = (6, 4, 7, 5, 2, 3, 1, 0)
ORDER = ((0, 1, 2, 3), (1, 0, 2, 3), (2, 3, 1, 0), (3, 2, 1, 0))
SKIP = -1
NONE = (0, 0)
PAIR = (0, 2)
FULL = (0, CHUNKS)
ONE = tuple((c, c + 1) for c in range(CHUNKS))
END_STEPS = (
    (0, NONE, NONE, NONE, NONE),
    (SKIP, ONE[0], NONE, NONE, NONE),
    (1, ONE[1], PAIR, NONE, NONE),
    (SKIP, NONE, NONE, NONE, NONE),
    (2, NONE, NONE, PAIR, NONE),
    (SKIP, ONE[2], ONE[2], ONE[2], NONE),
    (SKIP, ONE[3], ONE[3], ONE[3], NONE),
    (3, NONE, NONE, NONE, (0, 4)),
) + tuple((SKIP, c, c, c, c) for c in ONE[4:])
MID_STEPS = (
    (0, ONE[0], NONE, NONE, NONE),
    (SKIP, ONE[1], NONE, NONE, NONE),
    (SKIP, ONE[2], NONE, NONE, NONE),
    (1, NONE, PAIR, NONE, NONE),
    (SKIP, ONE[3], (2, 4), NONE, NONE),
) + tuple((SKIP, c, c, NONE, NONE) for c in ONE[4:]) + (
    (2, NONE, NONE, FULL, NONE),
    (3, NONE, NONE, NONE, NONE),
    (SKIP, NONE, NONE, NONE, FULL),
)
SEND_STEP = 7
GATHER_STEP = 10


def capacity_of(tok_dev, top_k, experts):
    return max(8, ((CAP_FACTOR * tok_dev * top_k // experts + 7) // 8) * 8)


def flip(p, q):
    for b in (1, 2, 4):
        turned = b - 2 * b * lax.rem(lax.div(p, b), 2)
        if isinstance(q, int):
            p = p + turned if q & b else p
        else:
            p = p + lax.rem(lax.div(q, b), 2) * turned
    return p


def dot_nn(a, b):
    return jnp.dot(a, b, preferred_element_type=F32)


def dot_nt(a, b):
    return lax.dot_general(a, b, (((1,), (1,)), ((), ())), preferred_element_type=F32)


def dot_tn(a, b):
    return lax.dot_general(a, b, (((0,), (0,)), ((), ())), preferred_element_type=F32)


def iota_f32(shape, dim):
    return lax.broadcasted_iota(jnp.int32, shape, dim).astype(F32)


def earlier(n):
    return jnp.where(iota_f32((n, n), 0) < iota_f32((n, n), 1), 1.0, 0.0).astype(BF16)


def positions(meta, tri, cap):
    ids0, ids1 = meta[0:1, :], meta[1:2, :]
    row = iota_f32((16, meta.shape[1]), 0)
    chosen = jnp.where(ids0 == row, 1.0, 0.0) + jnp.where(ids1 == row, 1.0, 0.0)
    before = dot_nn(chosen.astype(BF16), tri)
    return jnp.where((chosen > 0.0) & (before < cap), before, -1.0)


def pick_row(pos16, e):
    row = iota_f32(pos16.shape, 0)
    return jnp.sum(jnp.where(row == e, pos16, 0.0), axis=0, keepdims=True)


def pick(table, i):
    return sum(jnp.where(i == n, v, 0) for n, v in enumerate(table))


def kernel(cap, n_z, n_p, ids_ref, rw_ref, x_ref, dy_ref, wg_ref, wu_ref, wd_ref,
           gx_out, dr_out, dw0_out, dw1_out, dw2_out,
           xd_all, meta_all, w_all, tri_ref, xc_ref, gc_ref, dyc_ref, xt_ref, gt_ref, dy_y_ref, dx_ref,
           dxs_ref, drs_ref, dxr_ref, drr_ref, gxa_ref, gx_ref, dr_ref,
           dw0_ref, dw1_ref, dwt_ref, dw2_ref, wd_own, ids_own, rw_own,
           s_zt, r_zt, s_zm, r_zm, s_w, r_w, s_p, r_p, s_pm, r_pm, s_r, s_rm,
           s_dx, r_dx, s_dr, r_dr, s_gx, r_gx, s_dw, s_loc):
    z = lax.axis_index("fsdp")
    p = lax.axis_index("ep")
    e_mine = p.astype(F32)
    n_tok, d = x_ref.shape
    dl, f = wg_ref.shape[1:]
    fc = f // CHUNKS
    per_h = 4
    n_h = n_p // per_h
    partner = flip(p, 1)
    mid = (z > 0) & (z < n_z - 1)
    own_rows = pl.ds(pl.multiple_of(z * dl, dl), dl)

    def plane_of(o):
        if isinstance(o, int):
            return pick([t[o] for t in ORDER], z)
        return sum(jnp.where(z == n, pick(t, o), 0) for n, t in enumerate(ORDER))

    barrier = pltpu.get_barrier_semaphore()
    for q in range(1, n_p):
        pl.semaphore_signal(barrier, inc=1, device_id={"ep": flip(p, q)}, device_id_type=MESH)
    for step in (1, -1):
        nb = z + step

        @pl.when((nb >= 0) & (nb < n_z))
        def _():
            pl.semaphore_signal(barrier, inc=1, device_id={"fsdp": nb}, device_id_type=MESH)

    load_wd = pltpu.make_async_copy(wd_ref.at[0], wd_own, s_loc.at[4])
    loads = (
        pltpu.make_async_copy(wg_ref.at[0], w_all.at[0, own_rows, :], s_loc.at[2]),
        pltpu.make_async_copy(wu_ref.at[0], w_all.at[1, own_rows, :], s_loc.at[3]),
        pltpu.make_async_copy(x_ref, xd_all.at[z, p, :, pl.ds(0, d)], s_loc.at[0]),
        pltpu.make_async_copy(dy_ref, xd_all.at[z, p, :, pl.ds(d, d)], s_loc.at[1]),
    )
    small = (pltpu.make_async_copy(ids_ref, ids_own, s_loc.at[5]),
             pltpu.make_async_copy(rw_ref, rw_own, s_loc.at[6]))
    load_wd.start()
    for c in small + loads:
        c.start()
    for c in small:
        c.wait()
    meta_all[z, p, 0:2, :] = ids_own[...].astype(F32)
    meta_all[z, p, 2:4, :] = rw_own[...]
    meta_all[z, p, 4:8, :] = jnp.zeros((4, n_tok), F32)
    load_wd.wait()
    for c in range(CHUNKS):
        w_all[2, own_rows, c * fc:(c + 1) * fc] = wd_own[c * fc:(c + 1) * fc, :].T
    for c in loads:
        c.wait()
    inner = jnp.where(z > 0, 1, 0) + jnp.where(z < n_z - 1, 1, 0)
    pl.semaphore_wait(barrier, n_p - 1 + inner)

    def remote(src, dst, ssem, rsem, dev):
        return pltpu.make_async_remote_copy(
            src_ref=src, dst_ref=dst, send_sem=ssem, recv_sem=rsem, device_id=dev, device_id_type=MESH)

    def w_block(j, c):
        return w_all.at[:, pl.ds(pl.multiple_of(j * dl, dl), dl), pl.ds(pl.multiple_of(c * fc, fc), fc)]

    def zt_copy(j, way):
        dev = {"fsdp": z + 1 - 2 * way}
        return (remote(meta_all.at[j, p], meta_all.at[j, p], s_zm.at[way, j], r_zm.at[j], dev),
                remote(xd_all.at[j, p], xd_all.at[j, p], s_zt.at[way, j], r_zt.at[j], dev))

    def w_copy(j, c, way):
        return remote(w_block(j, c), w_block(j, c), s_w.at[way, j, c], r_w.at[j, c], {"fsdp": z + 1 - 2 * way})

    def plane_copy(j, i):
        dev = {"ep": flip(p, DIRECT[i])}
        return (remote(meta_all.at[j, p], meta_all.at[j, p], s_pm.at[j, i], r_pm.at[j, p], dev),
                remote(xd_all.at[j, p], xd_all.at[j, p], s_p.at[j, i], r_p.at[j, p], dev))

    def relay_copy(j, i):
        pp = flip(p, DIAG[i])
        dev = {"ep": partner}
        return (remote(meta_all.at[j, pp], meta_all.at[j, pp], s_rm.at[j, i], r_pm.at[j, pp], dev),
                remote(xd_all.at[j, pp], xd_all.at[j, pp], s_r.at[j, i], r_p.at[j, pp], dev))

    def plane_wait(j, pp):
        remote(meta_all.at[j, pp], meta_all.at[j, pp], s_pm.at[j, 0], r_pm.at[j, pp], {"ep": partner}).wait_recv()
        remote(xd_all.at[j, pp], xd_all.at[j, pp], s_p.at[j, 0], r_p.at[j, pp], {"ep": partner}).wait_recv()

    def valid_z(j):
        return (j >= 0) & (j < n_z)

    def start_all(copies):
        for c in copies:
            c.start()

    def link(way):
        return valid_z(z + 1 - 2 * way), (z if way == 0 else n_z - 1 - z)

    def upstream(way, dist):
        return z - dist * (1 - 2 * way)

    def own_w(depths, chunks):
        for way in (0, 1):
            there, depth = link(way)
            for q in depths:
                @pl.when(there & (depth == q))
                def _():
                    for c in chunks:
                        w_copy(z, c, way).start()

    def pass_w(q, dist, c, wait=True, send=True):
        for way in (0, 1):
            there, depth = link(way)

            @pl.when(there & (depth == q))
            def _():
                j = upstream(way, dist)
                if wait:
                    w_copy(j, c, way).wait_recv()
                if send:
                    w_copy(j, c, way).start()

    def pass_tokens(q, dist):
        for way in (0, 1):
            there, depth = link(way)

            @pl.when(there & (depth == q))
            def _():
                start_all(zt_copy(upstream(way, dist), way))

    def need_w(c):
        for way in (0, 1):
            there, _ = link(way)
            for dist in range(1, n_z):
                j = upstream(way, dist)

                @pl.when(jnp.logical_not(there) & valid_z(j))
                def _():
                    w_copy(j, c, way).wait_recv()

    def tokens(dist):
        for way, turn in ((0, z < 2), (1, z >= 0), (0, z >= 2)):
            there, depth = link(way)
            j = upstream(way, dist)

            @pl.when(turn & valid_z(j))
            def _():
                for c in zt_copy(j, way):
                    c.wait_recv()

                @pl.when(there & (depth == n_z - 2))
                def _():
                    start_all(zt_copy(j, way))

                for i in range(4):
                    start_all(plane_copy(j, i))

    def relay(o, which=(0, 1, 2)):
        j = plane_of(o)
        for i in which:
            plane_wait(j, flip(p, DIAG[i]))
            start_all(relay_copy(j, i))

    def landed(j, sources=DIRECT):
        for q in sources:
            plane_wait(j, partner if q == 1 else flip(partner, q))

    def early_pack(o):
        relay(o, (0, 1))
        landed(plane_of(o), DIRECT[:3])
        with jax.named_scope("compact_early"):
            pack(o, plane_of(o), EARLY, 3, True)
        relay(o, (2,))

    def batch(q, c):
        own_w((q,), (c,))
        for dist in range(1, q + 1):
            pass_w(q, dist, c)

    own_w((0, 1, 2), (0,))
    for way in (0, 1):
        there, _ = link(way)

        @pl.when(there)
        def _():
            start_all(zt_copy(z, way))
    for i in range(4):
        start_all(plane_copy(z, i))
    own_w((1,), (1,))
    own_w((0,), range(1, CHUNKS))
    tri_ref[...] = earlier(n_tok)
    for ref in (dw0_ref, dw1_ref, dwt_ref, dy_y_ref, dx_ref):
        ref[...] = jnp.zeros_like(ref)

    def end_events(k):
        if k == 0:
            tokens(1)
            relay(0)
        elif k == 1:
            tokens(2)
            need_w(0)
        elif k == 2:
            relay(1)
            need_w(1)
        elif k == 3:
            tokens(3)
        elif k == 4:
            relay(2)
        elif k in (5, 6):
            need_w(k - 3)
        elif k == 7:
            relay(3)
        else:
            need_w(k - 4)

    def mid_events(k):
        if k == 0:
            pass_w(1, 1, 0)
            pass_w(2, 1, 0)
            tokens(1)
            pass_w(1, 1, 1)
            own_w((1,), (2,))
            early_pack(0)
            pass_w(1, 1, 2)
            pass_tokens(1, 1)
            pass_w(2, 2, 0)
        elif k == 1:
            batch(2, 1)
            batch(1, 3)
        elif k == 2:
            own_w((2,), (2,))
            pass_w(2, 1, 2, send=False)
            pass_w(2, 2, 2, send=False)
        elif k == 3:
            early_pack(1)
            tokens(2)
            pass_w(2, 1, 2, wait=False)
            pass_w(2, 2, 2, wait=False)
            batch(1, 4)
            batch(1, 5)
            batch(1, 6)
        elif k == 4:
            batch(2, 3)
        elif k == 5:
            batch(2, 4)
            relay(2)
        elif k in (6, 7):
            batch(2, k - 1)
        elif k == 8:
            relay(3)

    def rows_of(s):
        return lax.div(s, per_h), pl.ds(pl.multiple_of(lax.rem(s, per_h) * cap, cap), cap)

    def pack(o, j, sources, unroll, keep_dy):
        def one(n, carry):
            s = flip(p, pick(sources, n))
            meta = meta_all[j, s]
            pos = pick_row(positions(meta, tri_ref[...], cap), e_mine)
            hit = iota_f32((cap, n_tok), 0) == pos
            r_row = (jnp.where(meta[0:1, :] == e_mine, meta[2:3, :], 0.0)
                     + jnp.where(meta[1:2, :] == e_mine, meta[3:4, :], 0.0))
            r_col = jnp.sum(jnp.where(hit, r_row, 0.0), axis=1, keepdims=True)
            got = dot_nn(jnp.where(hit, 1.0, 0.0).astype(BF16), xd_all[j, s])
            h, rows = rows_of(s)
            dy = got[:, d:]
            xc_ref[o * n_h + h, rows, :] = got[:, :d].astype(BF16)
            gc_ref[o * n_h + h, rows, :] = (r_col * dy).astype(BF16)

            if keep_dy:
                dyc_ref[o, h, rows, :] = dy.astype(BF16)
            return carry

        lax.fori_loop(0, len(sources), one, 0, unroll=unroll)

    def turned(o):
        def turn(h, carry):
            xt_ref[o * n_h + h] = xc_ref[o * n_h + h, :, own_rows].T
            gt_ref[o * n_h + h] = gc_ref[o * n_h + h, :, own_rows].T
            return carry

        lax.fori_loop(0, n_h, turn, 0)

    def cells(o, c, own):
        cols = pl.ds(pl.multiple_of(c * fc, fc), fc)
        w1, w3, w2 = w_all[0, :, cols], w_all[1, :, cols], w_all[2, :, cols]
        rows = xc_ref.shape[1]
        size = rows // SUB
        subs = [(h, slice(n * size, (n + 1) * size)) for h in range(n_h) for n in range(SUB)]
        sums = [None] * 3
        held = []

        def behind(n):
            h, at = subs[n]
            a, dh1, dh3 = held[n]
            i = o * n_h + h
            for m, (left, right) in enumerate(((xt_ref, dh1), (xt_ref, dh3), (gt_ref, a))):
                term = dot_nn(left[i, :, at], right)
                sums[m] = term if sums[m] is None else sums[m] + term
            if own:
                grown = dyc_ref[o, h, at, :].astype(F32) * dot_nt(a, w2)
                wide = dy_y_ref.shape[-1]
                dy_y_ref[o, h, at, :] += sum(grown[:, m:m + wide] for m in range(0, d, wide))
                dx_ref[o, h, at, :] += dot_nt(dh1, w1) + dot_nt(dh3, w3)

        for n, (h, at) in enumerate(subs):
            i = o * n_h + h
            h1 = dot_nn(xc_ref[i, at, :], w1)
            h3 = dot_nn(xc_ref[i, at, :], w3)
            da = dot_nn(gc_ref[i, at, :], w2)
            s = jax.nn.sigmoid(h1)
            a = (h1 * s * h3).astype(BF16)
            t = da * s
            dh3 = (t * h1).astype(BF16)
            dh1 = (t * h3 * (1.0 + h1 * (1.0 - s))).astype(BF16)
            held.append((a, dh1, dh3))
            if n:
                behind(n - 1)
        behind(len(subs) - 1)
        for ref, total in zip((dw0_ref, dw1_ref, dwt_ref), sums):
            ref[:, cols] += total

    def send_back(o):
        j = plane_of(o)

        def leave(n):
            to = flip(p, pick(RETURN, n))

            @pl.when(to != p)
            def _():
                start_all(back_copy(o, to))

            @pl.when(to == p)
            def _():
                start_all(own_back(o))

        def one(n):
            s = flip(p, pick(RETURN, n))
            h, rows = rows_of(s)
            dxs_ref[o, s] = dx_ref[o, h, rows, :].astype(BF16)
            dr_col = jnp.sum(dy_y_ref[o, h, rows, :], axis=1, keepdims=True)
            pos = pick_row(positions(meta_all[j, s], tri_ref[...], cap), e_mine)
            hit = iota_f32((cap, n_tok), 0) == pos
            dr_row = jnp.sum(jnp.where(hit, dr_col, 0.0), axis=0, keepdims=True)
            drs_ref[o, s] = jnp.broadcast_to(dr_row, (8, n_tok))

        def pair(n, carry):
            one(2 * n)
            one(2 * n + 1)

            @pl.when(n > 0)
            def _():
                leave(2 * n - 2)
                leave(2 * n - 1)

            return carry

        lax.fori_loop(0, n_p // 2, pair, 0)
        leave(n_p - 2)
        leave(n_p - 1)

    def back_copy(o, to):
        return (remote(drs_ref.at[o, to], drr_ref.at[o, p], s_dr.at[o, to], r_dr.at[o, p], {"ep": to}),
                remote(dxs_ref.at[o, to], dxr_ref.at[o, p], s_dx.at[o, to], r_dx.at[o, p], {"ep": to}))

    def own_back(o):
        return (pltpu.make_async_copy(drs_ref.at[o, p], drr_ref.at[o, p], s_dr.at[o, p]),
                pltpu.make_async_copy(dxs_ref.at[o, p], dxr_ref.at[o, p], s_dx.at[o, p]))

    def gather(o):
        meta = meta_all[plane_of(o), p]
        pos16 = positions(meta, tri_ref[...], cap)
        gxa_ref[...] = jnp.zeros_like(gxa_ref)
        dr_ref[o] = jnp.zeros_like(dr_ref[o])

        for q in range(1, n_p):
            e = flip(p, q)
            remote(drs_ref.at[o, e], drr_ref.at[o, e], s_dr.at[o, e], r_dr.at[o, e], {"ep": e}).wait_recv()
            remote(dxs_ref.at[o, e], dxr_ref.at[o, e], s_dx.at[o, e], r_dx.at[o, e], {"ep": e}).wait_recv()
        for c in own_back(o):
            c.wait()

        def one(e, carry):
            ef = e.astype(F32)
            pos = pick_row(pos16, ef)
            hit = jnp.where(iota_f32((cap, n_tok), 0) == pos, 1.0, 0.0).astype(BF16)
            gxa_ref[...] += dot_tn(hit, dxr_ref[o, e])
            dr = drr_ref[o, e]
            dr_ref[o] += jnp.where(meta == ef, dr[0:1, :], 0.0)
            return carry

        lax.fori_loop(0, n_p, one, 0, unroll=4)
        gx_ref[o] = gxa_ref[...].astype(BF16)

    def sums_out(way):
        dev = {"fsdp": z + 1 - 2 * way}
        return (remote(dr_ref.at[1], dr_out, s_gx.at[0], r_gx.at[0], dev),
                remote(gx_ref.at[1], gx_out, s_gx.at[1], r_gx.at[1], dev))

    def own_sums():
        return (pltpu.make_async_copy(gx_ref.at[0], gx_out, s_loc.at[3]),
                pltpu.make_async_copy(dr_ref.at[0], dr_out, s_loc.at[4]))

    n_steps = len(END_STEPS)

    def stores(c):
        cols = pl.ds(pl.multiple_of(c * fc, fc), fc)
        return (pltpu.make_async_copy(dw0_ref.at[:, cols], dw0_out.at[:, cols], s_dw.at[0, c]),
                pltpu.make_async_copy(dw1_ref.at[:, cols], dw1_out.at[:, cols], s_dw.at[1, c]),
                pltpu.make_async_copy(dw2_ref.at[cols, :], dw2_out.at[cols, :], s_dw.at[2, c]))

    def chosen(of, k):
        return jnp.where(mid, pick([of(t) for t in MID_STEPS], k), pick([of(t) for t in END_STEPS], k))

    def step(k, carry):
        for n in range(n_steps):
            @pl.when((k == n) & mid)
            def _():
                with jax.named_scope(f"mid_{n}"):
                    mid_events(n)

            @pl.when((k == n) & jnp.logical_not(mid))
            def _():
                with jax.named_scope(f"end_{n}"):
                    end_events(n)

        packed = chosen(lambda t: t[0], k)

        @pl.when(packed >= 0)
        def _():
            j = plane_of(packed)
            @pl.when(mid & (packed < 2))
            def _():
                landed(j, DIRECT[3:])
                with jax.named_scope("compact"):
                    pack(packed, j, LATE, 2, True)

            @pl.when(jnp.logical_not(mid & (packed < 2)))
            def _():
                landed(j)
                with jax.named_scope("compact"):
                    pack(packed, j, EARLY + LATE, 4, False)

            turned(packed)

        @pl.when(mid & (k == GATHER_STEP))
        def _():
            with jax.named_scope("gather"):
                gather(1)
            for way in (0, 1):
                @pl.when((z == 2) if way == 0 else (z == 1))
                def _():
                    start_all(sums_out(way))

        def dx_plane(m, carry):
            o = 1 - m

            def chunk(c, carry):
                with jax.named_scope("cells_own"):
                    cells(o, c, True)
                return carry

            lo = pick([chosen(lambda t, n=n: t[1 + n][0], k) for n in range(2)], o)
            hi = pick([chosen(lambda t, n=n: t[1 + n][1], k) for n in range(2)], o)
            lax.fori_loop(lo, hi, chunk, 0)

            @pl.when(k == SEND_STEP)
            def _():
                with jax.named_scope("send_back"):
                    send_back(o)

            return carry

        lax.fori_loop(0, jnp.where(mid, 2, 0), dx_plane, 0)

        def plane(o, carry):
            def chunk(c, carry):
                with jax.named_scope("cells"):
                    cells(o, c, False)

                @pl.when(o == n_z - 1)
                def _():
                    cols = pl.ds(pl.multiple_of(c * fc, fc), fc)
                    dw2_ref[cols, :] = dwt_ref[:, cols].T
                    start_all(stores(c))

                @pl.when(mid & (o == n_z - 1) & (c == CHUNKS - 2))
                def _():
                    with jax.named_scope("gather"):
                        gather(0)
                    start_all(own_sums())

                return carry

            lo = pick([chosen(lambda t, n=n: t[1 + n][0], k) for n in range(n_z)], o)
            hi = pick([chosen(lambda t, n=n: t[1 + n][1], k) for n in range(n_z)], o)
            return lax.fori_loop(lo, hi, chunk, carry)

        return lax.fori_loop(jnp.where(mid, 2, 0), n_z, plane, carry)

    lax.fori_loop(0, n_steps, step, 0)

    @pl.when(mid)
    def _():
        for c in own_sums():
            c.wait()
        for way in (0, 1):
            @pl.when((z == 2) if way == 0 else (z == 1))
            def _():
                for c in sums_out(way):
                    c.wait_send()

    @pl.when(jnp.logical_not(mid))
    def _():
        with jax.named_scope("sums_wait"):
            for c in sums_out(0):
                c.wait_recv()

    def stored(c, carry):
        for copy in stores(c):
            copy.wait()
        return carry

    lax.fori_loop(0, CHUNKS, stored, 0)

    with jax.named_scope("drain"):
        @pl.when(mid)
        def _():
            for o in range(2):
                for q in range(1, n_p):
                    for c in back_copy(o, flip(p, q)):
                        c.wait_send()

        for i in range(4):
            for j in range(n_z):
                for c in plane_copy(j, i):
                    c.wait_send()
        for i in range(3):
            for j in range(n_z):
                for c in relay_copy(j, i):
                    c.wait_send()
        for way in (0, 1):
            there, _ = link(way)
            for dist in range(n_z):
                j = upstream(way, dist)

                @pl.when(valid_z(j) & there)
                def _():
                    for c in zt_copy(j, way):
                        c.wait_send()

                    def drain(c, carry):
                        w_copy(j, c, way).wait_send()
                        return carry

                    lax.fori_loop(0, CHUNKS, drain, 0)


def finish(gx_in, dr_in, dw0_in, dw1_in, dw2_in, gx_out, dr_out, dw0_out, dw1_out, dw2_out,
           gx_ref, dr_ref, drt_ref, dw0_ref, dw1_ref, dw2_ref, s_in, s_out):
    moves = []
    for src, via, dst in ((dw0_in, dw0_ref, dw0_out), (dw1_in, dw1_ref, dw1_out), (dw2_in, dw2_ref, dw2_out),
                          (gx_in, gx_ref, gx_out)):
        rows = src.shape[0] // PIECES
        for at in [pl.ds(i * rows, rows) for i in range(PIECES)]:
            n = len(moves)
            moves.append((pltpu.make_async_copy(src.at[at, :], via.at[at, :], s_in.at[n]),
                          pltpu.make_async_copy(via.at[at, :], dst.at[at, :], s_out.at[n])))
    dr_load = pltpu.make_async_copy(dr_in, dr_ref, s_in.at[len(moves)])
    dr_store = pltpu.make_async_copy(drt_ref, dr_out, s_out.at[len(moves)])
    dr_load.start()
    for c, _ in moves:
        c.start()
    dr_load.wait()
    drt_ref[...] = dr_ref[: drt_ref.shape[0], :]
    for c_in, c_out in moves:
        c_in.wait()
        c_out.start()
    dr_store.start()
    for _, c in moves:
        c.wait()
    dr_store.wait()


def solution(mesh):
    n_z, n_p = mesh.shape["fsdp"], mesh.shape["ep"]
    tok_spec = P(("fsdp", "ep"), None)
    spec_in = P("ep", "fsdp", None)
    spec_out = P("ep", None, "fsdp")

    def per_device(x_tok, dy_tok, expert_ids, route_w, w_gate, w_up, w_down):
        n_tok, top_k = expert_ids.shape
        d = x_tok.shape[1]
        dl, f = w_gate.shape[1], w_gate.shape[2]
        cap = capacity_of(n_tok, top_k, n_p)
        rows = 4 * cap
        n_t = n_z * n_p // 4
        sem = pltpu.SemaphoreType.DMA
        hbm = pl.BlockSpec(memory_space=pl.ANY)
        out = jax.ShapeDtypeStruct
        ids, rw = expert_ids.T, route_w.T
        dw_shapes = (out((dl, f), F32), out((dl, f), F32), out((f, dl), F32))
        back = pl.pallas_call(
            functools.partial(kernel, cap, n_z, n_p),
            out_shape=(out((n_tok, d), BF16), out((8, n_tok), F32)) + dw_shapes,
            in_specs=[hbm] * 7,
            out_specs=(hbm,) * 5,
            scratch_shapes=[
                pltpu.VMEM((n_z, n_p, n_tok, 2 * d), BF16),
                pltpu.VMEM((n_z, n_p, 8, n_tok), F32),
                pltpu.VMEM((3, n_z * dl, f), BF16),
                pltpu.VMEM((n_tok, n_tok), BF16),
                pltpu.VMEM((n_t, rows, d), BF16),
                pltpu.VMEM((n_t, rows, d), BF16),
                pltpu.VMEM((2, n_p // 4, rows, d), BF16),
                pltpu.VMEM((n_t, dl, rows), BF16),
                pltpu.VMEM((n_t, dl, rows), BF16),
                pltpu.VMEM((2, n_p // 4, rows, min(128, d)), F32),
                pltpu.VMEM((2, n_p // 4, rows, d), F32),
                pltpu.VMEM((2, n_p, cap, d), BF16),
                pltpu.VMEM((2, n_p, 8, n_tok), F32),
                pltpu.VMEM((2, n_p, cap, d), BF16),
                pltpu.VMEM((2, n_p, 8, n_tok), F32),
                pltpu.VMEM((n_tok, d), F32),
                pltpu.VMEM((2, n_tok, d), BF16),
                pltpu.VMEM((2, 8, n_tok), F32),
                pltpu.VMEM((dl, f), F32),
                pltpu.VMEM((dl, f), F32),
                pltpu.VMEM((dl, f), F32),
                pltpu.VMEM((f, dl), F32),
                pltpu.VMEM((f, dl), BF16),
                pltpu.VMEM((top_k, n_tok), jnp.int32),
                pltpu.VMEM((top_k, n_tok), F32),
                sem((2, n_z)), sem((n_z,)), sem((2, n_z)), sem((n_z,)),
                sem((2, n_z, CHUNKS)), sem((n_z, CHUNKS)),
                sem((n_z, 4)), sem((n_z, n_p)), sem((n_z, 4)), sem((n_z, n_p)),
                sem((n_z, 3)), sem((n_z, 3)),
                sem((2, n_p)), sem((2, n_p)), sem((2, n_p)), sem((2, n_p)), sem((2,)), sem((2,)),
                sem((3, CHUNKS)),
                sem((7,)),
            ],
            compiler_params=pltpu.CompilerParams(
                collective_id=0, has_side_effects=True, vmem_limit_bytes=67043328),
        )(ids, rw, x_tok, dy_tok, w_gate, w_up, w_down)
        gx, dr, dw0, dw1, dw2 = pl.pallas_call(
            finish,
            out_shape=(out((n_tok, d), BF16), out((top_k, n_tok), F32)) + dw_shapes,
            in_specs=[hbm] * 5,
            out_specs=(hbm,) * 5,
            scratch_shapes=[
                pltpu.VMEM((n_tok, d), BF16),
                pltpu.VMEM((8, n_tok), F32),
                pltpu.VMEM((top_k, n_tok), F32),
                pltpu.VMEM((dl, f), F32),
                pltpu.VMEM((dl, f), F32),
                pltpu.VMEM((f, dl), F32),
                sem((4 * PIECES + 1,)), sem((4 * PIECES + 1,)),
            ],
        )(*back)
        return gx, dr.T, dw0[None], dw1[None], dw2[None]

    return jax.shard_map(
        per_device, mesh=mesh,
        in_specs=(tok_spec, tok_spec, tok_spec, tok_spec, spec_in, spec_in, spec_out),
        out_specs=(tok_spec, tok_spec, spec_in, spec_in, spec_out),
        check_vma=False)
```
